32 devices in a mesh: cfg: 2 (over y), ta: 2 (over x), gz: 4 (over z), gy: 2 (over core).
Axes of the slice: x: 2, y: 2, z: 4, core: 2. Of those that a mesh axis runs over, the one named last changes fastest.
Arguments:
- spatial_links: float32 [6, 2, 3, 3, 4, 4, 16, 128], P('cfg', None, None, None, 'ta', 'gz', 'gy'), parts along dimension 0, may hold values from -1 to 1, as said below
- time_links: float32 [4, 3, 3, 4, 4, 16, 128], P('cfg', None, None, 'ta', 'gz', 'gy'), parts along dimension 0, may hold values from -1 to 1, as said below
Outputs:
- polyakov: float32 [4, 4, 16, 128], P('cfg', 'gz', 'gy'), parts along dimension 0
- site_mean: float32 [4], P('cfg'), parts along dimension 0
The draws below stay inside these ranges and needn't reach their ends.
There are 2 independent parts, one for each index of `cfg`. The reference program is written for one: setup_inputs(seed, part) draws one part's arguments, and reference() takes and returns one part's arrays. A program takes and returns all parts, laid end to end along the dimension named above; each array names one. Nothing has to cross between parts.
Inputs may be any that keep to these rules, and one draw needn't show every extreme that they name: `spatial_links`: every 3x3 complex matrix (real part at index 0, imaginary at index 1 of its part dimension) is Proj, as defined in the reference program, of some complex matrix; it is special unitary where both of its first two rows had a squared norm of 0.25 or more before their division, and need not be elsewhere. `time_links`: every 3x3 complex matrix (real part at index 0, imaginary at index 1 of its part dimension) is Proj, as defined in the reference program, of some complex matrix; it is special unitary where both of its first two rows had a squared norm of 0.25 or more before their division, and need not be elsewhere.
All inputs are finite; a program needn't handle non-finite values.
Results may differ from the reference program's by a relative error of at most 0.0003.
Values sent between devices are 32-bit elements; how exact they have to be, the bound alone decides.
A program may use at most 64 MiB of HBM per device.

```python
from functools import partial
import jax
import jax.numpy as jnp
from jax import lax

NX = 128
ITERS = 3
NT = 4
NZ = 4
NY = 16


norm_floor = 0.25


def normalize_row_drawn(row_vec):
    weight = jnp.sum(row_vec[0] * row_vec[0] + row_vec[1] * row_vec[1], axis=0)
    return row_vec / jnp.sqrt(jnp.maximum(weight, norm_floor))


def project_drawn(matrix):
    first = normalize_row_drawn(matrix[:, 0])
    second_raw = matrix[:, 1]
    inner_re = jnp.sum(first[0] * second_raw[0] + first[1] * second_raw[1], axis=0)
    inner_im = jnp.sum(first[0] * second_raw[1] - first[1] * second_raw[0], axis=0)
    ortho = jnp.stack([second_raw[0] - (inner_re * first[0] - inner_im * first[1]), second_raw[1] - (inner_re * first[1] + inner_im * first[0])])
    second = normalize_row_drawn(ortho)
    first_one = jnp.roll(first, -1, axis=1)
    first_two = jnp.roll(first, -2, axis=1)
    second_one = jnp.roll(second, -1, axis=1)
    second_two = jnp.roll(second, -2, axis=1)
    cross_re = first_one[0] * second_two[0] - first_one[1] * second_two[1] - (first_two[0] * second_one[0] - first_two[1] * second_one[1])
    cross_im = first_one[0] * second_two[1] + first_one[1] * second_two[0] - (first_two[0] * second_one[1] + first_two[1] * second_one[0])
    third = jnp.stack([cross_re, -cross_im])
    return jnp.stack([first, second, third], axis=1)


def link_draw(key, leading):
    count_lead = len(leading)
    site_shape = (NT, NZ, NY, NX)
    full_shape = leading + (2, 3, 3) + site_shape
    key_noise = jax.random.fold_in(key, 1)
    key_spread = jax.random.fold_in(key, 2)
    z_share = (jnp.arange(NZ, dtype=jnp.float32) / NZ)[:, None, None]
    noise_part = jax.random.normal(key_noise, full_shape, jnp.float32)
    scale_z = 0.08 + 0.3 * z_share
    spread = jax.random.uniform(key_spread, leading + site_shape, jnp.float32, 0.5, 1.5)
    strength = jnp.expand_dims(scale_z * spread, (count_lead, count_lead + 1, count_lead + 2))
    unit_mat = jnp.stack([jnp.eye(3, dtype=jnp.float32), jnp.zeros((3, 3), jnp.float32)])
    unit_mat = unit_mat.reshape((1,) * count_lead + (2, 3, 3, 1, 1, 1, 1))
    matrix = unit_mat + strength * noise_part
    if count_lead:
        matrix = jnp.moveaxis(matrix, 0, -1)
        matrix = project_drawn(matrix)
        return jnp.moveaxis(matrix, -1, 0)
    return project_drawn(matrix)


def draw_spatial_links(key, part):
    return link_draw(jax.random.fold_in(key, 11), (3,))


def draw_time_links(key, part):
    return link_draw(jax.random.fold_in(key, 23), ())


def setup_inputs(seed: int = 0, part: int = 0) -> dict:
    arg_keys = jax.random.split(jax.random.key(seed), 3)
    part_splits = jax.random.split(jax.random.fold_in(arg_keys[2], part), 3)
    return {
        "spatial_links": draw_spatial_links(jax.random.fold_in(jax.random.fold_in(arg_keys[2], part), 71), part),
        "time_links": draw_time_links(jax.random.fold_in(jax.random.fold_in(arg_keys[2], part), 71), part),
    }


smear_weight = 0.5
norm_floor = 0.25
unit_steps = ((1, 0, 0), (0, 1, 0), (0, 0, 1))

def mat_product(lhs_mat, rhs_mat):
    lhs_re = lhs_mat[0][:, :, None]
    lhs_im = lhs_mat[1][:, :, None]
    rhs_re = rhs_mat[0][None]
    rhs_im = rhs_mat[1][None]
    real_part = lax.optimization_barrier(jnp.sum(lhs_re * rhs_re - lhs_im * rhs_im, axis=1))
    imag_part = lax.optimization_barrier(jnp.sum(lhs_re * rhs_im + lhs_im * rhs_re, axis=1))
    return jnp.stack([real_part, imag_part])

def dagger(matrix):
    return jnp.stack([jnp.swapaxes(matrix[0], 0, 1), -jnp.swapaxes(matrix[1], 0, 1)])

def normalize_row(row_vec):
    weight = lax.optimization_barrier(jnp.sum(row_vec[0] * row_vec[0] + row_vec[1] * row_vec[1], axis=0))
    return row_vec / jnp.sqrt(jnp.maximum(weight, norm_floor))

def project(matrix):
    first = normalize_row(matrix[:, 0])
    second_raw = matrix[:, 1]
    inner_re = lax.optimization_barrier(jnp.sum(first[0] * second_raw[0] + first[1] * second_raw[1], axis=0))
    inner_im = lax.optimization_barrier(jnp.sum(first[0] * second_raw[1] - first[1] * second_raw[0], axis=0))
    ortho = jnp.stack([second_raw[0] - (inner_re * first[0] - inner_im * first[1]), second_raw[1] - (inner_re * first[1] + inner_im * first[0])])
    second = normalize_row(ortho)
    first_one = jnp.roll(first, -1, axis=1)
    first_two = jnp.roll(first, -2, axis=1)
    second_one = jnp.roll(second, -1, axis=1)
    second_two = jnp.roll(second, -2, axis=1)
    cross_re = first_one[0] * second_two[0] - first_one[1] * second_two[1] - (first_two[0] * second_one[0] - first_two[1] * second_one[1])
    cross_im = first_one[0] * second_two[1] + first_one[1] * second_two[0] - (first_two[0] * second_one[1] + first_two[1] * second_one[0])
    third = jnp.stack([cross_re, -cross_im])
    return jnp.stack([first, second, third], axis=1)

def moved(offset, unit_vec, factor):
    return (offset[0] + factor * unit_vec[0], offset[1] + factor * unit_vec[1], offset[2] + factor * unit_vec[2])

def smear_spatial(neighbour):
    anchor = (0, 0, 0)
    result = []
    for mu_dir in range(3):
        staples = None
        for nu_dir in range(3):
            if nu_dir == mu_dir:
                continue
            forward = unit_steps[nu_dir]
            sideways = unit_steps[mu_dir]
            upper_staple = mat_product(mat_product(neighbour(nu_dir, anchor), neighbour(mu_dir, forward)), dagger(neighbour(nu_dir, sideways)))
            back_offset = moved(anchor, forward, -1)
            lower_staple = mat_product(mat_product(dagger(neighbour(nu_dir, back_offset)), neighbour(mu_dir, back_offset)), neighbour(nu_dir, moved(back_offset, sideways, 1)))
            if staples is None:
                staples = upper_staple + lower_staple
            else:
                staples = staples + upper_staple + lower_staple
        mixed_link = (1.0 - smear_weight) * neighbour(mu_dir, anchor) + smear_weight / 4.0 * staples
        result.append(project(mixed_link))
    return jnp.stack(result)

def smear_time(neighbour):
    anchor = (0, 0, 0)
    staples = None
    for nu_dir in range(3):
        forward = unit_steps[nu_dir]
        upper_staple = mat_product(mat_product(neighbour(nu_dir, anchor, 0), neighbour(3, forward, 0)), dagger(neighbour(nu_dir, anchor, 1)))
        back_offset = moved(anchor, forward, -1)
        lower_staple = mat_product(mat_product(dagger(neighbour(nu_dir, back_offset, 0)), neighbour(3, back_offset, 0)), neighbour(nu_dir, back_offset, 1))
        if staples is None:
            staples = upper_staple + lower_staple
        else:
            staples = staples + upper_staple + lower_staple
    mixed_link = (1.0 - smear_weight) * neighbour(3, anchor, 0) + smear_weight / 6.0 * staples
    return project(mixed_link)

def periodic(field, offset):
    return jnp.roll(field, (-offset[2], -offset[1], -offset[0]), axis=(-3, -2, -1))

def slice_neighbour(field, direction, offset):
    return periodic(field[direction], offset)

def time_neighbour(here_links, ahead_links, time_slice, direction, offset, later):
    if direction == 3:
        return periodic(time_slice, offset)
    if later:
        return periodic(ahead_links[direction], offset)
    return periodic(here_links[direction], offset)

def smear_slice(link_slice):
    for sweep_index in range(ITERS):
        current = link_slice
        link_slice = smear_spatial(partial(slice_neighbour, current))
    return link_slice

def smooth_slice(packed):
    return smear_time(partial(time_neighbour, packed[0], packed[1], packed[2]))

def reference(spatial_links, time_links):
    smeared = lax.map(smear_slice, jnp.moveaxis(spatial_links, 4, 0))
    following = jnp.roll(smeared, -1, axis=0)
    time_major = jnp.moveaxis(time_links, 3, 0)
    smoothed = lax.map(smooth_slice, (smeared, following, time_major))
    shape_rest = smoothed.shape[4:]
    unit_mat = jnp.stack([jnp.broadcast_to(jnp.eye(3, dtype=time_links.dtype)[:, :, None, None, None], (3, 3) + shape_rest), jnp.zeros((3, 3) + shape_rest, time_links.dtype)])

    def advance(carry, link_now):
        return (mat_product(carry, link_now), None)
    whole_prod, unused = lax.scan(advance, unit_mat, smoothed)
    polyakov = jnp.stack([whole_prod[0, 0, 0] + whole_prod[0, 1, 1] + whole_prod[0, 2, 2], whole_prod[1, 0, 0] + whole_prod[1, 1, 1] + whole_prod[1, 2, 2]]) / 3.0
    site_mean = lax.optimization_barrier(jnp.mean(polyakov, axis=(1, 2, 3)))
    return (polyakov, site_mean)
```

```python
from functools import partial

import jax
import jax.numpy as jnp
from jax import lax
from jax.experimental import pallas as pl
from jax.experimental.pallas import tpu as pltpu
from jax.sharding import PartitionSpec as P

ITERS = 3


smear_weight = 0.5
norm_floor = 0.25
unit_steps = ((1, 0, 0), (0, 1, 0), (0, 0, 1))


def padded_2(cells, sides, width):
    for axis, dim in sides:
        count = lax.axis_size(axis)
        head = lax.slice_in_dim(cells, 0, width, axis=dim)
        tail = lax.slice_in_dim(cells, cells.shape[dim] - width, cells.shape[dim], axis=dim)
        cells = jnp.concatenate(
            [
                lax.ppermute(tail, axis, [(i, (i + 1) % count) for i in range(count)]),
                cells,
                lax.ppermute(head, axis, [((i + 1) % count, i) for i in range(count)]),
            ],
            axis=dim,
        )
    return cells


def shifted(shard, axis, by):
    devices = lax.axis_size(axis)
    return lax.ppermute(shard, axis, [(i, (i + by) % devices) for i in range(devices)])


def mat_product(lhs_mat, rhs_mat):
    lhs_re = lhs_mat[0][:, :, None]
    lhs_im = lhs_mat[1][:, :, None]
    rhs_re = rhs_mat[0][None]
    rhs_im = rhs_mat[1][None]
    real_part = jnp.sum(lhs_re * rhs_re - lhs_im * rhs_im, axis=1)
    imag_part = jnp.sum(lhs_re * rhs_im + lhs_im * rhs_re, axis=1)
    return jnp.stack([real_part, imag_part])


def dagger(matrix):
    return jnp.stack([jnp.swapaxes(matrix[0], 0, 1), -jnp.swapaxes(matrix[1], 0, 1)])


def normalize_row(row_vec):
    weight = jnp.sum(row_vec[0] * row_vec[0] + row_vec[1] * row_vec[1], axis=0)
    return row_vec / jnp.sqrt(jnp.maximum(weight, norm_floor))


def project(matrix):
    first = normalize_row(matrix[:, 0])
    second_raw = matrix[:, 1]
    inner_re = jnp.sum(first[0] * second_raw[0] + first[1] * second_raw[1], axis=0)
    inner_im = jnp.sum(first[0] * second_raw[1] - first[1] * second_raw[0], axis=0)
    ortho = jnp.stack(
        [
            second_raw[0] - (inner_re * first[0] - inner_im * first[1]),
            second_raw[1] - (inner_re * first[1] + inner_im * first[0]),
        ]
    )
    second = normalize_row(ortho)
    first_one = jnp.roll(first, -1, axis=1)
    first_two = jnp.roll(first, -2, axis=1)
    second_one = jnp.roll(second, -1, axis=1)
    second_two = jnp.roll(second, -2, axis=1)
    cross_re = (
        first_one[0] * second_two[0]
        - first_one[1] * second_two[1]
        - (first_two[0] * second_one[0] - first_two[1] * second_one[1])
    )
    cross_im = (
        first_one[0] * second_two[1]
        + first_one[1] * second_two[0]
        - (first_two[0] * second_one[1] + first_two[1] * second_one[0])
    )
    third = jnp.stack([cross_re, -cross_im])
    return jnp.stack([first, second, third], axis=1)


def moved(offset, unit_vec, factor):
    return (
        offset[0] + factor * unit_vec[0],
        offset[1] + factor * unit_vec[1],
        offset[2] + factor * unit_vec[2],
    )


def smear_spatial(neighbour):
    anchor = (0, 0, 0)
    result = []
    for mu_dir in range(3):
        staples = None
        for nu_dir in range(3):
            if nu_dir == mu_dir:
                continue
            forward = unit_steps[nu_dir]
            sideways = unit_steps[mu_dir]
            upper_staple = mat_product(
                mat_product(neighbour(nu_dir, anchor), neighbour(mu_dir, forward)),
                dagger(neighbour(nu_dir, sideways)),
            )
            back_offset = moved(anchor, forward, -1)
            lower_staple = mat_product(
                mat_product(dagger(neighbour(nu_dir, back_offset)), neighbour(mu_dir, back_offset)),
                neighbour(nu_dir, moved(back_offset, sideways, 1)),
            )
            if staples is None:
                staples = upper_staple + lower_staple
            else:
                staples = staples + upper_staple + lower_staple
        mixed_link = (1.0 - smear_weight) * neighbour(mu_dir, anchor) + smear_weight / 4.0 * staples
        result.append(project(mixed_link))
    return jnp.stack(result)


def window_cut(field, offset):
    z_inner = field.shape[-3] - 2
    y_inner = field.shape[-2] - 2
    piece = field[
        ..., 1 + offset[2] : 1 + offset[2] + z_inner, 1 + offset[1] : 1 + offset[1] + y_inner, :
    ]
    return jnp.roll(piece, -offset[0], axis=-1)


def padded_neighbour(padded, direction, offset):
    return window_cut(padded[direction], offset)


def smooth_by_products(link_field, time_links, extended, depth):
    later_links = extended[0:3, :, :, :, 1 : depth + 1]
    lowers = [
        mat_product(mat_product(dagger(link_field[nu_dir]), time_links), later_links[nu_dir])
        for nu_dir in range(3)
    ]
    carried = jnp.stack([time_links] + lowers)
    padded = padded_2(carried, (("gz", 5), ("gy", 6)), 1)
    anchor = (0, 0, 0)
    staples = None
    for nu_dir in range(3):
        forward = unit_steps[nu_dir]
        upper_staple = mat_product(
            mat_product(link_field[nu_dir], window_cut(padded[0], forward)),
            dagger(later_links[nu_dir]),
        )
        lower_staple = window_cut(padded[1 + nu_dir], moved(anchor, forward, -1))
        if staples is None:
            staples = upper_staple + lower_staple
        else:
            staples = staples + upper_staple + lower_staple
    mixed_link = (1.0 - smear_weight) * time_links + smear_weight / 6.0 * staples
    return project(mixed_link)


def on_device(spatial_links, time_links):
    link_field = spatial_links
    for sweep_index in range(ITERS):
        padded = padded_2(link_field, (("gz", 5), ("gy", 6)), 1)
        link_field = smear_spatial(partial(padded_neighbour, padded))
    stacked = jnp.concatenate([link_field, time_links[None]], axis=0)
    ahead_slice = shifted(stacked[:, :, :, :, 0:1], "ta", -1)
    extended = jnp.concatenate([stacked, ahead_slice], axis=4)
    depth = time_links.shape[3]
    smoothed = smooth_by_products(link_field, time_links, extended, depth)
    block_prod = smoothed[:, :, :, 0]
    block_prod = mat_product(block_prod, smoothed[:, :, :, 1])
    pieces = lax.all_gather(block_prod[None], "ta", axis=0, tiled=True)

    def advance(index, carry):
        return mat_product(carry, pieces[index])

    whole_prod = lax.fori_loop(1, pieces.shape[0], advance, pieces[0])
    polyakov = (
        jnp.stack(
            [
                whole_prod[0, 0, 0] + whole_prod[0, 1, 1] + whole_prod[0, 2, 2],
                whole_prod[1, 0, 0] + whole_prod[1, 1, 1] + whole_prod[1, 2, 2],
            ]
        )
        / 3.0
    )
    local_sums = jnp.sum(polyakov, axis=(1, 2, 3))
    totals = lax.psum(local_sums, ("gz", "gy"))
    site_count = (
        polyakov.shape[1]
        * polyakov.shape[2]
        * polyakov.shape[3]
        * lax.axis_size("gz")
        * lax.axis_size("gy")
    )
    site_mean = totals / site_count
    return (polyakov, site_mean)


HALO = ITERS + 1
MESH_ID = pl.DeviceIdType.MESH


def signed_sum(terms):
    total = None
    for sign, value in terms:
        if total is None:
            total = value if sign > 0 else -value
        elif sign > 0:
            total = total + value
        else:
            total = total - value
    return total


def times(lhs, rhs, lhs_dag=False, rhs_dag=False, rows=3):
    out = []
    for i in range(rows):
        line = []
        for j in range(3):
            real_terms, imag_terms = [], []
            for k in range(3):
                a_re, a_im = lhs[k][i] if lhs_dag else lhs[i][k]
                b_re, b_im = rhs[j][k] if rhs_dag else rhs[k][j]
                sa = -1 if lhs_dag else 1
                sb = -1 if rhs_dag else 1
                real_terms += [(1, a_re * b_re), (-sa * sb, a_im * b_im)]
                if sb > 0:
                    imag_terms += [(1, a_re * b_im), (sa, a_im * b_re)]
                else:
                    imag_terms += [(1, a_im * b_re), (-1, a_re * b_im)]
            line.append((signed_sum(real_terms), signed_sum(imag_terms)))
        out.append(line)
    return out


def unit_row(row):
    weight = signed_sum([(1, p * p) for pair in row for p in pair])
    scale = lax.rsqrt(jnp.maximum(weight, norm_floor))
    return [(re * scale, im * scale) for re, im in row]


def third_row(first, second):
    out = []
    for j in range(3):
        (a_re, a_im), (b_re, b_im) = first[(j + 1) % 3], second[(j + 2) % 3]
        (c_re, c_im), (d_re, d_im) = first[(j + 2) % 3], second[(j + 1) % 3]
        re = a_re * b_re - a_im * b_im - (c_re * d_re - c_im * d_im)
        im = c_re * d_im + c_im * d_re - (a_re * b_im + a_im * b_re)
        out.append((re, im))
    return out


def project_rows(rows):
    first = unit_row(rows[0])
    inner_re = signed_sum(
        [(1, p) for (a, b), (c, d) in zip(first, rows[1]) for p in (a * c, b * d)]
    )
    inner_im = None
    for (a, b), (c, d) in zip(first, rows[1]):
        part = a * d - b * c
        inner_im = part if inner_im is None else inner_im + part
    ortho = [
        (c - (inner_re * a - inner_im * b), d - (inner_re * b + inner_im * a))
        for (a, b), (c, d) in zip(first, rows[1])
    ]
    second = unit_row(ortho)
    return [first, second, third_row(first, second)]


def fused_kernel(
    dims, sl_hbm, tl_hbm, poly_ref, mean_ref,
    raw, packed, landed, state, ups, lows, outgoing, ahead, smooth_out, smooth_in,
    trace_out, traces, row_out, rows_in,
    load_sem, a_send, a_recv, n_send, n_recv, w_send, w_recv,
    t_send, t_recv, r_send, r_recv, near_sem, far_sem, side_sem,
):
    n_ta, n_gz, n_gy, width, sites = dims
    quarter = width // n_gz
    window = quarter + 2 * HALO
    seg = width // 2
    a, k, c = lax.axis_index("ta"), lax.axis_index("gz"), lax.axis_index("gy")
    lane = lax.broadcasted_iota(jnp.int32, (8, width), 1)
    row_id = lax.broadcasted_iota(jnp.int32, (8, width), 0)
    n_group = n_ta * n_gz * n_gy
    middle = lax.rem((k + 1) // 2, 2)
    far_half = k // 2

    def mirrored(z):
        return z + far_half * (n_gz - 1 - 2 * z)

    barrier = pltpu.get_barrier_semaphore()

    def greet(device):
        pl.semaphore_signal(barrier, inc=1, device_id=device, device_id_type=MESH_ID)

    def tell(sem, z):
        pl.semaphore_signal(sem, inc=1, device_id={"gz": z}, device_id_type=MESH_ID)

    greet({"gy": 1 - c})
    greet({"ta": 1 - a})
    for core in range(n_gy):
        greet({"gz": mirrored(middle + 1), "gy": core})

    @pl.when(middle == 1)
    def _():
        for core in range(n_gy):
            greet({"gz": mirrored(0), "gy": core})

    loads = [pltpu.make_async_copy(sl_hbm.at[d], raw.at[d], load_sem.at[d]) for d in range(3)]
    loads.append(pltpu.make_async_copy(tl_hbm, raw.at[3], load_sem.at[3]))
    for copy in loads:
        copy.start()
    wide = lax.broadcasted_iota(jnp.int32, (32, width), 1)

    def side_by_side(blocks, shift_of):
        tile = None
        for j in range(3):
            moved_block = pltpu.roll(blocks[j].reshape(32, width), shift_of(j), 1)
            tile = moved_block if j == 0 else jnp.where(wide >= window * j, moved_block, tile)
        return tile.reshape(2, 2, 8, width)

    dests = [mirrored(middle + 1), mirrored(2 - 2 * middle), mirrored(3), k]
    own = len(dests) - 1

    def pack(hop, d):
        dest = dests[hop]
        for t in range(2):
            blocks = [raw[d, :, 0:2, j, t] for j in range(3)]
            packed[hop, t, d] = side_by_side(
                blocks,
                lambda j: lax.rem(window * j + HALO + width - quarter * dest + width, width),
            )

    groups = ((0, 1), (2,), (3,))

    def exchange(hop, t_rel, group):
        t = lax.rem(c + t_rel, 2)
        part = pl.ds(groups[group][0], len(groups[group]))
        src = packed.at[hop, t, part]
        dst = landed.at[k, c, part]
        if hop == own and t_rel == 0:
            return pltpu.make_async_copy(src, dst, a_recv.at[group, k, c])
        return pltpu.make_async_remote_copy(
            src_ref=src, dst_ref=dst,
            send_sem=a_send.at[group, hop, t_rel], recv_sem=a_recv.at[group, k, c],
            device_id={"gz": dests[hop], "gy": t}, device_id_type=MESH_ID,
        )

    hops = list(range(len(dests)))
    for group, members in enumerate(groups):
        for d in members:
            loads[d].wait()
        for d in members:
            pack(0, d)
        if group == 0:
            pl.semaphore_wait(barrier, 4 + 2 * middle)

            @pl.when(middle == 1)
            def _():
                tell(near_sem, mirrored(0))
                tell(far_sem, mirrored(2))
        for hop in hops:
            if hop:
                for d in members:
                    pack(hop, d)
            if group == 0 and hop == 1:

                @pl.when(middle == 0)
                def _():
                    pl.semaphore_wait(near_sem, 1)

            if group == 0 and hop == 2:
                pl.semaphore_wait(far_sem, 1)

                @pl.when(middle == 1)
                def _():
                    tell(far_sem, mirrored(0))

                pl.semaphore_signal(
                    side_sem, inc=1, device_id={"ta": 1 - a}, device_id_type=MESH_ID
                )
            for t_rel in range(2):
                exchange(hop, t_rel, group).start()

    def arrived(group):
        part = pl.ds(groups[group][0], len(groups[group]))
        for z in range(n_gz):
            for h in range(2):
                ref = landed.at[z, h, part]
                pltpu.make_async_copy(ref, ref, a_recv.at[group, z, h]).wait()

    def spread(read, v, h):
        rows = []
        for r in range(2):
            line = []
            for j in range(3):
                pair = []
                for ri in range(2):
                    low = pltpu.roll(read(v, h, ri, r), (width - window * j) % width, 1)
                    high = pltpu.roll(
                        read(2 + v, h, ri, r), (width + seg - window * j) % width, 1
                    )
                    pair.append(jnp.where(lane < seg, low, high))
                line.append(tuple(pair))
            rows.append(line)
        rows.append(third_row(rows[0], rows[1]))
        return rows

    def unpack(d):
        for v in range(2):
            for h in range(2):
                put(d, v, h, spread(lambda z, hh, ri, r: landed[z, hh, d, ri, r], v, h))

    def put(d, v, h, mat):
        for r in range(3):
            for j in range(3):
                for ri in range(2):
                    state[d, ri, r, j, v, h] = mat[r][j][ri]

    def get(read, rows=3):
        return [[(read(0, r, j), read(1, r, j)) for j in range(3)] for r in range(rows)]

    def shift_plus(read, nu, v, h):
        if nu == 0:
            return pltpu.roll(read(v, h), width - 1, 1)
        if nu == 1:
            return jnp.where(
                row_id == 7, pltpu.roll(read(v, 1 - h), 7, 0), pltpu.roll(read(v, h), 7, 0)
            )
        return pltpu.roll(read(1 - v, h), seg * v, 1)

    def shift_minus(read, nu, v, h):
        if nu == 0:
            return pltpu.roll(read(v, h), 1, 1)
        if nu == 1:
            return jnp.where(
                row_id == 0, pltpu.roll(read(v, 1 - h), 1, 0), pltpu.roll(read(v, h), 1, 0)
            )
        return pltpu.roll(read(1 - v, h), seg * (1 - v), 1)

    def here(d, v, h):
        return get(lambda ri, r, j: state[d, ri, r, j, v, h])

    def plus(d, nu, v, h):
        return get(
            lambda ri, r, j: shift_plus(lambda vv, hh: state[d, ri, r, j, vv, hh], nu, v, h)
        )

    def keep(ref, slot, v, h, mat):
        for r in range(2):
            for j in range(3):
                for ri in range(2):
                    ref[slot, ri, r, j, v, h] = mat[r][j][ri]

    pairs = [(0, 1), (0, 2), (1, 2)]
    slot_of = {}
    for mu in range(3):
        for nu in range(3):
            if mu != nu:
                slot_of[mu, nu] = len(slot_of)

    def staples_at(chosen, index, carry):
        v, h = index // 2, lax.rem(index, 2)
        for mu, nu in chosen:
            u_mu, u_nu = here(mu, v, h), here(nu, v, h)
            nu_ahead, mu_ahead = plus(nu, mu, v, h), plus(mu, nu, v, h)
            one = times(u_mu, nu_ahead)
            keep(lows, slot_of[mu, nu], v, h, times(u_nu, one, lhs_dag=True, rows=2))
            keep(ups, slot_of[nu, mu], v, h, times(one, mu_ahead, rhs_dag=True, rows=2))
            two = times(u_nu, mu_ahead)
            keep(lows, slot_of[nu, mu], v, h, times(u_mu, two, lhs_dag=True, rows=2))
            keep(ups, slot_of[mu, nu], v, h, times(two, nu_ahead, rhs_dag=True, rows=2))
        return carry

    def mix(d, v, h, entries, factor):
        def entry(ri, r, j):
            total = None
            for slot, nu in entries:
                low = shift_minus(lambda vv, hh: lows[slot, ri, r, j, vv, hh], nu, v, h)
                part = ups[slot, ri, r, j, v, h] + low
                total = part if total is None else total + part
            return (1.0 - smear_weight) * state[d, ri, r, j, v, h] + factor * total

        return project_rows(get(entry, rows=2))

    def update_at(chosen, index, carry):
        v, h = index // 2, lax.rem(index, 2)
        for mu in chosen:
            entries = [(slot_of[mu, nu], nu) for nu in range(3) if nu != mu]
            put(mu, v, h, mix(mu, v, h, entries, smear_weight / 4.0))
        return carry

    def staples(chosen):
        lax.fori_loop(0, 4, partial(staples_at, chosen), 0)

    def update(chosen):
        lax.fori_loop(0, 4, partial(update_at, chosen), 0)

    def sweep(index, carry):
        staples(pairs)
        update((0, 1, 2))
        return carry
    arrived(0)
    unpack(0)
    unpack(1)
    staples(pairs[0:1])
    arrived(1)
    unpack(2)
    staples(pairs[1:3])
    update((0, 1, 2))
    lax.fori_loop(0, ITERS - 2, sweep, 0)

    next_copies = [
        pltpu.make_async_remote_copy(
            src_ref=outgoing.at[mu], dst_ref=ahead.at[mu],
            send_sem=n_send.at[mu], recv_sem=n_recv.at[mu],
            device_id={"ta": lax.rem(a + c + n_ta - 1, n_ta), "gy": 1 - c},
            device_id_type=MESH_ID,
        )
        for mu in range(3)
    ]

    def send_next(mu):
        for v in range(2):
            for h in range(2):
                blocks = [state[mu, :, 0:2, j, v, h] for j in range(3)]
                for s in range(2):
                    outgoing[mu, 2 * s + v, h] = side_by_side(
                        blocks, lambda j: (window * j + width - seg * s) % width
                    )
        next_copies[mu].start()
    pl.semaphore_wait(side_sem, 1)
    staples(pairs[0:2])
    update((0,))
    send_next(0)
    staples(pairs[2:3])
    update((1,))
    send_next(1)
    update((2,))
    send_next(2)
    arrived(2)
    unpack(3)

    def time_firsts_at(index, carry):
        v, h = index // 2, lax.rem(index, 2)
        for nu in range(3):
            u_nu = here(nu, v, h)
            keep(ups, nu, v, h, times(u_nu, plus(3, nu, v, h), rows=2))
            keep(lows, nu, v, h, times(u_nu, here(3, v, h), lhs_dag=True, rows=2))
        return carry

    def time_staples_at(nu, index, carry):
        v, h = index // 2, lax.rem(index, 2)
        later = spread(lambda z, hh, ri, r: ahead[nu, z, hh, ri, r], v, h)
        up = get(lambda ri, r, j: ups[nu, ri, r, j, v, h], rows=2)
        keep(ups, nu, v, h, times(up, later, rhs_dag=True, rows=2))
        low = get(lambda ri, r, j: lows[nu, ri, r, j, v, h], rows=2)
        keep(lows, nu, v, h, times(low, later, rows=2))
        return carry

    place = lax.rem(lane, seg)
    inside = (place >= HALO) & (place < HALO + quarter)

    def smooth(v, h, out_ref):
        mat = mix(3, v, h, [(nu, nu) for nu in range(3)], smear_weight / 6.0)
        for r in range(2):
            for j in range(3):
                re, im = mat[r][j]
                out_ref[r, j] = jnp.where(inside, re, pltpu.roll(im, quarter, 1))
    lax.fori_loop(0, 4, time_firsts_at, 0)
    for nu in range(3):
        next_copies[nu].wait_recv()
        lax.fori_loop(0, 4, partial(time_staples_at, nu), 0)
    w_copies = []
    for da, dc in ((1, 0), (1, 1), (0, 1)):
        to_a, to_c = lax.rem(a + da, n_ta), lax.rem(c + dc, n_gy)
        smooth(to_c, to_a, smooth_out.at[2 * da + dc])
        copy = pltpu.make_async_remote_copy(
            src_ref=smooth_out.at[2 * da + dc], dst_ref=smooth_in.at[n_gy * a + c],
            send_sem=w_send.at[2 * da + dc], recv_sem=w_recv.at[n_gy * a + c],
            device_id={"ta": to_a, "gy": to_c}, device_id_type=MESH_ID,
        )
        copy.start()
        w_copies.append(copy)
    smooth(c, a, smooth_in.at[n_gy * a + c])
    for da, dc in ((0, 1), (1, 0), (1, 1)):
        slot = n_gy * lax.rem(a + da, n_ta) + lax.rem(c + dc, n_gy)
        pltpu.make_async_copy(smooth_in.at[slot], smooth_in.at[slot], w_recv.at[slot]).wait()

    def time_link(t):
        rows = []
        for r in range(2):
            tiles = [smooth_in[t, r, j] for j in range(3)]
            rows.append([(tile, pltpu.roll(tile, width - quarter, 1)) for tile in tiles])
        rows.append(third_row(rows[0], rows[1]))
        return rows
    early = times(time_link(0), time_link(1))
    late = times(time_link(2), time_link(3))
    re_terms, im_terms = [], []
    for i in range(3):
        for j in range(3):
            p_re, p_im = early[i][j]
            q_re, q_im = late[j][i]
            re_terms += [(1, p_re * q_re), (-1, p_im * q_im)]
            im_terms += [(1, p_re * q_im), (1, p_im * q_re)]
    trace_re = signed_sum(re_terms) / 3.0
    trace_im = signed_sum(im_terms) / 3.0
    trace_out[0] = trace_re
    trace_out[1] = trace_im
    sum_re = jnp.sum(jnp.where(inside, trace_re, 0.0), axis=0, keepdims=True)
    sum_im = jnp.sum(jnp.where(inside, trace_im, 0.0), axis=0, keepdims=True)
    both_re = sum_re + pltpu.roll(sum_re, seg, 1)
    both_im = sum_im + pltpu.roll(sum_im, seg, 1)
    sums = jnp.where(lane[0:1] < seg, both_re, both_im)
    row_out[0] = sums
    targets = []
    for s in range(2):
        for ta in range(n_ta):
            z = 2 * s + c
            is_self = (z == k) & (a == ta) & (a == c)
            remote = pltpu.make_async_remote_copy(
                src_ref=trace_out, dst_ref=traces.at[k],
                send_sem=t_send.at[s, ta], recv_sem=t_recv.at[k],
                device_id={"ta": ta, "gz": z, "gy": a}, device_id_type=MESH_ID,
            )
            local = pltpu.make_async_copy(trace_out, traces.at[k], t_recv.at[k])
            targets.append((is_self, remote))
            pl.when(jnp.logical_not(is_self))(remote.start)
            pl.when(is_self)(local.start)
    row_copies = []
    for step in range(1, n_group):
        da, dk, dc = step // (n_gz * n_gy), step // n_gy % n_gz, step % n_gy
        device = {
            "ta": lax.rem(a + da, n_ta),
            "gz": lax.rem(k + dk, n_gz),
            "gy": lax.rem(c + dc, n_gy),
        }
        copy = pltpu.make_async_remote_copy(
            src_ref=row_out, dst_ref=rows_in.at[pl.ds(step, 1)],
            send_sem=r_send.at[step], recv_sem=r_recv.at[step],
            device_id=device, device_id_type=MESH_ID,
        )
        copy.start()
        row_copies.append(copy)

    for z in range(n_gz):
        pltpu.make_async_copy(traces.at[z], traces.at[z], t_recv.at[z]).wait()
    s_me = k // 2
    for ri in range(2):
        out = None
        for z in range(n_gz):
            shift = lax.rem(quarter * z + 2 * width - seg * s_me - HALO, width)
            piece = pltpu.roll(traces[z, ri], shift, 1)
            out = piece if out is None else jnp.where(lane >= quarter * z, piece, out)
        poly_ref[ri] = out
    total = sums
    for copy in row_copies:
        copy.wait_recv()
    for step in range(1, n_group):
        total = total + rows_in[step]
    mean_ref[0] = jnp.sum(jnp.where(lane[0:1] < seg, total, 0.0)) / sites
    mean_ref[1] = jnp.sum(jnp.where(lane[0:1] >= seg, total, 0.0)) / sites
    for group in range(len(groups)):
        for hop in hops:
            for t_rel in range(2):
                if hop != own or t_rel:
                    exchange(hop, t_rel, group).wait_send()
    for copy in next_copies:
        copy.wait_send()
    for copy in w_copies:
        copy.wait_send()
    for is_self, remote in targets:
        pl.when(jnp.logical_not(is_self))(remote.wait_send)
    for copy in row_copies:
        copy.wait_send()
def hand_over(poly_in, mean_in, poly_ref, mean_ref):
    poly_ref[...] = poly_in[...]
    for ri in range(2):
        mean_ref[ri] = mean_in[ri]


def fused_on_device(mesh_shape, spatial_links, time_links):
    n_ta, n_gz, n_gy = (mesh_shape[name] for name in ("ta", "gz", "gy"))
    width = spatial_links.shape[-1]
    n_group = n_ta * n_gz * n_gy
    sites = float(n_gz * n_gy * 8 * width)
    spatial = spatial_links.reshape(3, 2, 3, 3, 2, 8, width)
    times_in = time_links.reshape(2, 3, 3, 2, 8, width)
    vm = lambda *shape: pltpu.VMEM(shape + (8, width), jnp.float32)
    dma = pltpu.SemaphoreType.DMA
    poly, mean = pl.pallas_call(
        partial(fused_kernel, (n_ta, n_gz, n_gy, width, sites)),
        out_shape=(
            jax.ShapeDtypeStruct((2, 8, width), jnp.float32),
            jax.ShapeDtypeStruct((2,), jnp.float32),
        ),
        in_specs=[pl.BlockSpec(memory_space=pl.ANY)] * 2,
        out_specs=(
            pl.BlockSpec(memory_space=pltpu.VMEM),
            pl.BlockSpec(memory_space=pltpu.SMEM),
        ),
        scratch_shapes=[
            vm(4, 2, 3, 3, 2),
            vm(n_gz, 2, 4, 2, 2),
            vm(n_gz, 2, 4, 2, 2),
            vm(4, 2, 3, 3, 2, 2),
            vm(6, 2, 2, 3, 2, 2),
            vm(6, 2, 2, 3, 2, 2),
            vm(3, n_gz, 2, 2, 2),
            vm(3, n_gz, 2, 2, 2),
            vm(4, 2, 3),
            vm(4, 2, 3),
            vm(2),
            vm(n_gz, 2),
            pltpu.VMEM((1, 1, width), jnp.float32),
            pltpu.VMEM((n_group, 1, width), jnp.float32),
            dma((4,)),
            dma((3, n_gz, 2)), dma((3, n_gz, 2)),
            dma((3,)), dma((3,)), dma((4,)), dma((4,)),
            dma((2, n_ta)), dma((n_gz,)),
            dma((n_group,)), dma((n_group,)),
            *[pltpu.SemaphoreType.REGULAR] * 3,
        ],
        compiler_params=pltpu.CompilerParams(collective_id=0, has_side_effects=True),
    )(spatial, times_in)
    poly, mean = pl.pallas_call(
        hand_over,
        out_shape=(
            jax.ShapeDtypeStruct((2, 8, width), jnp.float32),
            jax.ShapeDtypeStruct((2,), jnp.float32),
        ),
        in_specs=[
            pl.BlockSpec(memory_space=pltpu.VMEM),
            pl.BlockSpec(memory_space=pltpu.SMEM),
        ],
        out_specs=(
            pl.BlockSpec(memory_space=pltpu.VMEM),
            pl.BlockSpec(memory_space=pltpu.SMEM),
        ),
    )(poly, mean)
    return poly.reshape(2, 1, 8, width), mean


def fits_fused(mesh_shape, shape):
    width = shape[-1]
    n_ta, n_gz, n_gy = (mesh_shape[name] for name in ("ta", "gz", "gy"))
    per = shape[4] // n_ta, shape[5] // n_gz, shape[6] // n_gy
    window = width // n_gz + 2 * HALO
    return (
        per == (2, 1, 8) and n_ta == 2 and n_gz == 4 and n_gy == 2
        and width == 128 and ITERS >= 2 and 3 * window <= width and 2 * window <= width
    )


def solution(mesh):
    placed = (
        P("cfg", None, None, None, "ta", "gz", "gy", None),
        P("cfg", None, None, "ta", "gz", "gy", None),
    )

    def run(spatial_links, time_links):
        fused = fits_fused(mesh.shape, spatial_links.shape)
        body = partial(fused_on_device, dict(mesh.shape)) if fused else on_device
        return jax.shard_map(
            body,
            mesh=mesh,
            in_specs=placed,
            out_specs=(P("cfg", "gz", "gy", None), P("cfg")),
            check_vma=False,
        )(spatial_links, time_links)

    return run
```

```python
from functools import partial

import jax
import jax.numpy as jnp
from jax import lax
from jax.experimental import pallas as pl
from jax.experimental.pallas import tpu as pltpu
from jax.sharding import PartitionSpec as P

ITERS = 3


smear_weight = 0.5
norm_floor = 0.25
unit_steps = ((1, 0, 0), (0, 1, 0), (0, 0, 1))


def padded_2(cells, sides, width):
    for axis, dim in sides:
        count = lax.axis_size(axis)
        head = lax.slice_in_dim(cells, 0, width, axis=dim)
        tail = lax.slice_in_dim(cells, cells.shape[dim] - width, cells.shape[dim], axis=dim)
        cells = jnp.concatenate(
            [
                lax.ppermute(tail, axis, [(i, (i + 1) % count) for i in range(count)]),
                cells,
                lax.ppermute(head, axis, [((i + 1) % count, i) for i in range(count)]),
            ],
            axis=dim,
        )
    return cells


def shifted(shard, axis, by):
    devices = lax.axis_size(axis)
    return lax.ppermute(shard, axis, [(i, (i + by) % devices) for i in range(devices)])


def mat_product(lhs_mat, rhs_mat):
    lhs_re = lhs_mat[0][:, :, None]
    lhs_im = lhs_mat[1][:, :, None]
    rhs_re = rhs_mat[0][None]
    rhs_im = rhs_mat[1][None]
    real_part = jnp.sum(lhs_re * rhs_re - lhs_im * rhs_im, axis=1)
    imag_part = jnp.sum(lhs_re * rhs_im + lhs_im * rhs_re, axis=1)
    return jnp.stack([real_part, imag_part])


def dagger(matrix):
    return jnp.stack([jnp.swapaxes(matrix[0], 0, 1), -jnp.swapaxes(matrix[1], 0, 1)])


def normalize_row(row_vec):
    weight = jnp.sum(row_vec[0] * row_vec[0] + row_vec[1] * row_vec[1], axis=0)
    return row_vec / jnp.sqrt(jnp.maximum(weight, norm_floor))


def project(matrix):
    first = normalize_row(matrix[:, 0])
    second_raw = matrix[:, 1]
    inner_re = jnp.sum(first[0] * second_raw[0] + first[1] * second_raw[1], axis=0)
    inner_im = jnp.sum(first[0] * second_raw[1] - first[1] * second_raw[0], axis=0)
    ortho = jnp.stack(
        [
            second_raw[0] - (inner_re * first[0] - inner_im * first[1]),
            second_raw[1] - (inner_re * first[1] + inner_im * first[0]),
        ]
    )
    second = normalize_row(ortho)
    first_one = jnp.roll(first, -1, axis=1)
    first_two = jnp.roll(first, -2, axis=1)
    second_one = jnp.roll(second, -1, axis=1)
    second_two = jnp.roll(second, -2, axis=1)
    cross_re = (
        first_one[0] * second_two[0]
        - first_one[1] * second_two[1]
        - (first_two[0] * second_one[0] - first_two[1] * second_one[1])
    )
    cross_im = (
        first_one[0] * second_two[1]
        + first_one[1] * second_two[0]
        - (first_two[0] * second_one[1] + first_two[1] * second_one[0])
    )
    third = jnp.stack([cross_re, -cross_im])
    return jnp.stack([first, second, third], axis=1)


def moved(offset, unit_vec, factor):
    return (
        offset[0] + factor * unit_vec[0],
        offset[1] + factor * unit_vec[1],
        offset[2] + factor * unit_vec[2],
    )


def smear_spatial(neighbour):
    anchor = (0, 0, 0)
    result = []
    for mu_dir in range(3):
        staples = None
        for nu_dir in range(3):
            if nu_dir == mu_dir:
                continue
            forward = unit_steps[nu_dir]
            sideways = unit_steps[mu_dir]
            upper_staple = mat_product(
                mat_product(neighbour(nu_dir, anchor), neighbour(mu_dir, forward)),
                dagger(neighbour(nu_dir, sideways)),
            )
            back_offset = moved(anchor, forward, -1)
            lower_staple = mat_product(
                mat_product(dagger(neighbour(nu_dir, back_offset)), neighbour(mu_dir, back_offset)),
                neighbour(nu_dir, moved(back_offset, sideways, 1)),
            )
            if staples is None:
                staples = upper_staple + lower_staple
            else:
                staples = staples + upper_staple + lower_staple
        mixed_link = (1.0 - smear_weight) * neighbour(mu_dir, anchor) + smear_weight / 4.0 * staples
        result.append(project(mixed_link))
    return jnp.stack(result)


def window_cut(field, offset):
    z_inner = field.shape[-3] - 2
    y_inner = field.shape[-2] - 2
    piece = field[
        ..., 1 + offset[2] : 1 + offset[2] + z_inner, 1 + offset[1] : 1 + offset[1] + y_inner, :
    ]
    return jnp.roll(piece, -offset[0], axis=-1)


def padded_neighbour(padded, direction, offset):
    return window_cut(padded[direction], offset)


def smooth_by_products(link_field, time_links, extended, depth):
    later_links = extended[0:3, :, :, :, 1 : depth + 1]
    lowers = [
        mat_product(mat_product(dagger(link_field[nu_dir]), time_links), later_links[nu_dir])
        for nu_dir in range(3)
    ]
    carried = jnp.stack([time_links] + lowers)
    padded = padded_2(carried, (("gz", 5), ("gy", 6)), 1)
    anchor = (0, 0, 0)
    staples = None
    for nu_dir in range(3):
        forward = unit_steps[nu_dir]
        upper_staple = mat_product(
            mat_product(link_field[nu_dir], window_cut(padded[0], forward)),
            dagger(later_links[nu_dir]),
        )
        lower_staple = window_cut(padded[1 + nu_dir], moved(anchor, forward, -1))
        if staples is None:
            staples = upper_staple + lower_staple
        else:
            staples = staples + upper_staple + lower_staple
    mixed_link = (1.0 - smear_weight) * time_links + smear_weight / 6.0 * staples
    return project(mixed_link)


def on_device(spatial_links, time_links):
    link_field = spatial_links
    for sweep_index in range(ITERS):
        padded = padded_2(link_field, (("gz", 5), ("gy", 6)), 1)
        link_field = smear_spatial(partial(padded_neighbour, padded))
    stacked = jnp.concatenate([link_field, time_links[None]], axis=0)
    ahead_slice = shifted(stacked[:, :, :, :, 0:1], "ta", -1)
    extended = jnp.concatenate([stacked, ahead_slice], axis=4)
    depth = time_links.shape[3]
    smoothed = smooth_by_products(link_field, time_links, extended, depth)
    block_prod = smoothed[:, :, :, 0]
    block_prod = mat_product(block_prod, smoothed[:, :, :, 1])
    pieces = lax.all_gather(block_prod[None], "ta", axis=0, tiled=True)

    def advance(index, carry):
        return mat_product(carry, pieces[index])

    whole_prod = lax.fori_loop(1, pieces.shape[0], advance, pieces[0])
    polyakov = (
        jnp.stack(
            [
                whole_prod[0, 0, 0] + whole_prod[0, 1, 1] + whole_prod[0, 2, 2],
                whole_prod[1, 0, 0] + whole_prod[1, 1, 1] + whole_prod[1, 2, 2],
            ]
        )
        / 3.0
    )
    local_sums = jnp.sum(polyakov, axis=(1, 2, 3))
    totals = lax.psum(local_sums, ("gz", "gy"))
    site_count = (
        polyakov.shape[1]
        * polyakov.shape[2]
        * polyakov.shape[3]
        * lax.axis_size("gz")
        * lax.axis_size("gy")
    )
    site_mean = totals / site_count
    return (polyakov, site_mean)


HALO = ITERS + 1
MESH_ID = pl.DeviceIdType.MESH


def signed_sum(terms):
    total = None
    for sign, value in terms:
        if total is None:
            total = value if sign > 0 else -value
        elif sign > 0:
            total = total + value
        else:
            total = total - value
    return total


def times(lhs, rhs, lhs_dag=False, rhs_dag=False, rows=3):
    out = []
    for i in range(rows):
        line = []
        for j in range(3):
            real_terms, imag_terms = [], []
            for k in range(3):
                a_re, a_im = lhs[k][i] if lhs_dag else lhs[i][k]
                b_re, b_im = rhs[j][k] if rhs_dag else rhs[k][j]
                sa = -1 if lhs_dag else 1
                sb = -1 if rhs_dag else 1
                real_terms += [(1, a_re * b_re), (-sa * sb, a_im * b_im)]
                if sb > 0:
                    imag_terms += [(1, a_re * b_im), (sa, a_im * b_re)]
                else:
                    imag_terms += [(1, a_im * b_re), (-1, a_re * b_im)]
            line.append((signed_sum(real_terms), signed_sum(imag_terms)))
        out.append(line)
    return out


def unit_row(row):
    weight = signed_sum([(1, p * p) for pair in row for p in pair])
    scale = lax.rsqrt(jnp.maximum(weight, norm_floor))
    return [(re * scale, im * scale) for re, im in row]


def third_row(first, second):
    out = []
    for j in range(3):
        (a_re, a_im), (b_re, b_im) = first[(j + 1) % 3], second[(j + 2) % 3]
        (c_re, c_im), (d_re, d_im) = first[(j + 2) % 3], second[(j + 1) % 3]
        re = a_re * b_re - a_im * b_im - (c_re * d_re - c_im * d_im)
        im = c_re * d_im + c_im * d_re - (a_re * b_im + a_im * b_re)
        out.append((re, im))
    return out


def project_rows(rows):
    first = unit_row(rows[0])
    inner_re = signed_sum(
        [(1, p) for (a, b), (c, d) in zip(first, rows[1]) for p in (a * c, b * d)]
    )
    inner_im = None
    for (a, b), (c, d) in zip(first, rows[1]):
        part = a * d - b * c
        inner_im = part if inner_im is None else inner_im + part
    ortho = [
        (c - (inner_re * a - inner_im * b), d - (inner_re * b + inner_im * a))
        for (a, b), (c, d) in zip(first, rows[1])
    ]
    second = unit_row(ortho)
    return [first, second, third_row(first, second)]


def fused_kernel(
    dims, sl_hbm, tl_hbm, poly_ref, total_ref,
    raw, packed, landed, state, ups, lows, outgoing, ahead, smooth_out, smooth_in,
    trace_out, traces, row_out, rows_in,
    load_sem, a_send, a_recv, n_send, n_recv, w_send, w_recv,
    t_send, t_recv, r_send, r_recv, near_sem, far_sem, side_sem,
):
    n_ta, n_gz, n_gy, width, sites = dims
    quarter = width // n_gz
    window = quarter + 2 * HALO
    seg = width // 2
    a, k, c = lax.axis_index("ta"), lax.axis_index("gz"), lax.axis_index("gy")
    lane = lax.broadcasted_iota(jnp.int32, (8, width), 1)
    row_id = lax.broadcasted_iota(jnp.int32, (8, width), 0)
    n_group = n_ta * n_gz * n_gy
    middle = lax.rem((k + 1) // 2, 2)
    far_half = k // 2

    def mirrored(z):
        return z + far_half * (n_gz - 1 - 2 * z)

    barrier = pltpu.get_barrier_semaphore()

    def greet(device):
        pl.semaphore_signal(barrier, inc=1, device_id=device, device_id_type=MESH_ID)

    def tell(sem, z):
        pl.semaphore_signal(sem, inc=1, device_id={"gz": z}, device_id_type=MESH_ID)

    greet({"gy": 1 - c})
    greet({"ta": 1 - a})
    for core in range(n_gy):
        greet({"gz": mirrored(middle + 1), "gy": core})

    @pl.when(middle == 1)
    def _():
        for core in range(n_gy):
            greet({"gz": mirrored(0), "gy": core})

    loads = [pltpu.make_async_copy(sl_hbm.at[d], raw.at[d], load_sem.at[d]) for d in range(3)]
    loads.append(pltpu.make_async_copy(tl_hbm, raw.at[3], load_sem.at[3]))
    for copy in loads:
        copy.start()
    def settle(ref, sem):
        pltpu.make_async_copy(ref, ref, sem).wait()

    wide = lax.broadcasted_iota(jnp.int32, (32, width), 1)

    def side_by_side(blocks, shift_of):
        tile = None
        for j in range(3):
            moved_block = pltpu.roll(blocks[j].reshape(32, width), shift_of(j), 1)
            tile = moved_block if j == 0 else jnp.where(wide >= window * j, moved_block, tile)
        return tile.reshape(2, 2, 8, width)

    dests = [mirrored(middle + 1), mirrored(2 - 2 * middle), mirrored(3), k]
    own = len(dests) - 1

    def pack(hop, d):
        dest = dests[hop]
        for t in range(2):
            blocks = [raw[d, :, 0:2, j, t] for j in range(3)]
            packed[hop, t, d] = side_by_side(
                blocks,
                lambda j: lax.rem(window * j + HALO + width - quarter * dest + width, width),
            )

    groups = ((0, 1), (2,), (3,))

    def exchange(hop, t_rel, group):
        t = lax.rem(c + t_rel, 2)
        part = pl.ds(groups[group][0], len(groups[group]))
        src = packed.at[hop, t, part]
        dst = landed.at[k, c, part]
        if hop == own and t_rel == 0:
            return pltpu.make_async_copy(src, dst, a_recv.at[group])
        return pltpu.make_async_remote_copy(
            src_ref=src, dst_ref=dst,
            send_sem=a_send.at[hop // own], recv_sem=a_recv.at[group],
            device_id={"gz": dests[hop], "gy": t}, device_id_type=MESH_ID,
        )

    hops = list(range(len(dests)))

    def hand_out(group):
        members = groups[group]
        for d in members:
            loads[d].wait()
        for d in members:
            pack(0, d)
        if group == 0:
            pl.semaphore_wait(barrier, 4 + 2 * middle)

            @pl.when(middle == 1)
            def _():
                tell(near_sem, mirrored(0))
                tell(far_sem, mirrored(2))
        for hop in hops:
            if hop:
                for d in members:
                    pack(hop, d)
            if group == 0 and hop == 1:

                @pl.when(middle == 0)
                def _():
                    pl.semaphore_wait(near_sem, 1)

            if group == 0 and hop == 2:
                pl.semaphore_wait(far_sem, 1)

                @pl.when(middle == 1)
                def _():
                    tell(far_sem, mirrored(0))

                pl.semaphore_signal(
                    side_sem, inc=1, device_id={"ta": 1 - a}, device_id_type=MESH_ID
                )
            for t_rel in range(2):
                exchange(hop, t_rel, group).start()

    hand_out(0)
    hand_out(1)

    def arrived(group):
        part = pl.ds(groups[group][0], len(groups[group]))
        settle(landed.at[:, :, part], a_recv.at[group])

    def spread(read, v, h):
        rows = []
        for r in range(2):
            line = []
            for j in range(3):
                pair = []
                for ri in range(2):
                    low = pltpu.roll(read(v, h, ri, r), (width - window * j) % width, 1)
                    high = pltpu.roll(
                        read(2 + v, h, ri, r), (width + seg - window * j) % width, 1
                    )
                    pair.append(jnp.where(lane < seg, low, high))
                line.append(tuple(pair))
            rows.append(line)
        rows.append(third_row(rows[0], rows[1]))
        return rows

    def unpack(d):
        for v in range(2):
            for h in range(2):
                put(d, v, h, spread(lambda z, hh, ri, r: landed[z, hh, d, ri, r], v, h))

    def put(d, v, h, mat):
        for r in range(3):
            for j in range(3):
                for ri in range(2):
                    state[d, ri, r, j, v, h] = mat[r][j][ri]

    def get(read, rows=3):
        return [[(read(0, r, j), read(1, r, j)) for j in range(3)] for r in range(rows)]

    def shift_plus(read, nu, v, h):
        if nu == 0:
            return pltpu.roll(read(v, h), width - 1, 1)
        if nu == 1:
            return jnp.where(
                row_id == 7, pltpu.roll(read(v, 1 - h), 7, 0), pltpu.roll(read(v, h), 7, 0)
            )
        return pltpu.roll(read(1 - v, h), seg * v, 1)

    def shift_minus(read, nu, v, h):
        if nu == 0:
            return pltpu.roll(read(v, h), 1, 1)
        if nu == 1:
            return jnp.where(
                row_id == 0, pltpu.roll(read(v, 1 - h), 1, 0), pltpu.roll(read(v, h), 1, 0)
            )
        return pltpu.roll(read(1 - v, h), seg * (1 - v), 1)

    def here(d, v, h):
        return get(lambda ri, r, j: state[d, ri, r, j, v, h])

    def plus(d, nu, v, h):
        return get(
            lambda ri, r, j: shift_plus(lambda vv, hh: state[d, ri, r, j, vv, hh], nu, v, h)
        )

    def keep(ref, slot, v, h, mat):
        for r in range(2):
            for j in range(3):
                for ri in range(2):
                    ref[slot, ri, r, j, v, h] = mat[r][j][ri]

    pairs = [(0, 1), (0, 2), (1, 2)]
    slot_of = {}
    for mu in range(3):
        for nu in range(3):
            if mu != nu:
                slot_of[mu, nu] = len(slot_of)

    def staples_at(chosen, index, carry):
        v, h = index // 2, lax.rem(index, 2)
        for mu, nu in chosen:
            u_mu, u_nu = here(mu, v, h), here(nu, v, h)
            nu_ahead, mu_ahead = plus(nu, mu, v, h), plus(mu, nu, v, h)
            one = times(u_mu, nu_ahead)
            keep(lows, slot_of[mu, nu], v, h, times(u_nu, one, lhs_dag=True, rows=2))
            keep(ups, slot_of[nu, mu], v, h, times(one, mu_ahead, rhs_dag=True, rows=2))
            two = times(u_nu, mu_ahead)
            keep(lows, slot_of[nu, mu], v, h, times(u_mu, two, lhs_dag=True, rows=2))
            keep(ups, slot_of[mu, nu], v, h, times(two, nu_ahead, rhs_dag=True, rows=2))
        return carry

    def mix(d, v, h, entries, factor):
        def entry(ri, r, j):
            total = None
            for slot, nu in entries:
                low = shift_minus(lambda vv, hh: lows[slot, ri, r, j, vv, hh], nu, v, h)
                part = ups[slot, ri, r, j, v, h] + low
                total = part if total is None else total + part
            return (1.0 - smear_weight) * state[d, ri, r, j, v, h] + factor * total

        return project_rows(get(entry, rows=2))

    def update_at(chosen, index, carry):
        v, h = index // 2, lax.rem(index, 2)
        for mu in chosen:
            entries = [(slot_of[mu, nu], nu) for nu in range(3) if nu != mu]
            put(mu, v, h, mix(mu, v, h, entries, smear_weight / 4.0))
        return carry

    def staples(chosen):
        lax.fori_loop(0, 4, partial(staples_at, chosen), 0)

    def update(chosen):
        lax.fori_loop(0, 4, partial(update_at, chosen), 0)

    def sweep(index, carry):
        staples(pairs)
        update((0, 1, 2))
        return carry
    arrived(0)
    unpack(0)
    unpack(1)
    staples(pairs[0:1])
    arrived(1)
    hand_out(2)
    unpack(2)
    staples(pairs[1:3])
    update((0, 1, 2))
    lax.fori_loop(0, ITERS - 2, sweep, 0)

    next_copies = [
        pltpu.make_async_remote_copy(
            src_ref=outgoing.at[mu], dst_ref=ahead.at[mu],
            send_sem=n_send.at[0], recv_sem=n_recv.at[mu],
            device_id={"ta": lax.rem(a + c + n_ta - 1, n_ta), "gy": 1 - c},
            device_id_type=MESH_ID,
        )
        for mu in range(3)
    ]

    def send_next(mu):
        for v in range(2):
            for h in range(2):
                blocks = [state[mu, :, 0:2, j, v, h] for j in range(3)]
                for s in range(2):
                    outgoing[mu, 2 * s + v, h] = side_by_side(
                        blocks, lambda j: (window * j + width - seg * s) % width
                    )
        next_copies[mu].start()
    pl.semaphore_wait(side_sem, 1)
    staples(pairs[0:2])
    update((0,))
    send_next(0)
    staples(pairs[2:3])
    update((1,))
    send_next(1)
    update((2,))
    send_next(2)
    arrived(2)
    unpack(3)

    def time_firsts_at(index, carry):
        v, h = index // 2, lax.rem(index, 2)
        for nu in range(3):
            u_nu = here(nu, v, h)
            keep(ups, nu, v, h, times(u_nu, plus(3, nu, v, h), rows=2))
            keep(lows, nu, v, h, times(u_nu, here(3, v, h), lhs_dag=True, rows=2))
        return carry

    def time_staples_at(nu, index, carry):
        v, h = index // 2, lax.rem(index, 2)
        later = spread(lambda z, hh, ri, r: ahead[nu, z, hh, ri, r], v, h)
        up = get(lambda ri, r, j: ups[nu, ri, r, j, v, h], rows=2)
        keep(ups, nu, v, h, times(up, later, rhs_dag=True, rows=2))
        low = get(lambda ri, r, j: lows[nu, ri, r, j, v, h], rows=2)
        keep(lows, nu, v, h, times(low, later, rows=2))
        return carry

    place = lax.rem(lane, seg)
    inside = (place >= HALO) & (place < HALO + quarter)

    def smooth(v, h, out_ref):
        mat = mix(3, v, h, [(nu, nu) for nu in range(3)], smear_weight / 6.0)
        for r in range(2):
            for j in range(3):
                re, im = mat[r][j]
                out_ref[r, j] = jnp.where(inside, re, pltpu.roll(im, quarter, 1))
    lax.fori_loop(0, 4, time_firsts_at, 0)
    for nu in range(3):
        next_copies[nu].wait_recv()
        lax.fori_loop(0, 4, partial(time_staples_at, nu), 0)
    for da, dc in ((1, 0), (1, 1), (0, 1)):
        to_a, to_c = lax.rem(a + da, n_ta), lax.rem(c + dc, n_gy)
        smooth(to_c, to_a, smooth_out.at[2 * da + dc])
        copy = pltpu.make_async_remote_copy(
            src_ref=smooth_out.at[2 * da + dc], dst_ref=smooth_in.at[n_gy * a + c],
            send_sem=w_send.at[0], recv_sem=w_recv.at[0],
            device_id={"ta": to_a, "gy": to_c}, device_id_type=MESH_ID,
        )
        copy.start()
    smooth(c, a, smooth_in.at[n_gy * a + c])
    settle(smooth_out.at[pl.ds(1, n_ta * n_gy - 1)], w_recv.at[0])

    def time_link(t):
        rows = []
        for r in range(2):
            tiles = [smooth_in[t, r, j] for j in range(3)]
            rows.append([(tile, pltpu.roll(tile, width - quarter, 1)) for tile in tiles])
        rows.append(third_row(rows[0], rows[1]))
        return rows
    early = times(time_link(0), time_link(1))
    late = times(time_link(2), time_link(3))
    re_terms, im_terms = [], []
    for i in range(3):
        for j in range(3):
            p_re, p_im = early[i][j]
            q_re, q_im = late[j][i]
            re_terms += [(1, p_re * q_re), (-1, p_im * q_im)]
            im_terms += [(1, p_re * q_im), (1, p_im * q_re)]
    trace_re = signed_sum(re_terms) / 3.0
    trace_im = signed_sum(im_terms) / 3.0
    trace_out[0] = trace_re
    trace_out[1] = trace_im
    sum_re = jnp.sum(jnp.where(inside, trace_re, 0.0), axis=0, keepdims=True)
    sum_im = jnp.sum(jnp.where(inside, trace_im, 0.0), axis=0, keepdims=True)
    both_re = sum_re + pltpu.roll(sum_re, seg, 1)
    both_im = sum_im + pltpu.roll(sum_im, seg, 1)
    sums = jnp.where(lane[0:1] < seg, both_re, both_im)
    row_out[0] = sums
    keeps_one = (a == c) & (lax.rem(k, 2) == c)
    for s in range(2):
        for ta in range(n_ta):
            z = 2 * s + c
            is_self = (z == k) & (a == ta) & (a == c)
            remote = pltpu.make_async_remote_copy(
                src_ref=trace_out, dst_ref=traces.at[k],
                send_sem=t_send.at[0], recv_sem=t_recv.at[0],
                device_id={"ta": ta, "gz": z, "gy": a}, device_id_type=MESH_ID,
            )
            local = pltpu.make_async_copy(trace_out, traces.at[k], t_recv.at[0])
            pl.when(jnp.logical_not(is_self))(remote.start)
            pl.when(is_self)(local.start)
    for step in range(1, n_group):
        da, dk, dc = step // (n_gz * n_gy), step // n_gy % n_gz, step % n_gy
        device = {
            "ta": lax.rem(a + da, n_ta),
            "gz": lax.rem(k + dk, n_gz),
            "gy": lax.rem(c + dc, n_gy),
        }
        copy = pltpu.make_async_remote_copy(
            src_ref=row_out, dst_ref=rows_in.at[pl.ds(step, 1)],
            send_sem=r_send.at[0], recv_sem=r_recv.at[0],
            device_id=device, device_id_type=MESH_ID,
        )
        copy.start()

    settle(traces, t_recv.at[0])
    s_me = k // 2
    for ri in range(2):
        out = None
        for z in range(n_gz):
            shift = lax.rem(quarter * z + 2 * width - seg * s_me - HALO, width)
            piece = pltpu.roll(traces[z, ri], shift, 1)
            out = piece if out is None else jnp.where(lane >= quarter * z, piece, out)
        poly_ref[ri] = out
    total = sums
    settle(rows_in.at[pl.ds(1, n_group - 1)], r_recv.at[0])
    for step in range(1, n_group):
        total = total + rows_in[step]
    total_ref[...] = total
    settle(packed.at[pl.ds(0, own)], a_send.at[0])
    settle(packed.at[own, 0], a_send.at[1])
    settle(outgoing, n_send.at[0])
    settle(smooth_out.at[pl.ds(1, n_ta * n_gy - 1)], w_send.at[0])

    @pl.when(keeps_one)
    def _():
        settle(traces.at[pl.ds(1, n_gz - 1)], t_send.at[0])

    @pl.when(jnp.logical_not(keeps_one))
    def _():
        settle(traces, t_send.at[0])

    settle(rows_in.at[pl.ds(1, n_group - 1)], r_send.at[0])
def hand_over(sites, poly_in, total_in, poly_ref, mean_ref):
    poly_ref[...] = poly_in[...]
    total = total_in[...]
    seg = total.shape[1] // 2
    place = lax.broadcasted_iota(jnp.int32, total.shape, 1)
    mean_ref[0] = jnp.sum(jnp.where(place < seg, total, 0.0)) / sites
    mean_ref[1] = jnp.sum(jnp.where(place >= seg, total, 0.0)) / sites


def fused_on_device(mesh_shape, spatial_links, time_links):
    n_ta, n_gz, n_gy = (mesh_shape[name] for name in ("ta", "gz", "gy"))
    width = spatial_links.shape[-1]
    n_group = n_ta * n_gz * n_gy
    sites = float(n_gz * n_gy * 8 * width)
    spatial = spatial_links.reshape(3, 2, 3, 3, 2, 8, width)
    times_in = time_links.reshape(2, 3, 3, 2, 8, width)
    vm = lambda *shape: pltpu.VMEM(shape + (8, width), jnp.float32)
    dma = pltpu.SemaphoreType.DMA
    poly, total = pl.pallas_call(
        partial(fused_kernel, (n_ta, n_gz, n_gy, width, sites)),
        out_shape=(
            pltpu.VMEM((2, 8, width), jnp.float32),
            pltpu.VMEM((1, width), jnp.float32),
        ),
        in_specs=[pl.BlockSpec(memory_space=pl.ANY)] * 2,
        out_specs=(pl.BlockSpec(memory_space=pltpu.VMEM),) * 2,
        scratch_shapes=[
            vm(4, 2, 3, 3, 2),
            vm(n_gz, 2, 4, 2, 2),
            vm(n_gz, 2, 4, 2, 2),
            vm(4, 2, 3, 3, 2, 2),
            vm(6, 2, 2, 3, 2, 2),
            vm(6, 2, 2, 3, 2, 2),
            vm(3, n_gz, 2, 2, 2),
            vm(3, n_gz, 2, 2, 2),
            vm(4, 2, 3),
            vm(4, 2, 3),
            vm(2),
            vm(n_gz, 2),
            pltpu.VMEM((1, 1, width), jnp.float32),
            pltpu.VMEM((n_group, 1, width), jnp.float32),
            dma((4,)),
            dma((2,)), dma((3,)), dma((1,)), dma((3,)),
            *[dma((1,))] * 6,
            *[pltpu.SemaphoreType.REGULAR] * 3,
        ],
        compiler_params=pltpu.CompilerParams(collective_id=0, has_side_effects=True),
    )(spatial, times_in)
    poly, mean = pl.pallas_call(
        partial(hand_over, sites),
        out_shape=(
            jax.ShapeDtypeStruct((2, 8, width), jnp.float32),
            jax.ShapeDtypeStruct((2,), jnp.float32),
        ),
        in_specs=[pl.BlockSpec(memory_space=pltpu.VMEM)] * 2,
        out_specs=(
            pl.BlockSpec(memory_space=pltpu.VMEM),
            pl.BlockSpec(memory_space=pltpu.SMEM),
        ),
    )(*[pltpu.with_memory_space_constraint(x, pltpu.VMEM) for x in (poly, total)])
    return poly.reshape(2, 1, 8, width), mean


def fits_fused(mesh_shape, shape):
    width = shape[-1]
    n_ta, n_gz, n_gy = (mesh_shape[name] for name in ("ta", "gz", "gy"))
    per = shape[4] // n_ta, shape[5] // n_gz, shape[6] // n_gy
    window = width // n_gz + 2 * HALO
    return (
        per == (2, 1, 8) and n_ta == 2 and n_gz == 4 and n_gy == 2
        and width == 128 and ITERS >= 2 and 3 * window <= width and 2 * window <= width
    )


def solution(mesh):
    placed = (
        P("cfg", None, None, None, "ta", "gz", "gy", None),
        P("cfg", None, None, "ta", "gz", "gy", None),
    )

    def run(spatial_links, time_links):
        fused = fits_fused(mesh.shape, spatial_links.shape)
        body = partial(fused_on_device, dict(mesh.shape)) if fused else on_device
        return jax.shard_map(
            body,
            mesh=mesh,
            in_specs=placed,
            out_specs=(P("cfg", "gz", "gy", None), P("cfg")),
            check_vma=False,
        )(spatial_links, time_links)

    return run
```

```python
from functools import partial

import jax
import jax.numpy as jnp
from jax import lax
from jax.experimental import pallas as pl
from jax.experimental.pallas import tpu as pltpu
from jax.sharding import PartitionSpec as P

ITERS = 3


smear_weight = 0.5
norm_floor = 0.25
unit_steps = ((1, 0, 0), (0, 1, 0), (0, 0, 1))


def padded_2(cells, sides, width):
    for axis, dim in sides:
        count = lax.axis_size(axis)
        head = lax.slice_in_dim(cells, 0, width, axis=dim)
        tail = lax.slice_in_dim(cells, cells.shape[dim] - width, cells.shape[dim], axis=dim)
        cells = jnp.concatenate(
            [
                lax.ppermute(tail, axis, [(i, (i + 1) % count) for i in range(count)]),
                cells,
                lax.ppermute(head, axis, [((i + 1) % count, i) for i in range(count)]),
            ],
            axis=dim,
        )
    return cells


def shifted(shard, axis, by):
    devices = lax.axis_size(axis)
    return lax.ppermute(shard, axis, [(i, (i + by) % devices) for i in range(devices)])


def mat_product(lhs_mat, rhs_mat):
    lhs_re = lhs_mat[0][:, :, None]
    lhs_im = lhs_mat[1][:, :, None]
    rhs_re = rhs_mat[0][None]
    rhs_im = rhs_mat[1][None]
    real_part = jnp.sum(lhs_re * rhs_re - lhs_im * rhs_im, axis=1)
    imag_part = jnp.sum(lhs_re * rhs_im + lhs_im * rhs_re, axis=1)
    return jnp.stack([real_part, imag_part])


def dagger(matrix):
    return jnp.stack([jnp.swapaxes(matrix[0], 0, 1), -jnp.swapaxes(matrix[1], 0, 1)])


def normalize_row(row_vec):
    weight = jnp.sum(row_vec[0] * row_vec[0] + row_vec[1] * row_vec[1], axis=0)
    return row_vec / jnp.sqrt(jnp.maximum(weight, norm_floor))


def project(matrix):
    first = normalize_row(matrix[:, 0])
    second_raw = matrix[:, 1]
    inner_re = jnp.sum(first[0] * second_raw[0] + first[1] * second_raw[1], axis=0)
    inner_im = jnp.sum(first[0] * second_raw[1] - first[1] * second_raw[0], axis=0)
    ortho = jnp.stack(
        [
            second_raw[0] - (inner_re * first[0] - inner_im * first[1]),
            second_raw[1] - (inner_re * first[1] + inner_im * first[0]),
        ]
    )
    second = normalize_row(ortho)
    first_one = jnp.roll(first, -1, axis=1)
    first_two = jnp.roll(first, -2, axis=1)
    second_one = jnp.roll(second, -1, axis=1)
    second_two = jnp.roll(second, -2, axis=1)
    cross_re = (
        first_one[0] * second_two[0]
        - first_one[1] * second_two[1]
        - (first_two[0] * second_one[0] - first_two[1] * second_one[1])
    )
    cross_im = (
        first_one[0] * second_two[1]
        + first_one[1] * second_two[0]
        - (first_two[0] * second_one[1] + first_two[1] * second_one[0])
    )
    third = jnp.stack([cross_re, -cross_im])
    return jnp.stack([first, second, third], axis=1)


def moved(offset, unit_vec, factor):
    return (
        offset[0] + factor * unit_vec[0],
        offset[1] + factor * unit_vec[1],
        offset[2] + factor * unit_vec[2],
    )


def smear_spatial(neighbour):
    anchor = (0, 0, 0)
    result = []
    for mu_dir in range(3):
        staples = None
        for nu_dir in range(3):
            if nu_dir == mu_dir:
                continue
            forward = unit_steps[nu_dir]
            sideways = unit_steps[mu_dir]
            upper_staple = mat_product(
                mat_product(neighbour(nu_dir, anchor), neighbour(mu_dir, forward)),
                dagger(neighbour(nu_dir, sideways)),
            )
            back_offset = moved(anchor, forward, -1)
            lower_staple = mat_product(
                mat_product(dagger(neighbour(nu_dir, back_offset)), neighbour(mu_dir, back_offset)),
                neighbour(nu_dir, moved(back_offset, sideways, 1)),
            )
            if staples is None:
                staples = upper_staple + lower_staple
            else:
                staples = staples + upper_staple + lower_staple
        mixed_link = (1.0 - smear_weight) * neighbour(mu_dir, anchor) + smear_weight / 4.0 * staples
        result.append(project(mixed_link))
    return jnp.stack(result)


def window_cut(field, offset):
    z_inner = field.shape[-3] - 2
    y_inner = field.shape[-2] - 2
    piece = field[
        ..., 1 + offset[2] : 1 + offset[2] + z_inner, 1 + offset[1] : 1 + offset[1] + y_inner, :
    ]
    return jnp.roll(piece, -offset[0], axis=-1)


def padded_neighbour(padded, direction, offset):
    return window_cut(padded[direction], offset)


def smooth_by_products(link_field, time_links, extended, depth):
    later_links = extended[0:3, :, :, :, 1 : depth + 1]
    lowers = [
        mat_product(mat_product(dagger(link_field[nu_dir]), time_links), later_links[nu_dir])
        for nu_dir in range(3)
    ]
    carried = jnp.stack([time_links] + lowers)
    padded = padded_2(carried, (("gz", 5), ("gy", 6)), 1)
    anchor = (0, 0, 0)
    staples = None
    for nu_dir in range(3):
        forward = unit_steps[nu_dir]
        upper_staple = mat_product(
            mat_product(link_field[nu_dir], window_cut(padded[0], forward)),
            dagger(later_links[nu_dir]),
        )
        lower_staple = window_cut(padded[1 + nu_dir], moved(anchor, forward, -1))
        if staples is None:
            staples = upper_staple + lower_staple
        else:
            staples = staples + upper_staple + lower_staple
    mixed_link = (1.0 - smear_weight) * time_links + smear_weight / 6.0 * staples
    return project(mixed_link)


def on_device(spatial_links, time_links):
    link_field = spatial_links
    for sweep_index in range(ITERS):
        padded = padded_2(link_field, (("gz", 5), ("gy", 6)), 1)
        link_field = smear_spatial(partial(padded_neighbour, padded))
    stacked = jnp.concatenate([link_field, time_links[None]], axis=0)
    ahead_slice = shifted(stacked[:, :, :, :, 0:1], "ta", -1)
    extended = jnp.concatenate([stacked, ahead_slice], axis=4)
    depth = time_links.shape[3]
    smoothed = smooth_by_products(link_field, time_links, extended, depth)
    block_prod = smoothed[:, :, :, 0]
    block_prod = mat_product(block_prod, smoothed[:, :, :, 1])
    pieces = lax.all_gather(block_prod[None], "ta", axis=0, tiled=True)

    def advance(index, carry):
        return mat_product(carry, pieces[index])

    whole_prod = lax.fori_loop(1, pieces.shape[0], advance, pieces[0])
    polyakov = (
        jnp.stack(
            [
                whole_prod[0, 0, 0] + whole_prod[0, 1, 1] + whole_prod[0, 2, 2],
                whole_prod[1, 0, 0] + whole_prod[1, 1, 1] + whole_prod[1, 2, 2],
            ]
        )
        / 3.0
    )
    local_sums = jnp.sum(polyakov, axis=(1, 2, 3))
    totals = lax.psum(local_sums, ("gz", "gy"))
    site_count = (
        polyakov.shape[1]
        * polyakov.shape[2]
        * polyakov.shape[3]
        * lax.axis_size("gz")
        * lax.axis_size("gy")
    )
    site_mean = totals / site_count
    return (polyakov, site_mean)


HALO = ITERS + 1
MESH_ID = pl.DeviceIdType.MESH


def signed_sum(terms):
    total = None
    for sign, value in terms:
        if total is None:
            total = value if sign > 0 else -value
        elif sign > 0:
            total = total + value
        else:
            total = total - value
    return total


def times(lhs, rhs, lhs_dag=False, rhs_dag=False, rows=3):
    out = []
    for i in range(rows):
        line = []
        for j in range(3):
            real_terms, imag_terms = [], []
            for k in range(3):
                a_re, a_im = lhs[k][i] if lhs_dag else lhs[i][k]
                b_re, b_im = rhs[j][k] if rhs_dag else rhs[k][j]
                sa = -1 if lhs_dag else 1
                sb = -1 if rhs_dag else 1
                real_terms += [(1, a_re * b_re), (-sa * sb, a_im * b_im)]
                if sb > 0:
                    imag_terms += [(1, a_re * b_im), (sa, a_im * b_re)]
                else:
                    imag_terms += [(1, a_im * b_re), (-1, a_re * b_im)]
            line.append((signed_sum(real_terms), signed_sum(imag_terms)))
        out.append(line)
    return out


def unit_row(row):
    weight = signed_sum([(1, p * p) for pair in row for p in pair])
    scale = lax.rsqrt(jnp.maximum(weight, norm_floor))
    return [(re * scale, im * scale) for re, im in row]


def third_row(first, second):
    out = []
    for j in range(3):
        (a_re, a_im), (b_re, b_im) = first[(j + 1) % 3], second[(j + 2) % 3]
        (c_re, c_im), (d_re, d_im) = first[(j + 2) % 3], second[(j + 1) % 3]
        re = a_re * b_re - a_im * b_im - (c_re * d_re - c_im * d_im)
        im = c_re * d_im + c_im * d_re - (a_re * b_im + a_im * b_re)
        out.append((re, im))
    return out


def project_rows(rows):
    first = unit_row(rows[0])
    inner_re = signed_sum(
        [(1, p) for (a, b), (c, d) in zip(first, rows[1]) for p in (a * c, b * d)]
    )
    inner_im = None
    for (a, b), (c, d) in zip(first, rows[1]):
        part = a * d - b * c
        inner_im = part if inner_im is None else inner_im + part
    ortho = [
        (c - (inner_re * a - inner_im * b), d - (inner_re * b + inner_im * a))
        for (a, b), (c, d) in zip(first, rows[1])
    ]
    second = unit_row(ortho)
    return [first, second, third_row(first, second)]


def fused_kernel(
    dims, sl_hbm, tl_hbm, poly_ref, total_ref,
    raw, packed, landed, state, ups, lows, outgoing, ahead, ahead_x, smooth_out, smooth_in,
    trace_out, traces, row_out, rows_in,
    load_sem, a_send, a_recv, n_send, n_recv, w_send, w_recv,
    t_send, t_recv, r_send, r_recv, near_sem, far_sem, side_sem,
):
    n_ta, n_gz, n_gy, width, sites = dims
    quarter = width // n_gz
    slot = width // 3
    tiles = range(3)
    a, k, c = lax.axis_index("ta"), lax.axis_index("gz"), lax.axis_index("gy")
    lane = lax.broadcasted_iota(jnp.int32, (8, width), 1)
    n_group = n_ta * n_gz * n_gy
    middle = lax.rem((k + 1) // 2, 2)
    far_half = k // 2

    def mirrored(z):
        return z + far_half * (n_gz - 1 - 2 * z)

    barrier = pltpu.get_barrier_semaphore()

    def greet(device):
        pl.semaphore_signal(barrier, inc=1, device_id=device, device_id_type=MESH_ID)

    def tell(sem, z):
        pl.semaphore_signal(sem, inc=1, device_id={"gz": z}, device_id_type=MESH_ID)

    greet({"gy": 1 - c})
    greet({"ta": 1 - a})
    for core in range(n_gy):
        greet({"gz": mirrored(middle + 1), "gy": core})

    @pl.when(middle == 1)
    def _():
        for core in range(n_gy):
            greet({"gz": mirrored(0), "gy": core})

    loads = [pltpu.make_async_copy(sl_hbm.at[d], raw.at[d], load_sem.at[d]) for d in range(3)]
    loads.append(pltpu.make_async_copy(tl_hbm, raw.at[3], load_sem.at[3]))
    for copy in loads:
        copy.start()
    def settle(ref, sem):
        pltpu.make_async_copy(ref, ref, sem).wait()

    wide = lax.broadcasted_iota(jnp.int32, (32, width), 1)

    def side_by_side(blocks, shift_of):
        tile = None
        for j in range(3):
            moved_block = pltpu.roll(blocks[j].reshape(32, width), shift_of(j), 1)
            tile = moved_block if j == 0 else jnp.where(wide >= slot * j, moved_block, tile)
        return tile.reshape(2, 2, 8, width)

    dests = [mirrored(middle + 1), mirrored(2 - 2 * middle), mirrored(3), k]
    own = len(dests) - 1

    def pack(hop, d):
        dest = dests[hop]
        for t in range(2):
            blocks = [raw[d, :, 0:2, j, t] for j in range(3)]
            packed[hop, t, d] = side_by_side(
                blocks,
                lambda j: lax.rem(slot * j + HALO + width - quarter * dest + width, width),
            )

    groups = ((0, 1), (2,), (3,))

    def exchange(hop, t_rel, group):
        t = lax.rem(c + t_rel, 2)
        part = pl.ds(groups[group][0], len(groups[group]))
        src = packed.at[hop, t, part]
        dst = landed.at[k, part, :, :, pl.ds(pl.multiple_of(8 * c, 8), 8)]
        if hop == own and t_rel == 0:
            return pltpu.make_async_copy(src, dst, a_recv.at[group])
        return pltpu.make_async_remote_copy(
            src_ref=src, dst_ref=dst,
            send_sem=a_send.at[hop // own], recv_sem=a_recv.at[group],
            device_id={"gz": dests[hop], "gy": t}, device_id_type=MESH_ID,
        )

    hops = list(range(len(dests)))

    def hand_out(group):
        members = groups[group]
        for d in members:
            loads[d].wait()
        for d in members:
            pack(0, d)
        if group == 0:
            pl.semaphore_wait(barrier, 4 + 2 * middle)

            @pl.when(middle == 1)
            def _():
                tell(near_sem, mirrored(0))
                tell(far_sem, mirrored(2))
        for hop in hops:
            if hop:
                for d in members:
                    pack(hop, d)
            if group == 0 and hop == 1:

                @pl.when(middle == 0)
                def _():
                    pl.semaphore_wait(near_sem, 1)

            if group == 0 and hop == 2:
                pl.semaphore_wait(far_sem, 1)

                @pl.when(middle == 1)
                def _():
                    tell(far_sem, mirrored(0))

                pl.semaphore_signal(
                    side_sem, inc=1, device_id={"ta": 1 - a}, device_id_type=MESH_ID
                )
            for t_rel in range(2):
                exchange(hop, t_rel, group).start()

    hand_out(0)
    hand_out(1)

    def arrived(group):
        part = pl.ds(groups[group][0], len(groups[group]))
        settle(landed.at[:, part], a_recv.at[group])

    def turn(value, lanes):
        lanes = lanes % width
        return pltpu.roll(value, lanes, 1) if lanes else value

    def by_slot(values):
        tile = values[-1]
        for g in reversed(range(len(values) - 1)):
            tile = jnp.where(lane < slot * (g + 1), values[g], tile)
        return tile

    places = [[(z, 0) for z in range(3)], [(z, 1) for z in range(3)], [(3, 0), (3, 1)]]

    def closed(read):
        rows = [[(read(0, r, j), read(1, r, j)) for j in range(3)] for r in range(2)]
        rows.append(third_row(rows[0], rows[1]))
        return rows

    def unpack(d):
        for tile in tiles:

            def entry(ri, r, j):
                return by_slot([
                    turn(landed[z, d, ri, r, pl.ds(h, 8, stride=2)], slot * (g - j))
                    for g, (z, h) in enumerate(places[tile])
                ])

            put(d, tile, closed(entry))

    def put(d, tile, mat):
        for r in range(3):
            for j in range(3):
                for ri in range(2):
                    state[d, ri, r, j, tile] = mat[r][j][ri]

    def get(read, rows=3):
        return [[(read(0, r, j), read(1, r, j)) for j in range(3)] for r in range(rows)]

    def down(value):
        return pltpu.roll(value, 7, 0)

    def up_row(value):
        return pltpu.roll(value, 1, 0)

    def shift_plus(read, nu, tile):
        if nu == 0:
            return turn(read(tile), -1)
        if nu == 1:
            if tile == 0:
                return read(1)
            if tile == 1:
                return down(read(0))
            return by_slot([turn(read(2), -slot), down(turn(read(2), slot))])
        if tile == 2:
            return by_slot([read(0), turn(read(1), slot)])
        inner = turn(read(tile), -slot)
        return jnp.where(lane < 2 * slot, inner, turn(read(2), slot * (2 - tile)))

    def shift_minus(read, nu, tile):
        if nu == 0:
            return turn(read(tile), 1)
        if nu == 1:
            if tile == 0:
                return up_row(read(1))
            if tile == 1:
                return read(0)
            return by_slot([up_row(turn(read(2), -slot)), turn(read(2), slot)])
        if tile == 2:
            return by_slot([turn(read(0), -2 * slot), turn(read(1), -slot)])
        return by_slot([turn(read(2), -slot * tile), turn(read(tile), slot)])

    def here(d, tile):
        return get(lambda ri, r, j: state[d, ri, r, j, tile])

    def plus(d, nu, tile):
        return get(
            lambda ri, r, j: shift_plus(lambda other: state[d, ri, r, j, other], nu, tile)
        )

    def keep(ref, entry, tile, mat):
        for r in range(2):
            for j in range(3):
                for ri in range(2):
                    ref[entry, ri, r, j, tile] = mat[r][j][ri]

    pairs = [(0, 1), (0, 2), (1, 2)]
    slot_of = {}
    for mu in range(3):
        for nu in range(3):
            if mu != nu:
                slot_of[mu, nu] = len(slot_of)

    def staples(chosen):
        for tile in tiles:
            for mu, nu in chosen:
                u_mu, u_nu = here(mu, tile), here(nu, tile)
                nu_ahead, mu_ahead = plus(nu, mu, tile), plus(mu, nu, tile)
                one = times(u_mu, nu_ahead)
                keep(lows, slot_of[mu, nu], tile, times(u_nu, one, lhs_dag=True, rows=2))
                keep(ups, slot_of[nu, mu], tile, times(one, mu_ahead, rhs_dag=True, rows=2))
                two = times(u_nu, mu_ahead)
                keep(lows, slot_of[nu, mu], tile, times(u_mu, two, lhs_dag=True, rows=2))
                keep(ups, slot_of[mu, nu], tile, times(two, nu_ahead, rhs_dag=True, rows=2))

    def mix(d, tile, entries, factor):
        def entry(ri, r, j):
            total = None
            for at, nu in entries:
                low = shift_minus(lambda other: lows[at, ri, r, j, other], nu, tile)
                part = ups[at, ri, r, j, tile] + low
                total = part if total is None else total + part
            return (1.0 - smear_weight) * state[d, ri, r, j, tile] + factor * total

        return project_rows(get(entry, rows=2))

    def update(chosen):
        for tile in tiles:
            for mu in chosen:
                entries = [(slot_of[mu, nu], nu) for nu in range(3) if nu != mu]
                put(mu, tile, mix(mu, tile, entries, smear_weight / 4.0))
    arrived(0)
    unpack(0)
    unpack(1)

    def sweep(index, carry):
        staples(pairs[0:1])

        @pl.when(index == 0)
        def _():
            arrived(1)
            hand_out(2)
            unpack(2)

        staples(pairs[1:3])
        update((0, 1, 2))
        return carry
    lax.fori_loop(0, ITERS - 1, sweep, 0)

    def next_copy(mu):
        return pltpu.make_async_remote_copy(
            src_ref=outgoing.at[mu - 1] if mu else state.at[0, :, pl.ds(0, 2)],
            dst_ref=ahead.at[mu - 1] if mu else ahead_x,
            send_sem=n_send.at[int(mu > 0)], recv_sem=n_recv.at[mu],
            device_id={"ta": lax.rem(a + c + n_ta - 1, n_ta), "gy": 1 - c},
            device_id_type=MESH_ID,
        )

    def send_next(mu):
        if mu:
            for ri in range(2):
                for r in range(2):
                    for j in range(3):
                        rest = state[mu, ri, r, j, 2]
                        for tile in range(2):
                            full = state[mu, ri, r, j, tile]
                            dense = turn(rest, 3 * quarter - HALO - slot * tile)
                            for g in reversed(range(3)):
                                dense = jnp.where(
                                    lane < quarter * (g + 1),
                                    turn(full, (quarter - slot) * g - HALO),
                                    dense,
                                )
                            outgoing[mu - 1, ri, r, j, tile] = dense
        next_copy(mu).start()

    def later_links(mu, tile):
        if mu == 0:
            return closed(lambda ri, r, j: ahead_x[ri, r, j, tile])

        def entry(ri, r, j):
            if tile < 2:
                dense = ahead[mu - 1, ri, r, j, tile]
                return by_slot([turn(dense, (slot - quarter) * g + HALO) for g in range(3)])
            return by_slot([
                turn(ahead[mu - 1, ri, r, j, half], slot * half + HALO - 3 * quarter)
                for half in range(2)
            ])

        return closed(entry)
    pl.semaphore_wait(side_sem, 1)
    staples(pairs[0:2])
    update((0,))
    send_next(0)
    staples(pairs[2:3])
    update((1,))
    send_next(1)
    update((2,))
    send_next(2)
    arrived(2)
    unpack(3)

    def time_firsts():
        for tile in tiles:
            for nu in range(3):
                u_nu = here(nu, tile)
                keep(ups, nu, tile, times(u_nu, plus(3, nu, tile), rows=2))
                keep(lows, nu, tile, times(u_nu, here(3, tile), lhs_dag=True, rows=2))

    def time_staples(nu):
        for tile in tiles:
            later = later_links(nu, tile)
            up = get(lambda ri, r, j: ups[nu, ri, r, j, tile], rows=2)
            keep(ups, nu, tile, times(up, later, rhs_dag=True, rows=2))
            low = get(lambda ri, r, j: lows[nu, ri, r, j, tile], rows=2)
            keep(lows, nu, tile, times(low, later, rows=2))

    def smooth(tile):
        return mix(3, tile, [(nu, nu) for nu in range(3)], smear_weight / 6.0)

    me = n_gy * a + c

    def deliver(z, mats):
        for r in range(2):
            for j in range(3):
                dense = None
                for p in reversed(range(4)):
                    mat, g = mats[p // 2]
                    piece = turn(mat[r][j][p % 2], quarter * p - slot * g - HALO)
                    dense = (
                        piece if dense is None
                        else jnp.where(lane < quarter * (p + 1), piece, dense)
                    )
                smooth_out[z, r, j] = dense

        @pl.when(me == z)
        def _():
            smooth_in[z] = smooth_out[z]

        @pl.when(me != z)
        def _():
            pltpu.make_async_remote_copy(
                src_ref=smooth_out.at[z], dst_ref=smooth_in.at[me],
                send_sem=w_send.at[0], recv_sem=w_recv.at[0],
                device_id={"ta": z // n_gy, "gy": z % n_gy}, device_id_type=MESH_ID,
            ).start()
    time_firsts()
    for nu in range(3):
        next_copy(nu).wait_recv()
        time_staples(nu)
    last = smooth(2)
    deliver(3, [(last, 0), (last, 1)])
    even, odd = smooth(0), smooth(1)
    for z in range(3):
        deliver(z, [(even, z), (odd, z)])
    settle(smooth_out.at[pl.ds(1, n_ta * n_gy - 1)], w_recv.at[0])

    def time_link(t):
        rows = []
        for r in range(2):
            tiles = [smooth_in[t, r, j] for j in range(3)]
            rows.append([(tile, pltpu.roll(tile, width - quarter, 1)) for tile in tiles])
        rows.append(third_row(rows[0], rows[1]))
        return rows
    early = times(time_link(0), time_link(1))
    late = times(time_link(2), time_link(3))
    re_terms, im_terms = [], []
    for i in range(3):
        for j in range(3):
            p_re, p_im = early[i][j]
            q_re, q_im = late[j][i]
            re_terms += [(1, p_re * q_re), (-1, p_im * q_im)]
            im_terms += [(1, p_re * q_im), (1, p_im * q_re)]
    trace_re = signed_sum(re_terms) / 3.0
    trace_im = signed_sum(im_terms) / 3.0
    trace = jnp.where(lax.rem(lane, 2 * quarter) < quarter, trace_re, turn(trace_im, quarter))
    trace_out[...] = trace
    sums = jnp.sum(trace, axis=0, keepdims=True)
    row_out[0] = sums
    keeps_one = k == me
    for ta in range(n_ta):
        for gy in range(n_gy):
            is_self = keeps_one & (a == ta) & (c == gy)
            remote = pltpu.make_async_remote_copy(
                src_ref=trace_out, dst_ref=traces.at[k],
                send_sem=t_send.at[0], recv_sem=t_recv.at[0],
                device_id={"ta": ta, "gz": me, "gy": gy}, device_id_type=MESH_ID,
            )
            local = pltpu.make_async_copy(trace_out, traces.at[k], t_recv.at[0])
            pl.when(jnp.logical_not(is_self))(remote.start)
            pl.when(is_self)(local.start)
    for step in range(1, n_group):
        da, dk, dc = step // (n_gz * n_gy), step // n_gy % n_gz, step % n_gy
        device = {
            "ta": lax.rem(a + da, n_ta),
            "gz": lax.rem(k + dk, n_gz),
            "gy": lax.rem(c + dc, n_gy),
        }
        copy = pltpu.make_async_remote_copy(
            src_ref=row_out, dst_ref=rows_in.at[pl.ds(step, 1)],
            send_sem=r_send.at[0], recv_sem=r_recv.at[0],
            device_id=device, device_id_type=MESH_ID,
        )
        copy.start()

    settle(traces, t_recv.at[0])
    for ri in range(2):
        for h in range(2):
            out = None
            for z in reversed(range(n_gz)):
                piece = turn(traces[z], quarter * (z - 2 * h - ri))
                out = piece if out is None else jnp.where(lane < quarter * (z + 1), piece, out)
            half = pltpu.roll(out, lax.rem(8 - 4 * c, 8), 0)
            poly_ref[ri, pl.ds(h, 4, stride=2)] = half[0:4]
    total = sums
    settle(rows_in.at[pl.ds(1, n_group - 1)], r_recv.at[0])
    for step in range(1, n_group):
        total = total + rows_in[step]
    total_ref[...] = total
    settle(packed.at[pl.ds(0, own)], a_send.at[0])
    settle(packed.at[own, 0], a_send.at[1])
    settle(ahead_x, n_send.at[0])
    settle(outgoing, n_send.at[1])
    settle(smooth_out.at[pl.ds(1, n_ta * n_gy - 1)], w_send.at[0])

    @pl.when(keeps_one)
    def _():
        settle(traces.at[pl.ds(1, n_gz - 1)], t_send.at[0])

    @pl.when(jnp.logical_not(keeps_one))
    def _():
        settle(traces, t_send.at[0])

    settle(rows_in.at[pl.ds(1, n_group - 1)], r_send.at[0])
def hand_over(quarter, sites, poly_in, total_in, poly_ref, mean_ref):
    poly_ref[...] = poly_in[...]
    total = total_in[...]
    place = lax.broadcasted_iota(jnp.int32, total.shape, 1)
    real = lax.rem(place, 2 * quarter) < quarter
    mean_ref[0] = jnp.sum(jnp.where(real, total, 0.0)) / sites
    mean_ref[1] = jnp.sum(jnp.where(real, 0.0, total)) / sites


def fused_on_device(mesh_shape, spatial_links, time_links):
    n_ta, n_gz, n_gy = (mesh_shape[name] for name in ("ta", "gz", "gy"))
    width = spatial_links.shape[-1]
    n_group = n_ta * n_gz * n_gy
    sites = float(n_gz * n_gy * 8 * width)
    spatial = spatial_links.reshape(3, 2, 3, 3, 2, 8, width)
    times_in = time_links.reshape(2, 3, 3, 2, 8, width)
    vm = lambda *shape: pltpu.VMEM(shape + (8, width), jnp.float32)
    dma = pltpu.SemaphoreType.DMA
    poly, total = pl.pallas_call(
        partial(fused_kernel, (n_ta, n_gz, n_gy, width, sites)),
        out_shape=(
            pltpu.VMEM((2, 8, width), jnp.float32),
            pltpu.VMEM((1, width), jnp.float32),
        ),
        in_specs=[pl.BlockSpec(memory_space=pl.ANY)] * 2,
        out_specs=(pl.BlockSpec(memory_space=pltpu.VMEM),) * 2,
        scratch_shapes=[
            vm(4, 2, 3, 3, 2),
            vm(n_gz, 2, 4, 2, 2),
            pltpu.VMEM((n_gz, 4, 2, 2, 2 * 8, width), jnp.float32),
            vm(4, 2, 3, 3, 3),
            vm(6, 2, 2, 3, 3),
            vm(6, 2, 2, 3, 3),
            vm(2, 2, 2, 3, 2),
            vm(2, 2, 2, 3, 2),
            vm(2, 2, 3, 3),
            vm(4, 2, 3),
            vm(4, 2, 3),
            vm(),
            vm(n_gz),
            pltpu.VMEM((1, 1, width), jnp.float32),
            pltpu.VMEM((n_group, 1, width), jnp.float32),
            dma((4,)),
            dma((2,)), dma((3,)), dma((2,)), dma((3,)),
            *[dma((1,))] * 6,
            *[pltpu.SemaphoreType.REGULAR] * 3,
        ],
        compiler_params=pltpu.CompilerParams(collective_id=0, has_side_effects=True),
    )(spatial, times_in)
    poly, mean = pl.pallas_call(
        partial(hand_over, width // n_gz, sites),
        out_shape=(
            jax.ShapeDtypeStruct((2, 8, width), jnp.float32),
            jax.ShapeDtypeStruct((2,), jnp.float32),
        ),
        in_specs=[pl.BlockSpec(memory_space=pltpu.VMEM)] * 2,
        out_specs=(
            pl.BlockSpec(memory_space=pltpu.VMEM),
            pl.BlockSpec(memory_space=pltpu.SMEM),
        ),
    )(*[pltpu.with_memory_space_constraint(x, pltpu.VMEM) for x in (poly, total)])
    return poly.reshape(2, 1, 8, width), mean


def fits_fused(mesh_shape, shape):
    width = shape[-1]
    n_ta, n_gz, n_gy = (mesh_shape[name] for name in ("ta", "gz", "gy"))
    per = shape[4] // n_ta, shape[5] // n_gz, shape[6] // n_gy
    window = width // n_gz + 2 * HALO
    return (
        per == (2, 1, 8) and n_ta == 2 and n_gz == 4 and n_gy == 2
        and width == 128 and ITERS >= 2 and window <= width // 3
    )


def solution(mesh):
    placed = (
        P("cfg", None, None, None, "ta", "gz", "gy", None),
        P("cfg", None, None, "ta", "gz", "gy", None),
    )

    def run(spatial_links, time_links):
        fused = fits_fused(mesh.shape, spatial_links.shape)
        body = partial(fused_on_device, dict(mesh.shape)) if fused else on_device
        return jax.shard_map(
            body,
            mesh=mesh,
            in_specs=placed,
            out_specs=(P("cfg", "gz", "gy", None), P("cfg")),
            check_vma=False,
        )(spatial_links, time_links)

    return run
```

```python
from functools import partial

import jax
import jax.numpy as jnp
from jax import lax
from jax.experimental import pallas as pl
from jax.experimental.pallas import tpu as pltpu
from jax.sharding import PartitionSpec as P

ITERS = 3


smear_weight = 0.5
norm_floor = 0.25
unit_steps = ((1, 0, 0), (0, 1, 0), (0, 0, 1))


def padded_2(cells, sides, width):
    for axis, dim in sides:
        count = lax.axis_size(axis)
        head = lax.slice_in_dim(cells, 0, width, axis=dim)
        tail = lax.slice_in_dim(cells, cells.shape[dim] - width, cells.shape[dim], axis=dim)
        cells = jnp.concatenate(
            [
                lax.ppermute(tail, axis, [(i, (i + 1) % count) for i in range(count)]),
                cells,
                lax.ppermute(head, axis, [((i + 1) % count, i) for i in range(count)]),
            ],
            axis=dim,
        )
    return cells


def shifted(shard, axis, by):
    devices = lax.axis_size(axis)
    return lax.ppermute(shard, axis, [(i, (i + by) % devices) for i in range(devices)])


def mat_product(lhs_mat, rhs_mat):
    lhs_re = lhs_mat[0][:, :, None]
    lhs_im = lhs_mat[1][:, :, None]
    rhs_re = rhs_mat[0][None]
    rhs_im = rhs_mat[1][None]
    real_part = jnp.sum(lhs_re * rhs_re - lhs_im * rhs_im, axis=1)
    imag_part = jnp.sum(lhs_re * rhs_im + lhs_im * rhs_re, axis=1)
    return jnp.stack([real_part, imag_part])


def dagger(matrix):
    return jnp.stack([jnp.swapaxes(matrix[0], 0, 1), -jnp.swapaxes(matrix[1], 0, 1)])


def normalize_row(row_vec):
    weight = jnp.sum(row_vec[0] * row_vec[0] + row_vec[1] * row_vec[1], axis=0)
    return row_vec / jnp.sqrt(jnp.maximum(weight, norm_floor))


def project(matrix):
    first = normalize_row(matrix[:, 0])
    second_raw = matrix[:, 1]
    inner_re = jnp.sum(first[0] * second_raw[0] + first[1] * second_raw[1], axis=0)
    inner_im = jnp.sum(first[0] * second_raw[1] - first[1] * second_raw[0], axis=0)
    ortho = jnp.stack(
        [
            second_raw[0] - (inner_re * first[0] - inner_im * first[1]),
            second_raw[1] - (inner_re * first[1] + inner_im * first[0]),
        ]
    )
    second = normalize_row(ortho)
    first_one = jnp.roll(first, -1, axis=1)
    first_two = jnp.roll(first, -2, axis=1)
    second_one = jnp.roll(second, -1, axis=1)
    second_two = jnp.roll(second, -2, axis=1)
    cross_re = (
        first_one[0] * second_two[0]
        - first_one[1] * second_two[1]
        - (first_two[0] * second_one[0] - first_two[1] * second_one[1])
    )
    cross_im = (
        first_one[0] * second_two[1]
        + first_one[1] * second_two[0]
        - (first_two[0] * second_one[1] + first_two[1] * second_one[0])
    )
    third = jnp.stack([cross_re, -cross_im])
    return jnp.stack([first, second, third], axis=1)


def moved(offset, unit_vec, factor):
    return (
        offset[0] + factor * unit_vec[0],
        offset[1] + factor * unit_vec[1],
        offset[2] + factor * unit_vec[2],
    )


def smear_spatial(neighbour):
    anchor = (0, 0, 0)
    result = []
    for mu_dir in range(3):
        staples = None
        for nu_dir in range(3):
            if nu_dir == mu_dir:
                continue
            forward = unit_steps[nu_dir]
            sideways = unit_steps[mu_dir]
            upper_staple = mat_product(
                mat_product(neighbour(nu_dir, anchor), neighbour(mu_dir, forward)),
                dagger(neighbour(nu_dir, sideways)),
            )
            back_offset = moved(anchor, forward, -1)
            lower_staple = mat_product(
                mat_product(dagger(neighbour(nu_dir, back_offset)), neighbour(mu_dir, back_offset)),
                neighbour(nu_dir, moved(back_offset, sideways, 1)),
            )
            if staples is None:
                staples = upper_staple + lower_staple
            else:
                staples = staples + upper_staple + lower_staple
        mixed_link = (1.0 - smear_weight) * neighbour(mu_dir, anchor) + smear_weight / 4.0 * staples
        result.append(project(mixed_link))
    return jnp.stack(result)


def window_cut(field, offset):
    z_inner = field.shape[-3] - 2
    y_inner = field.shape[-2] - 2
    piece = field[
        ..., 1 + offset[2] : 1 + offset[2] + z_inner, 1 + offset[1] : 1 + offset[1] + y_inner, :
    ]
    return jnp.roll(piece, -offset[0], axis=-1)


def padded_neighbour(padded, direction, offset):
    return window_cut(padded[direction], offset)


def smooth_by_products(link_field, time_links, extended, depth):
    later_links = extended[0:3, :, :, :, 1 : depth + 1]
    lowers = [
        mat_product(mat_product(dagger(link_field[nu_dir]), time_links), later_links[nu_dir])
        for nu_dir in range(3)
    ]
    carried = jnp.stack([time_links] + lowers)
    padded = padded_2(carried, (("gz", 5), ("gy", 6)), 1)
    anchor = (0, 0, 0)
    staples = None
    for nu_dir in range(3):
        forward = unit_steps[nu_dir]
        upper_staple = mat_product(
            mat_product(link_field[nu_dir], window_cut(padded[0], forward)),
            dagger(later_links[nu_dir]),
        )
        lower_staple = window_cut(padded[1 + nu_dir], moved(anchor, forward, -1))
        if staples is None:
            staples = upper_staple + lower_staple
        else:
            staples = staples + upper_staple + lower_staple
    mixed_link = (1.0 - smear_weight) * time_links + smear_weight / 6.0 * staples
    return project(mixed_link)


def on_device(spatial_links, time_links):
    link_field = spatial_links
    for sweep_index in range(ITERS):
        padded = padded_2(link_field, (("gz", 5), ("gy", 6)), 1)
        link_field = smear_spatial(partial(padded_neighbour, padded))
    stacked = jnp.concatenate([link_field, time_links[None]], axis=0)
    ahead_slice = shifted(stacked[:, :, :, :, 0:1], "ta", -1)
    extended = jnp.concatenate([stacked, ahead_slice], axis=4)
    depth = time_links.shape[3]
    smoothed = smooth_by_products(link_field, time_links, extended, depth)
    block_prod = smoothed[:, :, :, 0]
    block_prod = mat_product(block_prod, smoothed[:, :, :, 1])
    pieces = lax.all_gather(block_prod[None], "ta", axis=0, tiled=True)

    def advance(index, carry):
        return mat_product(carry, pieces[index])

    whole_prod = lax.fori_loop(1, pieces.shape[0], advance, pieces[0])
    polyakov = (
        jnp.stack(
            [
                whole_prod[0, 0, 0] + whole_prod[0, 1, 1] + whole_prod[0, 2, 2],
                whole_prod[1, 0, 0] + whole_prod[1, 1, 1] + whole_prod[1, 2, 2],
            ]
        )
        / 3.0
    )
    local_sums = jnp.sum(polyakov, axis=(1, 2, 3))
    totals = lax.psum(local_sums, ("gz", "gy"))
    site_count = (
        polyakov.shape[1]
        * polyakov.shape[2]
        * polyakov.shape[3]
        * lax.axis_size("gz")
        * lax.axis_size("gy")
    )
    site_mean = totals / site_count
    return (polyakov, site_mean)


HALO = ITERS + 1
MESH_ID = pl.DeviceIdType.MESH


def signed_sum(terms):
    total = None
    for sign, value in terms:
        if total is None:
            total = value if sign > 0 else -value
        elif sign > 0:
            total = total + value
        else:
            total = total - value
    return total


def times(lhs, rhs, lhs_dag=False, rhs_dag=False, rows=3):
    out = []
    for i in range(rows):
        line = []
        for j in range(3):
            real_terms, imag_terms = [], []
            for k in range(3):
                a_re, a_im = lhs[k][i] if lhs_dag else lhs[i][k]
                b_re, b_im = rhs[j][k] if rhs_dag else rhs[k][j]
                sa = -1 if lhs_dag else 1
                sb = -1 if rhs_dag else 1
                real_terms += [(1, a_re * b_re), (-sa * sb, a_im * b_im)]
                if sb > 0:
                    imag_terms += [(1, a_re * b_im), (sa, a_im * b_re)]
                else:
                    imag_terms += [(1, a_im * b_re), (-1, a_re * b_im)]
            line.append((signed_sum(real_terms), signed_sum(imag_terms)))
        out.append(line)
    return out


def unit_row(row):
    weight = signed_sum([(1, p * p) for pair in row for p in pair])
    scale = lax.rsqrt(jnp.maximum(weight, norm_floor))
    return [(re * scale, im * scale) for re, im in row]


def third_row(first, second):
    out = []
    for j in range(3):
        (a_re, a_im), (b_re, b_im) = first[(j + 1) % 3], second[(j + 2) % 3]
        (c_re, c_im), (d_re, d_im) = first[(j + 2) % 3], second[(j + 1) % 3]
        re = a_re * b_re - a_im * b_im - (c_re * d_re - c_im * d_im)
        im = c_re * d_im + c_im * d_re - (a_re * b_im + a_im * b_re)
        out.append((re, im))
    return out


def project_rows(rows):
    first = unit_row(rows[0])
    inner_re = signed_sum(
        [(1, p) for (a, b), (c, d) in zip(first, rows[1]) for p in (a * c, b * d)]
    )
    inner_im = None
    for (a, b), (c, d) in zip(first, rows[1]):
        part = a * d - b * c
        inner_im = part if inner_im is None else inner_im + part
    ortho = [
        (c - (inner_re * a - inner_im * b), d - (inner_re * b + inner_im * a))
        for (a, b), (c, d) in zip(first, rows[1])
    ]
    second = unit_row(ortho)
    return [first, second, third_row(first, second)]


def fused_kernel(
    dims, sl_hbm, tl_hbm, poly_ref, total_ref,
    raw, packed, landed, state, ups, lows, outgoing, outgoing_x, ahead, ahead_x, smooth_out, smooth_in,
    trace_out, traces, row_out, rows_in,
    load_sem, a_send, a_recv, n_send, n_recv, w_send, w_recv,
    t_send, t_recv, r_send, r_recv, near_sem, far_sem, side_sem,
):
    n_ta, n_gz, n_gy, width, sites = dims
    quarter = width // n_gz
    slot = width // 3
    tiles = range(3)
    a, k, c = lax.axis_index("ta"), lax.axis_index("gz"), lax.axis_index("gy")
    lane = lax.broadcasted_iota(jnp.int32, (8, width), 1)
    n_group = n_ta * n_gz * n_gy
    middle = lax.rem((k + 1) // 2, 2)
    far_half = k // 2

    def mirrored(z):
        return z + far_half * (n_gz - 1 - 2 * z)

    barrier = pltpu.get_barrier_semaphore()

    def greet(device):
        pl.semaphore_signal(barrier, inc=1, device_id=device, device_id_type=MESH_ID)

    def tell(sem, z):
        pl.semaphore_signal(sem, inc=1, device_id={"gz": z}, device_id_type=MESH_ID)

    greet({"gy": 1 - c})
    greet({"ta": 1 - a})
    for core in range(n_gy):
        greet({"gz": mirrored(middle + 1), "gy": core})

    @pl.when(middle == 1)
    def _():
        for core in range(n_gy):
            greet({"gz": mirrored(0), "gy": core})

    loads = [pltpu.make_async_copy(sl_hbm.at[d], raw.at[d], load_sem.at[d]) for d in range(3)]
    loads.append(pltpu.make_async_copy(tl_hbm, raw.at[3], load_sem.at[3]))
    for copy in loads:
        copy.start()
    def settle(ref, sem):
        pltpu.make_async_copy(ref, ref, sem).wait()

    wide = lax.broadcasted_iota(jnp.int32, (32, width), 1)

    def side_by_side(blocks, shift_of):
        tile = None
        for j in range(3):
            moved_block = pltpu.roll(blocks[j].reshape(32, width), shift_of(j), 1)
            tile = moved_block if j == 0 else jnp.where(wide >= slot * j, moved_block, tile)
        return tile.reshape(2, 2, 8, width)

    first_dests = [mirrored(middle + 1), mirrored(2 - 2 * middle), mirrored(3), k]
    own = n_gz - 1
    later_dests = [own - i - (own - i <= k).astype(jnp.int32) for i in range(own)] + [k]

    def pack(hop, d):
        dest = (later_dests if d > 1 else first_dests)[hop]
        for t in range(2):
            blocks = [raw[d, :, 0:2, j, t] for j in range(3)]
            packed[hop, t, d] = side_by_side(
                blocks,
                lambda j: lax.rem(slot * j + HALO + width - quarter * dest + width, width),
            )

    groups = ((0, 1), (2,), (3,))

    def exchange(hop, t_rel, group):
        t = lax.rem(c + t_rel, 2)
        part = pl.ds(groups[group][0], len(groups[group]))
        src = packed.at[hop, t, part]
        dst = landed.at[k, part, :, :, pl.ds(pl.multiple_of(8 * c, 8), 8)]
        if hop == own and t_rel == 0:
            return pltpu.make_async_copy(src, dst, a_recv.at[group])
        return pltpu.make_async_remote_copy(
            src_ref=src, dst_ref=dst,
            send_sem=a_send.at[hop // own], recv_sem=a_recv.at[group],
            device_id={"gz": (later_dests if group else first_dests)[hop], "gy": t}, device_id_type=MESH_ID,
        )

    hops = list(range(n_gz))

    def hand_out(group):
        members = groups[group]
        for d in members:
            loads[d].wait()
        for d in members:
            pack(0, d)
        if group == 0:
            pl.semaphore_wait(barrier, 4 + 2 * middle)

            @pl.when(middle == 1)
            def _():
                tell(near_sem, mirrored(0))
                tell(far_sem, mirrored(2))
        for hop in hops:
            if hop:
                for d in members:
                    pack(hop, d)
            if group == 0 and hop == 1:

                @pl.when(middle == 0)
                def _():
                    pl.semaphore_wait(near_sem, 1)

            if group == 0 and hop == 2:
                pl.semaphore_wait(far_sem, 1)

                @pl.when(middle == 1)
                def _():
                    tell(far_sem, mirrored(0))

                pl.semaphore_signal(
                    side_sem, inc=1, device_id={"ta": 1 - a}, device_id_type=MESH_ID
                )
            for t_rel in range(2):
                exchange(hop, t_rel, group).start()

    hand_out(0)
    hand_out(1)

    def arrived(group):
        part = pl.ds(groups[group][0], len(groups[group]))
        settle(landed.at[:, part], a_recv.at[group])

    def turn(value, lanes):
        lanes = lanes % width
        return pltpu.roll(value, lanes, 1) if lanes else value

    def by_slot(values):
        tile = values[-1]
        for g in reversed(range(len(values) - 1)):
            tile = jnp.where(lane < slot * (g + 1), values[g], tile)
        return tile

    places = [[(z, 0) for z in range(3)], [(z, 1) for z in range(3)], [(3, 0), (3, 1)]]

    def closed(read):
        rows = [[(read(0, r, j), read(1, r, j)) for j in range(3)] for r in range(2)]
        rows.append(third_row(rows[0], rows[1]))
        return rows

    def unpack(d):
        for tile in tiles:

            def entry(ri, r, j):
                return by_slot([
                    turn(landed[z, d, ri, r, pl.ds(h, 8, stride=2)], slot * (g - j))
                    for g, (z, h) in enumerate(places[tile])
                ])

            put(d, tile, closed(entry))

    def put(d, tile, mat):
        for r in range(3):
            for j in range(3):
                for ri in range(2):
                    state[d, ri, r, j, tile] = mat[r][j][ri]

    def get(read, rows=3):
        return [[(read(0, r, j), read(1, r, j)) for j in range(3)] for r in range(rows)]

    def down(value):
        return pltpu.roll(value, 7, 0)

    def up_row(value):
        return pltpu.roll(value, 1, 0)

    def shift_plus(read, nu, tile):
        if nu == 0:
            return turn(read(tile), -1)
        if nu == 1:
            if tile == 0:
                return read(1)
            if tile == 1:
                return down(read(0))
            return by_slot([turn(read(2), -slot), down(turn(read(2), slot))])
        if tile == 2:
            return by_slot([read(0), turn(read(1), slot)])
        inner = turn(read(tile), -slot)
        return jnp.where(lane < 2 * slot, inner, turn(read(2), slot * (2 - tile)))

    def shift_minus(read, nu, tile):
        if nu == 0:
            return turn(read(tile), 1)
        if nu == 1:
            if tile == 0:
                return up_row(read(1))
            if tile == 1:
                return read(0)
            return by_slot([up_row(turn(read(2), -slot)), turn(read(2), slot)])
        if tile == 2:
            return by_slot([turn(read(0), -2 * slot), turn(read(1), -slot)])
        return by_slot([turn(read(2), -slot * tile), turn(read(tile), slot)])

    def here(d, tile):
        return get(lambda ri, r, j: state[d, ri, r, j, tile])

    def plus(d, nu, tile):
        return get(
            lambda ri, r, j: shift_plus(lambda other: state[d, ri, r, j, other], nu, tile)
        )

    def keep(ref, entry, tile, mat):
        for r in range(2):
            for j in range(3):
                for ri in range(2):
                    ref[entry, ri, r, j, tile] = mat[r][j][ri]

    pairs = [(0, 1), (0, 2), (1, 2)]
    slot_of = {}
    for mu in range(3):
        for nu in range(3):
            if mu != nu:
                slot_of[mu, nu] = len(slot_of)

    def staples(chosen):
        for tile in tiles:
            for mu, nu in chosen:
                u_mu, u_nu = here(mu, tile), here(nu, tile)
                nu_ahead, mu_ahead = plus(nu, mu, tile), plus(mu, nu, tile)
                one = times(u_mu, nu_ahead)
                keep(lows, slot_of[mu, nu], tile, times(u_nu, one, lhs_dag=True, rows=2))
                keep(ups, slot_of[nu, mu], tile, times(one, mu_ahead, rhs_dag=True, rows=2))
                two = times(u_nu, mu_ahead)
                keep(lows, slot_of[nu, mu], tile, times(u_mu, two, lhs_dag=True, rows=2))
                keep(ups, slot_of[mu, nu], tile, times(two, nu_ahead, rhs_dag=True, rows=2))

    def mix(d, tile, entries, factor):
        def entry(ri, r, j):
            total = None
            for at, nu in entries:
                low = shift_minus(lambda other: lows[at, ri, r, j, other], nu, tile)
                part = ups[at, ri, r, j, tile] + low
                total = part if total is None else total + part
            return (1.0 - smear_weight) * state[d, ri, r, j, tile] + factor * total

        return project_rows(get(entry, rows=2))

    def update(chosen):
        for tile in tiles:
            for mu in chosen:
                entries = [(slot_of[mu, nu], nu) for nu in range(3) if nu != mu]
                put(mu, tile, mix(mu, tile, entries, smear_weight / 4.0))
    arrived(0)
    unpack(0)
    unpack(1)

    def sweep(index, carry):
        staples(pairs[0:1])

        @pl.when(index == 0)
        def _():
            arrived(1)
            hand_out(2)
            unpack(2)

        staples(pairs[1:3])
        update((0, 1, 2))
        return carry
    lax.fori_loop(0, ITERS - 1, sweep, 0)

    comps = [(ri, r, j) for ri in range(2) for r in range(2) for j in range(3)]
    n_dense = 2 * len(comps)
    in_slot = lax.rem(lane, slot)

    def next_copy(mu):
        return pltpu.make_async_remote_copy(
            src_ref=outgoing.at[mu - 1] if mu else outgoing_x,
            dst_ref=ahead.at[mu - 1] if mu else ahead_x,
            send_sem=n_send.at[int(mu > 0)], recv_sem=n_recv.at[mu],
            device_id={"ta": lax.rem(a + c + n_ta - 1, n_ta), "gy": 1 - c},
            device_id_type=MESH_ID,
        )

    def send_next(mu):
        out = outgoing.at[mu - 1] if mu else outgoing_x
        for q, (ri, r, j) in enumerate(comps):
            rest = state[mu, ri, r, j, 2]
            for tile in range(2):
                full = state[mu, ri, r, j, tile]
                dense = turn(rest, 3 * quarter - HALO - slot * tile)
                for g in reversed(range(3)):
                    dense = jnp.where(
                        lane < quarter * (g + 1),
                        turn(full, (quarter - slot) * g - HALO),
                        dense,
                    )
                out[2 * q + tile] = dense
        if mu == 0:
            for tile in tiles:
                edge = None
                for q, (ri, r, j) in enumerate(comps):
                    piece = turn(state[mu, ri, r, j, tile], q + 1 - HALO)
                    edge = piece if edge is None else jnp.where(in_slot == q, piece, edge)
                out[n_dense + tile] = edge
        next_copy(mu).start()

    def later_links(mu, tile):
        source = ahead.at[mu - 1] if mu else ahead_x

        def entry(ri, r, j):
            q = comps.index((ri, r, j))
            if tile < 2:
                dense = source[2 * q + tile]
                value = by_slot([turn(dense, (slot - quarter) * g + HALO) for g in range(3)])
            else:
                value = by_slot([
                    turn(source[2 * q + half], slot * half + HALO - 3 * quarter)
                    for half in range(2)
                ])
            if mu == 0:
                edge = turn(source[n_dense + tile], HALO - 1 - q)
                value = jnp.where(in_slot == HALO - 1, edge, value)
            return value

        return closed(entry)
    pl.semaphore_wait(side_sem, 1)
    staples(pairs[0:2])
    update((0,))
    send_next(0)
    staples(pairs[2:3])
    update((1,))
    send_next(1)
    update((2,))
    send_next(2)
    arrived(2)
    unpack(3)

    def time_firsts():
        for tile in tiles:
            for nu in range(3):
                u_nu = here(nu, tile)
                keep(ups, nu, tile, times(u_nu, plus(3, nu, tile), rows=2))
                keep(lows, nu, tile, times(u_nu, here(3, tile), lhs_dag=True, rows=2))

    def time_staples(nu):
        for tile in tiles:
            later = later_links(nu, tile)
            up = get(lambda ri, r, j: ups[nu, ri, r, j, tile], rows=2)
            keep(ups, nu, tile, times(up, later, rhs_dag=True, rows=2))
            low = get(lambda ri, r, j: lows[nu, ri, r, j, tile], rows=2)
            keep(lows, nu, tile, times(low, later, rows=2))

    def smooth(tile):
        return mix(3, tile, [(nu, nu) for nu in range(3)], smear_weight / 6.0)

    me = n_gy * a + c

    def lay_out(z, mats):
        for r in range(2):
            for j in range(3):
                dense = None
                for p in reversed(range(4)):
                    mat, g = mats[p // 2]
                    piece = turn(mat[r][j][p % 2], quarter * p - slot * g - HALO)
                    dense = (
                        piece if dense is None
                        else jnp.where(lane < quarter * (p + 1), piece, dense)
                    )
                smooth_out[z, r, j] = dense

    def deliver(z):
        @pl.when(me == z)
        def _():
            smooth_in[z] = smooth_out[z]

        @pl.when(me != z)
        def _():
            pltpu.make_async_remote_copy(
                src_ref=smooth_out.at[z], dst_ref=smooth_in.at[me],
                send_sem=w_send.at[0], recv_sem=w_recv.at[0],
                device_id={"ta": z // n_gy, "gy": z % n_gy}, device_id_type=MESH_ID,
            ).start()
    time_firsts()
    for nu in range(3):
        next_copy(nu).wait_recv()
        time_staples(nu)
    mats = [smooth(tile) for tile in tiles]
    for z in range(n_gz):
        lay_out(z, [(mats[0], z), (mats[1], z)] if z < 3 else [(mats[2], 0), (mats[2], 1)])
    for z in range(n_gz):
        deliver(z)
    settle(smooth_out.at[pl.ds(1, n_ta * n_gy - 1)], w_recv.at[0])

    def time_link(t):
        rows = []
        for r in range(2):
            tiles = [smooth_in[t, r, j] for j in range(3)]
            rows.append([(tile, pltpu.roll(tile, width - quarter, 1)) for tile in tiles])
        rows.append(third_row(rows[0], rows[1]))
        return rows
    early = times(time_link(0), time_link(1))
    late = times(time_link(2), time_link(3))
    re_terms, im_terms = [], []
    for i in range(3):
        for j in range(3):
            p_re, p_im = early[i][j]
            q_re, q_im = late[j][i]
            re_terms += [(1, p_re * q_re), (-1, p_im * q_im)]
            im_terms += [(1, p_re * q_im), (1, p_im * q_re)]
    trace_re = signed_sum(re_terms) / 3.0
    trace_im = signed_sum(im_terms) / 3.0
    trace = jnp.where(lax.rem(lane, 2 * quarter) < quarter, trace_re, turn(trace_im, quarter))
    trace_out[...] = trace
    sums = jnp.sum(trace, axis=0, keepdims=True)
    row_out[0] = sums
    for step in range(1, n_group):
        da, dk, dc = step // (n_gz * n_gy), step // n_gy % n_gz, step % n_gy
        device = {
            "ta": lax.rem(a + da, n_ta),
            "gz": lax.rem(k + dk, n_gz),
            "gy": lax.rem(c + dc, n_gy),
        }
        copy = pltpu.make_async_remote_copy(
            src_ref=row_out, dst_ref=rows_in.at[pl.ds(step, 1)],
            send_sem=r_send.at[0], recv_sem=r_recv.at[0],
            device_id=device, device_id_type=MESH_ID,
        )
        copy.start()
    keeps_one = k == me
    for ta in range(n_ta):
        for gy in range(n_gy):
            is_self = keeps_one & (a == ta) & (c == gy)
            remote = pltpu.make_async_remote_copy(
                src_ref=trace_out, dst_ref=traces.at[k],
                send_sem=t_send.at[0], recv_sem=t_recv.at[0],
                device_id={"ta": ta, "gz": me, "gy": gy}, device_id_type=MESH_ID,
            )
            local = pltpu.make_async_copy(trace_out, traces.at[k], t_recv.at[0])
            pl.when(jnp.logical_not(is_self))(remote.start)
            pl.when(is_self)(local.start)

    settle(traces, t_recv.at[0])
    for ri in range(2):
        for h in range(2):
            out = None
            for z in reversed(range(n_gz)):
                piece = turn(traces[z], quarter * (z - 2 * h - ri))
                out = piece if out is None else jnp.where(lane < quarter * (z + 1), piece, out)
            half = pltpu.roll(out, lax.rem(8 - 4 * c, 8), 0)
            poly_ref[ri, pl.ds(h, 4, stride=2)] = half[0:4]
    total = sums
    settle(rows_in.at[pl.ds(1, n_group - 1)], r_recv.at[0])
    for step in range(1, n_group):
        total = total + rows_in[step]
    total_ref[...] = total
    settle(packed.at[pl.ds(0, own)], a_send.at[0])
    settle(packed.at[own, 0], a_send.at[1])
    settle(ahead_x, n_send.at[0])
    settle(outgoing, n_send.at[1])
    settle(smooth_out.at[pl.ds(1, n_ta * n_gy - 1)], w_send.at[0])

    @pl.when(keeps_one)
    def _():
        settle(traces.at[pl.ds(1, n_gz - 1)], t_send.at[0])

    @pl.when(jnp.logical_not(keeps_one))
    def _():
        settle(traces, t_send.at[0])

    settle(rows_in.at[pl.ds(1, n_group - 1)], r_send.at[0])
def hand_over(quarter, sites, poly_in, total_in, poly_ref, mean_ref):
    poly_ref[...] = poly_in[...]
    total = total_in[...]
    place = lax.broadcasted_iota(jnp.int32, total.shape, 1)
    real = lax.rem(place, 2 * quarter) < quarter
    mean_ref[0] = jnp.sum(jnp.where(real, total, 0.0)) / sites
    mean_ref[1] = jnp.sum(jnp.where(real, 0.0, total)) / sites


def fused_on_device(mesh_shape, spatial_links, time_links):
    n_ta, n_gz, n_gy = (mesh_shape[name] for name in ("ta", "gz", "gy"))
    width = spatial_links.shape[-1]
    n_group = n_ta * n_gz * n_gy
    sites = float(n_gz * n_gy * 8 * width)
    spatial = spatial_links.reshape(3, 2, 3, 3, 2, 8, width)
    times_in = time_links.reshape(2, 3, 3, 2, 8, width)
    vm = lambda *shape: pltpu.VMEM(shape + (8, width), jnp.float32)
    dma = pltpu.SemaphoreType.DMA
    poly, total = pl.pallas_call(
        partial(fused_kernel, (n_ta, n_gz, n_gy, width, sites)),
        out_shape=(
            pltpu.VMEM((2, 8, width), jnp.float32),
            pltpu.VMEM((1, width), jnp.float32),
        ),
        in_specs=[pl.BlockSpec(memory_space=pl.ANY)] * 2,
        out_specs=(pl.BlockSpec(memory_space=pltpu.VMEM),) * 2,
        scratch_shapes=[
            vm(4, 2, 3, 3, 2),
            vm(n_gz, 2, 4, 2, 2),
            pltpu.VMEM((n_gz, 4, 2, 2, 2 * 8, width), jnp.float32),
            vm(4, 2, 3, 3, 3),
            vm(6, 2, 2, 3, 3),
            vm(6, 2, 2, 3, 3),
            vm(2, 24),
            vm(27),
            vm(2, 24),
            vm(27),
            vm(4, 2, 3),
            vm(4, 2, 3),
            vm(),
            vm(n_gz),
            pltpu.VMEM((1, 1, width), jnp.float32),
            pltpu.VMEM((n_group, 1, width), jnp.float32),
            dma((4,)),
            dma((2,)), dma((3,)), dma((2,)), dma((3,)),
            *[dma((1,))] * 6,
            *[pltpu.SemaphoreType.REGULAR] * 3,
        ],
        compiler_params=pltpu.CompilerParams(collective_id=0, has_side_effects=True),
    )(spatial, times_in)
    poly, mean = pl.pallas_call(
        partial(hand_over, width // n_gz, sites),
        out_shape=(
            jax.ShapeDtypeStruct((2, 8, width), jnp.float32),
            jax.ShapeDtypeStruct((2,), jnp.float32),
        ),
        in_specs=[pl.BlockSpec(memory_space=pltpu.VMEM)] * 2,
        out_specs=(
            pl.BlockSpec(memory_space=pltpu.VMEM),
            pl.BlockSpec(memory_space=pltpu.SMEM),
        ),
    )(*[pltpu.with_memory_space_constraint(x, pltpu.VMEM) for x in (poly, total)])
    return poly.reshape(2, 1, 8, width), mean


def fits_fused(mesh_shape, shape):
    width = shape[-1]
    n_ta, n_gz, n_gy = (mesh_shape[name] for name in ("ta", "gz", "gy"))
    per = shape[4] // n_ta, shape[5] // n_gz, shape[6] // n_gy
    window = width // n_gz + 2 * HALO
    return (
        per == (2, 1, 8) and n_ta == 2 and n_gz == 4 and n_gy == 2
        and width == 128 and ITERS >= 2 and window <= width // 3
    )


def solution(mesh):
    placed = (
        P("cfg", None, None, None, "ta", "gz", "gy", None),
        P("cfg", None, None, "ta", "gz", "gy", None),
    )

    def run(spatial_links, time_links):
        fused = fits_fused(mesh.shape, spatial_links.shape)
        body = partial(fused_on_device, dict(mesh.shape)) if fused else on_device
        return jax.shard_map(
            body,
            mesh=mesh,
            in_specs=placed,
            out_specs=(P("cfg", "gz", "gy", None), P("cfg")),
            check_vma=False,
        )(spatial_links, time_links)

    return run
```

```python
from functools import partial

import jax
import jax.numpy as jnp
from jax import lax
from jax.experimental import pallas as pl
from jax.experimental.pallas import tpu as pltpu
from jax.sharding import PartitionSpec as P

ITERS = 3


smear_weight = 0.5
norm_floor = 0.25
unit_steps = ((1, 0, 0), (0, 1, 0), (0, 0, 1))


def padded_2(cells, sides, width):
    for axis, dim in sides:
        count = lax.axis_size(axis)
        head = lax.slice_in_dim(cells, 0, width, axis=dim)
        tail = lax.slice_in_dim(cells, cells.shape[dim] - width, cells.shape[dim], axis=dim)
        cells = jnp.concatenate(
            [
                lax.ppermute(tail, axis, [(i, (i + 1) % count) for i in range(count)]),
                cells,
                lax.ppermute(head, axis, [((i + 1) % count, i) for i in range(count)]),
            ],
            axis=dim,
        )
    return cells


def shifted(shard, axis, by):
    devices = lax.axis_size(axis)
    return lax.ppermute(shard, axis, [(i, (i + by) % devices) for i in range(devices)])


def mat_product(lhs_mat, rhs_mat):
    lhs_re = lhs_mat[0][:, :, None]
    lhs_im = lhs_mat[1][:, :, None]
    rhs_re = rhs_mat[0][None]
    rhs_im = rhs_mat[1][None]
    real_part = jnp.sum(lhs_re * rhs_re - lhs_im * rhs_im, axis=1)
    imag_part = jnp.sum(lhs_re * rhs_im + lhs_im * rhs_re, axis=1)
    return jnp.stack([real_part, imag_part])


def dagger(matrix):
    return jnp.stack([jnp.swapaxes(matrix[0], 0, 1), -jnp.swapaxes(matrix[1], 0, 1)])


def normalize_row(row_vec):
    weight = jnp.sum(row_vec[0] * row_vec[0] + row_vec[1] * row_vec[1], axis=0)
    return row_vec / jnp.sqrt(jnp.maximum(weight, norm_floor))


def project(matrix):
    first = normalize_row(matrix[:, 0])
    second_raw = matrix[:, 1]
    inner_re = jnp.sum(first[0] * second_raw[0] + first[1] * second_raw[1], axis=0)
    inner_im = jnp.sum(first[0] * second_raw[1] - first[1] * second_raw[0], axis=0)
    ortho = jnp.stack(
        [
            second_raw[0] - (inner_re * first[0] - inner_im * first[1]),
            second_raw[1] - (inner_re * first[1] + inner_im * first[0]),
        ]
    )
    second = normalize_row(ortho)
    first_one = jnp.roll(first, -1, axis=1)
    first_two = jnp.roll(first, -2, axis=1)
    second_one = jnp.roll(second, -1, axis=1)
    second_two = jnp.roll(second, -2, axis=1)
    cross_re = (
        first_one[0] * second_two[0]
        - first_one[1] * second_two[1]
        - (first_two[0] * second_one[0] - first_two[1] * second_one[1])
    )
    cross_im = (
        first_one[0] * second_two[1]
        + first_one[1] * second_two[0]
        - (first_two[0] * second_one[1] + first_two[1] * second_one[0])
    )
    third = jnp.stack([cross_re, -cross_im])
    return jnp.stack([first, second, third], axis=1)


def moved(offset, unit_vec, factor):
    return (
        offset[0] + factor * unit_vec[0],
        offset[1] + factor * unit_vec[1],
        offset[2] + factor * unit_vec[2],
    )


def smear_spatial(neighbour):
    anchor = (0, 0, 0)
    result = []
    for mu_dir in range(3):
        staples = None
        for nu_dir in range(3):
            if nu_dir == mu_dir:
                continue
            forward = unit_steps[nu_dir]
            sideways = unit_steps[mu_dir]
            upper_staple = mat_product(
                mat_product(neighbour(nu_dir, anchor), neighbour(mu_dir, forward)),
                dagger(neighbour(nu_dir, sideways)),
            )
            back_offset = moved(anchor, forward, -1)
            lower_staple = mat_product(
                mat_product(dagger(neighbour(nu_dir, back_offset)), neighbour(mu_dir, back_offset)),
                neighbour(nu_dir, moved(back_offset, sideways, 1)),
            )
            if staples is None:
                staples = upper_staple + lower_staple
            else:
                staples = staples + upper_staple + lower_staple
        mixed_link = (1.0 - smear_weight) * neighbour(mu_dir, anchor) + smear_weight / 4.0 * staples
        result.append(project(mixed_link))
    return jnp.stack(result)


def window_cut(field, offset):
    z_inner = field.shape[-3] - 2
    y_inner = field.shape[-2] - 2
    piece = field[
        ..., 1 + offset[2] : 1 + offset[2] + z_inner, 1 + offset[1] : 1 + offset[1] + y_inner, :
    ]
    return jnp.roll(piece, -offset[0], axis=-1)


def padded_neighbour(padded, direction, offset):
    return window_cut(padded[direction], offset)


def smooth_by_products(link_field, time_links, extended, depth):
    later_links = extended[0:3, :, :, :, 1 : depth + 1]
    lowers = [
        mat_product(mat_product(dagger(link_field[nu_dir]), time_links), later_links[nu_dir])
        for nu_dir in range(3)
    ]
    carried = jnp.stack([time_links] + lowers)
    padded = padded_2(carried, (("gz", 5), ("gy", 6)), 1)
    anchor = (0, 0, 0)
    staples = None
    for nu_dir in range(3):
        forward = unit_steps[nu_dir]
        upper_staple = mat_product(
            mat_product(link_field[nu_dir], window_cut(padded[0], forward)),
            dagger(later_links[nu_dir]),
        )
        lower_staple = window_cut(padded[1 + nu_dir], moved(anchor, forward, -1))
        if staples is None:
            staples = upper_staple + lower_staple
        else:
            staples = staples + upper_staple + lower_staple
    mixed_link = (1.0 - smear_weight) * time_links + smear_weight / 6.0 * staples
    return project(mixed_link)


def on_device(spatial_links, time_links):
    link_field = spatial_links
    for sweep_index in range(ITERS):
        padded = padded_2(link_field, (("gz", 5), ("gy", 6)), 1)
        link_field = smear_spatial(partial(padded_neighbour, padded))
    stacked = jnp.concatenate([link_field, time_links[None]], axis=0)
    ahead_slice = shifted(stacked[:, :, :, :, 0:1], "ta", -1)
    extended = jnp.concatenate([stacked, ahead_slice], axis=4)
    depth = time_links.shape[3]
    smoothed = smooth_by_products(link_field, time_links, extended, depth)
    block_prod = smoothed[:, :, :, 0]
    block_prod = mat_product(block_prod, smoothed[:, :, :, 1])
    pieces = lax.all_gather(block_prod[None], "ta", axis=0, tiled=True)

    def advance(index, carry):
        return mat_product(carry, pieces[index])

    whole_prod = lax.fori_loop(1, pieces.shape[0], advance, pieces[0])
    polyakov = (
        jnp.stack(
            [
                whole_prod[0, 0, 0] + whole_prod[0, 1, 1] + whole_prod[0, 2, 2],
                whole_prod[1, 0, 0] + whole_prod[1, 1, 1] + whole_prod[1, 2, 2],
            ]
        )
        / 3.0
    )
    local_sums = jnp.sum(polyakov, axis=(1, 2, 3))
    totals = lax.psum(local_sums, ("gz", "gy"))
    site_count = (
        polyakov.shape[1]
        * polyakov.shape[2]
        * polyakov.shape[3]
        * lax.axis_size("gz")
        * lax.axis_size("gy")
    )
    site_mean = totals / site_count
    return (polyakov, site_mean)


HALO = ITERS + 1
MESH_ID = pl.DeviceIdType.MESH


def signed_sum(terms):
    total = None
    for sign, value in terms:
        if total is None:
            total = value if sign > 0 else -value
        elif sign > 0:
            total = total + value
        else:
            total = total - value
    return total


def times(lhs, rhs, lhs_dag=False, rhs_dag=False, rows=3):
    out = []
    for i in range(rows):
        line = []
        for j in range(3):
            real_terms, imag_terms = [], []
            for k in range(3):
                a_re, a_im = lhs[k][i] if lhs_dag else lhs[i][k]
                b_re, b_im = rhs[j][k] if rhs_dag else rhs[k][j]
                sa = -1 if lhs_dag else 1
                sb = -1 if rhs_dag else 1
                real_terms += [(1, a_re * b_re), (-sa * sb, a_im * b_im)]
                if sb > 0:
                    imag_terms += [(1, a_re * b_im), (sa, a_im * b_re)]
                else:
                    imag_terms += [(1, a_im * b_re), (-1, a_re * b_im)]
            line.append((signed_sum(real_terms), signed_sum(imag_terms)))
        out.append(line)
    return out


def unit_row(row):
    weight = signed_sum([(1, p * p) for pair in row for p in pair])
    scale = lax.rsqrt(jnp.maximum(weight, norm_floor))
    return [(re * scale, im * scale) for re, im in row]


def third_row(first, second):
    out = []
    for j in range(3):
        (a_re, a_im), (b_re, b_im) = first[(j + 1) % 3], second[(j + 2) % 3]
        (c_re, c_im), (d_re, d_im) = first[(j + 2) % 3], second[(j + 1) % 3]
        re = a_re * b_re - a_im * b_im - (c_re * d_re - c_im * d_im)
        im = c_re * d_im + c_im * d_re - (a_re * b_im + a_im * b_re)
        out.append((re, im))
    return out


def project_rows(rows):
    first = unit_row(rows[0])
    inner_re = signed_sum(
        [(1, p) for (a, b), (c, d) in zip(first, rows[1]) for p in (a * c, b * d)]
    )
    inner_im = None
    for (a, b), (c, d) in zip(first, rows[1]):
        part = a * d - b * c
        inner_im = part if inner_im is None else inner_im + part
    ortho = [
        (c - (inner_re * a - inner_im * b), d - (inner_re * b + inner_im * a))
        for (a, b), (c, d) in zip(first, rows[1])
    ]
    second = unit_row(ortho)
    return [first, second, third_row(first, second)]


def fused_kernel(
    dims, sl_hbm, tl_hbm, poly_ref, total_ref,
    raw, packed, landed, state, stash, ups, lows, outgoing, outgoing_x, ahead, ahead_x, smooth_out, smooth_in,
    trace_out, traces, row_out, rows_in,
    load_sem, a_send, a_recv, n_send, n_recv, w_send, w_recv,
    t_send, t_recv, r_send, r_recv, near_sem, far_sem, side_sem,
):
    n_ta, n_gz, n_gy, width, sites = dims
    quarter = width // n_gz
    slot = width // 3
    tiles = range(3)
    a, k, c = lax.axis_index("ta"), lax.axis_index("gz"), lax.axis_index("gy")
    lane = lax.broadcasted_iota(jnp.int32, (8, width), 1)
    n_group = n_ta * n_gz * n_gy
    middle = lax.rem((k + 1) // 2, 2)
    far_half = k // 2

    def mirrored(z):
        return z + far_half * (n_gz - 1 - 2 * z)

    barrier = pltpu.get_barrier_semaphore()

    def greet(device):
        pl.semaphore_signal(barrier, inc=1, device_id=device, device_id_type=MESH_ID)

    def tell(sem, z):
        pl.semaphore_signal(sem, inc=1, device_id={"gz": z}, device_id_type=MESH_ID)

    greet({"gy": 1 - c})
    greet({"ta": 1 - a})
    for core in range(n_gy):
        greet({"gz": mirrored(middle + 1), "gy": core})

    @pl.when(middle == 1)
    def _():
        for core in range(n_gy):
            greet({"gz": mirrored(0), "gy": core})

    loads = [pltpu.make_async_copy(sl_hbm.at[d], raw.at[d], load_sem.at[d]) for d in range(3)]
    loads.append(pltpu.make_async_copy(tl_hbm, raw.at[3], load_sem.at[3]))
    for copy in loads:
        copy.start()
    def settle(ref, sem):
        pltpu.make_async_copy(ref, ref, sem).wait()

    wide = lax.broadcasted_iota(jnp.int32, (32, width), 1)
    reach = quarter + 2 * HALO - 2
    spare = width - 3 * reach
    spread_over = list(range(8)) + [8]
    spilled = 11

    def side_by_side(d, t, dest):
        tile = None
        for j in range(3):
            shift = lax.rem(reach * j + HALO - 1 + width - quarter * dest + width, width)
            moved_block = pltpu.roll(raw[d, :, 0:2, j, t].reshape(32, width), shift, 1)
            tile = moved_block if j == 0 else jnp.where(wide >= reach * j, moved_block, tile)
        return tile.reshape(4, 8, width)

    first_dests = [mirrored(middle + 1), mirrored(2 - 2 * middle), mirrored(3), k]
    own = n_gz - 1
    later_dests = [own - i - (own - i <= k).astype(jnp.int32) for i in range(own)] + [k]

    def pack(hop, d):
        dest = (later_dests if d > 1 else first_dests)[hop]
        for t in range(2):
            block = side_by_side(d, t, dest)
            if d < 2:
                spill = side_by_side(2, t, dest)[3]
                for n in range(4):
                    at = spread_over.index(4 * d + n)
                    packed[hop, t, 4 * d + n] = jnp.where(
                        lane < 3 * reach, block[n], turn(spill, 3 * reach - spare * at)
                    )
            elif d == 2:
                at = spread_over.index(4 * d)
                packed[hop, t, 4 * d] = jnp.where(
                    lane < 3 * reach, block[0], turn(block[3], 3 * reach - spare * at)
                )
                packed[hop, t, pl.ds(4 * d + 1, 2)] = block[1:3]
            else:
                packed[hop, t, pl.ds(4 * d, 4)] = block

    def turn(value, lanes):
        lanes = lanes % width
        return pltpu.roll(value, lanes, 1) if lanes else value

    groups = ((0, 1), (2,), (3,))
    parts = [pl.ds(0, 8), pl.ds(8, 3), pl.ds(12, 4)]

    def exchange(hop, t_rel, group):
        t = lax.rem(c + t_rel, 2)
        src = packed.at[hop, t, parts[group]]
        dst = landed.at[k, parts[group], pl.ds(pl.multiple_of(8 * c, 8), 8)]
        if hop == own and t_rel == 0:
            return pltpu.make_async_copy(src, dst, a_recv.at[group])
        return pltpu.make_async_remote_copy(
            src_ref=src, dst_ref=dst,
            send_sem=a_send.at[hop // own + 2 * (group // 2)], recv_sem=a_recv.at[group],
            device_id={"gz": (later_dests if group else first_dests)[hop], "gy": t}, device_id_type=MESH_ID,
        )

    hops = list(range(n_gz))

    def hand_out(group):
        members = groups[group]
        for d in ((0, 1, 2), (), (3,))[group]:
            loads[d].wait()
        for d in members:
            pack(0, d)
        if group == 0:
            pl.semaphore_wait(barrier, 4 + 2 * middle)

            @pl.when(middle == 1)
            def _():
                tell(near_sem, mirrored(0))
                tell(far_sem, mirrored(2))
        for hop in hops:
            if hop:
                for d in members:
                    pack(hop, d)
            if group == 0 and hop == 1:

                @pl.when(middle == 0)
                def _():
                    pl.semaphore_wait(near_sem, 1)

            if group == 0 and hop == 2:
                pl.semaphore_wait(far_sem, 1)

                @pl.when(middle == 1)
                def _():
                    tell(far_sem, mirrored(0))

                pl.semaphore_signal(
                    side_sem, inc=1, device_id={"ta": 1 - a}, device_id_type=MESH_ID
                )
            for t_rel in range(2):
                exchange(hop, t_rel, group).start()

    hand_out(0)
    hand_out(1)

    def arrived(group):
        settle(landed.at[:, parts[group]], a_recv.at[group])

    def by_slot(values):
        tile = values[-1]
        for g in reversed(range(len(values) - 1)):
            tile = jnp.where(lane < slot * (g + 1), values[g], tile)
        return tile

    places = [[(z, 0) for z in range(3)], [(z, 1) for z in range(3)], [(3, 0), (3, 1)]]

    def closed(read):
        rows = [[(read(0, r, j), read(1, r, j)) for j in range(3)] for r in range(2)]
        rows.append(third_row(rows[0], rows[1]))
        return rows

    def gather_spill():
        for z in range(n_gz):
            for half in range(2):
                rows = pl.ds(8 * half, 8)
                tile = None
                for at, n in reversed(list(enumerate(spread_over))):
                    piece = turn(landed[z, n, rows], spare * at - 3 * reach)
                    tile = (
                        piece if tile is None
                        else jnp.where(lane < spare * (at + 1), piece, tile)
                    )
                landed[z, spilled, rows] = tile

    def unpack(d):
        if d == 2:
            gather_spill()
        for tile in tiles:

            def entry(ri, r, j):
                return by_slot([
                    turn(
                        landed[z, 4 * d + 2 * ri + r, pl.ds(h, 8, stride=2)],
                        slot * g - reach * j + 1,
                    )
                    for g, (z, h) in enumerate(places[tile])
                ])

            put(d, tile, closed(entry))

    def put(d, tile, mat):
        for r in range(3):
            for j in range(3):
                for ri in range(2):
                    state[d, ri, r, j, tile] = mat[r][j][ri]

    def get(read, rows=3):
        return [[(read(0, r, j), read(1, r, j)) for j in range(3)] for r in range(rows)]

    def down(value):
        return pltpu.roll(value, 7, 0)

    def up_row(value):
        return pltpu.roll(value, 1, 0)

    def shift_plus(read, nu, tile):
        if nu == 0:
            return turn(read(tile), -1)
        if nu == 1:
            if tile == 0:
                return read(1)
            if tile == 1:
                return down(read(0))
            return by_slot([turn(read(2), -slot), down(turn(read(2), slot))])
        if tile == 2:
            return by_slot([read(0), turn(read(1), slot)])
        inner = turn(read(tile), -slot)
        return jnp.where(lane < 2 * slot, inner, turn(read(2), slot * (2 - tile)))

    def shift_minus(read, nu, tile):
        if nu == 0:
            return turn(read(tile), 1)
        if nu == 1:
            if tile == 0:
                return up_row(read(1))
            if tile == 1:
                return read(0)
            return by_slot([up_row(turn(read(2), -slot)), turn(read(2), slot)])
        if tile == 2:
            return by_slot([turn(read(0), -2 * slot), turn(read(1), -slot)])
        return by_slot([turn(read(2), -slot * tile), turn(read(tile), slot)])

    def here(d, tile):
        return get(lambda ri, r, j: state[d, ri, r, j, tile])

    def plus(d, nu, tile):
        return get(
            lambda ri, r, j: shift_plus(lambda other: state[d, ri, r, j, other], nu, tile)
        )

    def keep(ref, entry, tile, mat):
        for r in range(2):
            for j in range(3):
                for ri in range(2):
                    ref[entry, ri, r, j, tile] = mat[r][j][ri]

    pairs = [(0, 1), (0, 2), (1, 2)]
    slot_of = {}
    for mu in range(3):
        for nu in range(3):
            if mu != nu:
                slot_of[mu, nu] = len(slot_of)

    def staples(chosen):
        for tile in tiles:
            for mu, nu in chosen:
                u_mu, u_nu = here(mu, tile), here(nu, tile)
                nu_ahead, mu_ahead = plus(nu, mu, tile), plus(mu, nu, tile)
                one = times(u_mu, nu_ahead)
                keep(lows, slot_of[mu, nu], tile, times(u_nu, one, lhs_dag=True, rows=2))
                keep(ups, slot_of[nu, mu], tile, times(one, mu_ahead, rhs_dag=True, rows=2))
                two = times(u_nu, mu_ahead)
                keep(lows, slot_of[nu, mu], tile, times(u_mu, two, lhs_dag=True, rows=2))
                keep(ups, slot_of[mu, nu], tile, times(two, nu_ahead, rhs_dag=True, rows=2))

    final_x = 4

    def staples_first():
        for tile in tiles:
            for nu in (1, 2):
                u_mu, u_nu = here(0, tile), here(nu, tile)
                nu_ahead, mu_ahead = plus(nu, 0, tile), plus(0, nu, tile)
                one = times(u_mu, nu_ahead)
                two = times(u_nu, mu_ahead)
                keep(lows, slot_of[0, nu], tile, times(u_nu, one, lhs_dag=True, rows=2))
                keep(ups, slot_of[0, nu], tile, times(two, nu_ahead, rhs_dag=True, rows=2))
                for row, line in enumerate(one[0:2] + two):
                    for j in range(3):
                        for ri in range(2):
                            stash[nu - 1, row, ri, j, tile] = line[j][ri]

    def staples_rest(nu):
        for tile in tiles:
            rows = [
                [(stash[nu - 1, row, 0, j, tile], stash[nu - 1, row, 1, j, tile])
                 for j in range(3)]
                for row in range(5)
            ]
            one, two = rows[0:2], rows[2:5]
            keep(lows, slot_of[nu, 0], tile, times(here(0, tile), two, lhs_dag=True, rows=2))
            mu_ahead = plus(0, nu, tile)
            keep(ups, slot_of[nu, 0], tile, times(one, mu_ahead, rhs_dag=True, rows=2))

    def mix(d, tile, entries, factor):
        def entry(ri, r, j):
            total = None
            for at, nu in entries:
                low = shift_minus(lambda other: lows[at, ri, r, j, other], nu, tile)
                part = ups[at, ri, r, j, tile] + low
                total = part if total is None else total + part
            return (1.0 - smear_weight) * state[d, ri, r, j, tile] + factor * total

        return project_rows(get(entry, rows=2))

    def update(chosen):
        for tile in tiles:
            for mu in chosen:
                entries = [(slot_of[mu, nu], nu) for nu in range(3) if nu != mu]
                put(mu, tile, mix(mu, tile, entries, smear_weight / 4.0))
    arrived(0)
    unpack(0)
    unpack(1)

    def sweep(index, carry):
        staples(pairs[0:1])

        @pl.when(index == 0)
        def _():
            arrived(1)
            hand_out(2)
            unpack(2)

        staples(pairs[1:3])
        update((0, 1, 2))
        return carry
    lax.fori_loop(0, ITERS - 1, sweep, 0)

    comps = [(ri, r, j) for ri in range(2) for r in range(2) for j in range(3)]
    n_dense = 2 * len(comps)
    in_slot = lax.rem(lane, slot)

    def next_copy(mu):
        return pltpu.make_async_remote_copy(
            src_ref=outgoing.at[mu - 1] if mu else outgoing_x,
            dst_ref=ahead.at[mu - 1] if mu else ahead_x,
            send_sem=n_send.at[int(mu > 0)], recv_sem=n_recv.at[mu],
            device_id={"ta": lax.rem(a + c + n_ta - 1, n_ta), "gy": 1 - c},
            device_id_type=MESH_ID,
        )

    def send_next(mu):
        out = outgoing.at[mu - 1] if mu else outgoing_x
        done = mu or final_x
        for q, (ri, r, j) in enumerate(comps):
            rest = state[done, ri, r, j, 2]
            for tile in range(2):
                full = state[done, ri, r, j, tile]
                dense = turn(rest, 3 * quarter - HALO - slot * tile)
                for g in reversed(range(3)):
                    dense = jnp.where(
                        lane < quarter * (g + 1),
                        turn(full, (quarter - slot) * g - HALO),
                        dense,
                    )
                out[2 * q + tile] = dense
        if mu == 0:
            for tile in tiles:
                edge = None
                for q, (ri, r, j) in enumerate(comps):
                    piece = turn(state[done, ri, r, j, tile], q + 1 - HALO)
                    edge = piece if edge is None else jnp.where(in_slot == q, piece, edge)
                out[n_dense + tile] = edge
        next_copy(mu).start()

    def later_links(mu, tile):
        source = ahead.at[mu - 1] if mu else ahead_x

        def entry(ri, r, j):
            q = comps.index((ri, r, j))
            if tile < 2:
                dense = source[2 * q + tile]
                value = by_slot([turn(dense, (slot - quarter) * g + HALO) for g in range(3)])
            else:
                value = by_slot([
                    turn(source[2 * q + half], slot * half + HALO - 3 * quarter)
                    for half in range(2)
                ])
            if mu == 0:
                edge = turn(source[n_dense + tile], HALO - 1 - q)
                value = jnp.where(in_slot == HALO - 1, edge, value)
            return value

        return closed(entry)
    pl.semaphore_wait(side_sem, 1)
    staples_first()
    for tile in tiles:
        entries = [(slot_of[0, nu], nu) for nu in (1, 2)]
        put(final_x, tile, mix(0, tile, entries, smear_weight / 4.0))
    send_next(0)
    staples_rest(1)
    staples(pairs[2:3])
    update((1,))
    send_next(1)
    staples_rest(2)
    update((2,))
    send_next(2)
    arrived(2)
    unpack(3)

    def time_firsts():
        for tile in tiles:
            for nu in range(3):
                u_nu = here(nu or final_x, tile)
                keep(ups, nu, tile, times(u_nu, plus(3, nu, tile), rows=2))
                keep(lows, nu, tile, times(u_nu, here(3, tile), lhs_dag=True, rows=2))

    def time_staples(nu):
        for tile in tiles:
            later = later_links(nu, tile)
            up = get(lambda ri, r, j: ups[nu, ri, r, j, tile], rows=2)
            keep(ups, nu, tile, times(up, later, rhs_dag=True, rows=2))
            low = get(lambda ri, r, j: lows[nu, ri, r, j, tile], rows=2)
            keep(lows, nu, tile, times(low, later, rows=2))

    factor = smear_weight / 6.0

    def sum_two():
        for tile in tiles:
            for ri, r, j in comps:
                total = None
                for nu in range(2):
                    low = shift_minus(lambda other: lows[nu, ri, r, j, other], nu, tile)
                    part = ups[nu, ri, r, j, tile] + low
                    total = part if total is None else total + part
                kept = (1.0 - smear_weight) * state[3, ri, r, j, tile]
                ups[3, ri, r, j, tile] = kept + factor * total

    def smooth(tile):
        def entry(ri, r, j):
            low = shift_minus(lambda other: lows[2, ri, r, j, other], 2, tile)
            return ups[3, ri, r, j, tile] + factor * (ups[2, ri, r, j, tile] + low)

        return project_rows(get(entry, rows=2))

    me = n_gy * a + c

    def lay_out(z, mats):
        for r in range(2):
            for j in range(3):
                dense = None
                for p in reversed(range(4)):
                    mat, g = mats[p // 2]
                    piece = turn(mat[r][j][p % 2], quarter * p - slot * g - HALO)
                    dense = (
                        piece if dense is None
                        else jnp.where(lane < quarter * (p + 1), piece, dense)
                    )
                smooth_out[z, r, j] = dense

    def deliver(z):
        @pl.when(me == z)
        def _():
            smooth_in[z] = smooth_out[z]

        @pl.when(me != z)
        def _():
            pltpu.make_async_remote_copy(
                src_ref=smooth_out.at[z], dst_ref=smooth_in.at[me],
                send_sem=w_send.at[0], recv_sem=w_recv.at[0],
                device_id={"ta": z // n_gy, "gy": z % n_gy}, device_id_type=MESH_ID,
            ).start()
    time_firsts()
    for nu in range(3):
        next_copy(nu).wait_recv()
        time_staples(nu)
        if nu == 1:
            sum_two()
    mats = [smooth(tile) for tile in tiles]
    for z in range(n_gz):
        lay_out(z, [(mats[0], z), (mats[1], z)] if z < 3 else [(mats[2], 0), (mats[2], 1)])
    for z in range(n_gz):
        deliver(z)
    settle(smooth_out.at[pl.ds(1, n_ta * n_gy - 1)], w_recv.at[0])

    def time_link(t):
        rows = []
        for r in range(2):
            tiles = [smooth_in[t, r, j] for j in range(3)]
            rows.append([(tile, pltpu.roll(tile, width - quarter, 1)) for tile in tiles])
        rows.append(third_row(rows[0], rows[1]))
        return rows
    early = times(time_link(0), time_link(1))
    late = times(time_link(2), time_link(3))
    re_terms, im_terms = [], []
    for i in range(3):
        for j in range(3):
            p_re, p_im = early[i][j]
            q_re, q_im = late[j][i]
            re_terms += [(1, p_re * q_re), (-1, p_im * q_im)]
            im_terms += [(1, p_re * q_im), (1, p_im * q_re)]
    trace_re = signed_sum(re_terms) / 3.0
    trace_im = signed_sum(im_terms) / 3.0
    trace = jnp.where(lax.rem(lane, 2 * quarter) < quarter, trace_re, turn(trace_im, quarter))
    trace_out[...] = trace
    sums = jnp.sum(trace, axis=0, keepdims=True)
    row_out[0] = sums
    for step in range(1, n_group):
        da, dk, dc = step // (n_gz * n_gy), step // n_gy % n_gz, step % n_gy
        device = {
            "ta": lax.rem(a + da, n_ta),
            "gz": lax.rem(k + dk, n_gz),
            "gy": lax.rem(c + dc, n_gy),
        }
        copy = pltpu.make_async_remote_copy(
            src_ref=row_out, dst_ref=rows_in.at[pl.ds(step, 1)],
            send_sem=r_send.at[0], recv_sem=r_recv.at[0],
            device_id=device, device_id_type=MESH_ID,
        )
        copy.start()
    keeps_one = k == me
    for ta in range(n_ta):
        for gy in range(n_gy):
            is_self = keeps_one & (a == ta) & (c == gy)
            remote = pltpu.make_async_remote_copy(
                src_ref=trace_out, dst_ref=traces.at[k],
                send_sem=t_send.at[0], recv_sem=t_recv.at[0],
                device_id={"ta": ta, "gz": me, "gy": gy}, device_id_type=MESH_ID,
            )
            local = pltpu.make_async_copy(trace_out, traces.at[k], t_recv.at[0])
            pl.when(jnp.logical_not(is_self))(remote.start)
            pl.when(is_self)(local.start)

    settle(traces, t_recv.at[0])
    for ri in range(2):
        for h in range(2):
            out = None
            for z in reversed(range(n_gz)):
                piece = turn(traces[z], quarter * (z - 2 * h - ri))
                out = piece if out is None else jnp.where(lane < quarter * (z + 1), piece, out)
            half = pltpu.roll(out, lax.rem(8 - 4 * c, 8), 0)
            poly_ref[ri, pl.ds(h, 4, stride=2)] = half[0:4]
    total = sums
    settle(rows_in.at[pl.ds(1, n_group - 1)], r_recv.at[0])
    for step in range(1, n_group):
        total = total + rows_in[step]
    total_ref[...] = total
    for late, sent in enumerate((pl.ds(0, 11), parts[2])):
        settle(packed.at[pl.ds(0, own), :, sent], a_send.at[2 * late])
        settle(packed.at[own, 0, sent], a_send.at[2 * late + 1])
    settle(ahead_x, n_send.at[0])
    settle(outgoing, n_send.at[1])
    settle(smooth_out.at[pl.ds(1, n_ta * n_gy - 1)], w_send.at[0])

    @pl.when(keeps_one)
    def _():
        settle(traces.at[pl.ds(1, n_gz - 1)], t_send.at[0])

    @pl.when(jnp.logical_not(keeps_one))
    def _():
        settle(traces, t_send.at[0])

    settle(rows_in.at[pl.ds(1, n_group - 1)], r_send.at[0])
def hand_over(quarter, sites, poly_in, total_in, poly_ref, mean_ref):
    poly_ref[...] = poly_in[...]
    total = total_in[...]
    place = lax.broadcasted_iota(jnp.int32, total.shape, 1)
    real = lax.rem(place, 2 * quarter) < quarter
    mean_ref[0] = jnp.sum(jnp.where(real, total, 0.0)) / sites
    mean_ref[1] = jnp.sum(jnp.where(real, 0.0, total)) / sites


def fused_on_device(mesh_shape, spatial_links, time_links):
    n_ta, n_gz, n_gy = (mesh_shape[name] for name in ("ta", "gz", "gy"))
    width = spatial_links.shape[-1]
    n_group = n_ta * n_gz * n_gy
    sites = float(n_gz * n_gy * 8 * width)
    spatial = spatial_links.reshape(3, 2, 3, 3, 2, 8, width)
    times_in = time_links.reshape(2, 3, 3, 2, 8, width)
    vm = lambda *shape: pltpu.VMEM(shape + (8, width), jnp.float32)
    dma = pltpu.SemaphoreType.DMA
    poly, total = pl.pallas_call(
        partial(fused_kernel, (n_ta, n_gz, n_gy, width, sites)),
        out_shape=(
            pltpu.VMEM((2, 8, width), jnp.float32),
            pltpu.VMEM((1, width), jnp.float32),
        ),
        in_specs=[pl.BlockSpec(memory_space=pl.ANY)] * 2,
        out_specs=(pl.BlockSpec(memory_space=pltpu.VMEM),) * 2,
        scratch_shapes=[
            vm(4, 2, 3, 3, 2),
            vm(n_gz, 2, 16),
            pltpu.VMEM((n_gz, 16, 2 * 8, width), jnp.float32),
            vm(5, 2, 3, 3, 3),
            vm(2, 5, 2, 3, 3),
            vm(6, 2, 2, 3, 3),
            vm(6, 2, 2, 3, 3),
            vm(2, 24),
            vm(27),
            vm(2, 24),
            vm(27),
            vm(4, 2, 3),
            vm(4, 2, 3),
            vm(),
            vm(n_gz),
            pltpu.VMEM((1, 1, width), jnp.float32),
            pltpu.VMEM((n_group, 1, width), jnp.float32),
            dma((4,)),
            dma((4,)), dma((3,)), dma((2,)), dma((3,)),
            *[dma((1,))] * 6,
            *[pltpu.SemaphoreType.REGULAR] * 3,
        ],
        compiler_params=pltpu.CompilerParams(collective_id=0, has_side_effects=True),
    )(spatial, times_in)
    poly, mean = pl.pallas_call(
        partial(hand_over, width // n_gz, sites),
        out_shape=(
            jax.ShapeDtypeStruct((2, 8, width), jnp.float32),
            jax.ShapeDtypeStruct((2,), jnp.float32),
        ),
        in_specs=[pl.BlockSpec(memory_space=pltpu.VMEM)] * 2,
        out_specs=(
            pl.BlockSpec(memory_space=pltpu.VMEM),
            pl.BlockSpec(memory_space=pltpu.SMEM),
        ),
    )(*[pltpu.with_memory_space_constraint(x, pltpu.VMEM) for x in (poly, total)])
    return poly.reshape(2, 1, 8, width), mean


def fits_fused(mesh_shape, shape):
    width = shape[-1]
    n_ta, n_gz, n_gy = (mesh_shape[name] for name in ("ta", "gz", "gy"))
    per = shape[4] // n_ta, shape[5] // n_gz, shape[6] // n_gy
    window = width // n_gz + 2 * HALO
    return (
        per == (2, 1, 8) and n_ta == 2 and n_gz == 4 and n_gy == 2
        and width == 128 and ITERS >= 2 and window <= width // 3
    )


def solution(mesh):
    placed = (
        P("cfg", None, None, None, "ta", "gz", "gy", None),
        P("cfg", None, None, "ta", "gz", "gy", None),
    )

    def run(spatial_links, time_links):
        fused = fits_fused(mesh.shape, spatial_links.shape)
        body = partial(fused_on_device, dict(mesh.shape)) if fused else on_device
        return jax.shard_map(
            body,
            mesh=mesh,
            in_specs=placed,
            out_specs=(P("cfg", "gz", "gy", None), P("cfg")),
            check_vma=False,
        )(spatial_links, time_links)

    return run
```

```python
from functools import partial

import jax
import jax.numpy as jnp
from jax import lax
from jax.experimental import pallas as pl
from jax.experimental.pallas import tpu as pltpu
from jax.sharding import PartitionSpec as P

ITERS = 3


smear_weight = 0.5
norm_floor = 0.25
unit_steps = ((1, 0, 0), (0, 1, 0), (0, 0, 1))


def padded_2(cells, sides, width):
    for axis, dim in sides:
        count = lax.axis_size(axis)
        head = lax.slice_in_dim(cells, 0, width, axis=dim)
        tail = lax.slice_in_dim(cells, cells.shape[dim] - width, cells.shape[dim], axis=dim)
        cells = jnp.concatenate(
            [
                lax.ppermute(tail, axis, [(i, (i + 1) % count) for i in range(count)]),
                cells,
                lax.ppermute(head, axis, [((i + 1) % count, i) for i in range(count)]),
            ],
            axis=dim,
        )
    return cells


def shifted(shard, axis, by):
    devices = lax.axis_size(axis)
    return lax.ppermute(shard, axis, [(i, (i + by) % devices) for i in range(devices)])


def mat_product(lhs_mat, rhs_mat):
    lhs_re = lhs_mat[0][:, :, None]
    lhs_im = lhs_mat[1][:, :, None]
    rhs_re = rhs_mat[0][None]
    rhs_im = rhs_mat[1][None]
    real_part = jnp.sum(lhs_re * rhs_re - lhs_im * rhs_im, axis=1)
    imag_part = jnp.sum(lhs_re * rhs_im + lhs_im * rhs_re, axis=1)
    return jnp.stack([real_part, imag_part])


def dagger(matrix):
    return jnp.stack([jnp.swapaxes(matrix[0], 0, 1), -jnp.swapaxes(matrix[1], 0, 1)])


def normalize_row(row_vec):
    weight = jnp.sum(row_vec[0] * row_vec[0] + row_vec[1] * row_vec[1], axis=0)
    return row_vec / jnp.sqrt(jnp.maximum(weight, norm_floor))


def project(matrix):
    first = normalize_row(matrix[:, 0])
    second_raw = matrix[:, 1]
    inner_re = jnp.sum(first[0] * second_raw[0] + first[1] * second_raw[1], axis=0)
    inner_im = jnp.sum(first[0] * second_raw[1] - first[1] * second_raw[0], axis=0)
    ortho = jnp.stack(
        [
            second_raw[0] - (inner_re * first[0] - inner_im * first[1]),
            second_raw[1] - (inner_re * first[1] + inner_im * first[0]),
        ]
    )
    second = normalize_row(ortho)
    first_one = jnp.roll(first, -1, axis=1)
    first_two = jnp.roll(first, -2, axis=1)
    second_one = jnp.roll(second, -1, axis=1)
    second_two = jnp.roll(second, -2, axis=1)
    cross_re = (
        first_one[0] * second_two[0]
        - first_one[1] * second_two[1]
        - (first_two[0] * second_one[0] - first_two[1] * second_one[1])
    )
    cross_im = (
        first_one[0] * second_two[1]
        + first_one[1] * second_two[0]
        - (first_two[0] * second_one[1] + first_two[1] * second_one[0])
    )
    third = jnp.stack([cross_re, -cross_im])
    return jnp.stack([first, second, third], axis=1)


def moved(offset, unit_vec, factor):
    return (
        offset[0] + factor * unit_vec[0],
        offset[1] + factor * unit_vec[1],
        offset[2] + factor * unit_vec[2],
    )


def smear_spatial(neighbour):
    anchor = (0, 0, 0)
    result = []
    for mu_dir in range(3):
        staples = None
        for nu_dir in range(3):
            if nu_dir == mu_dir:
                continue
            forward = unit_steps[nu_dir]
            sideways = unit_steps[mu_dir]
            upper_staple = mat_product(
                mat_product(neighbour(nu_dir, anchor), neighbour(mu_dir, forward)),
                dagger(neighbour(nu_dir, sideways)),
            )
            back_offset = moved(anchor, forward, -1)
            lower_staple = mat_product(
                mat_product(dagger(neighbour(nu_dir, back_offset)), neighbour(mu_dir, back_offset)),
                neighbour(nu_dir, moved(back_offset, sideways, 1)),
            )
            if staples is None:
                staples = upper_staple + lower_staple
            else:
                staples = staples + upper_staple + lower_staple
        mixed_link = (1.0 - smear_weight) * neighbour(mu_dir, anchor) + smear_weight / 4.0 * staples
        result.append(project(mixed_link))
    return jnp.stack(result)


def window_cut(field, offset):
    z_inner = field.shape[-3] - 2
    y_inner = field.shape[-2] - 2
    piece = field[
        ..., 1 + offset[2] : 1 + offset[2] + z_inner, 1 + offset[1] : 1 + offset[1] + y_inner, :
    ]
    return jnp.roll(piece, -offset[0], axis=-1)


def padded_neighbour(padded, direction, offset):
    return window_cut(padded[direction], offset)


def smooth_by_products(link_field, time_links, extended, depth):
    later_links = extended[0:3, :, :, :, 1 : depth + 1]
    lowers = [
        mat_product(mat_product(dagger(link_field[nu_dir]), time_links), later_links[nu_dir])
        for nu_dir in range(3)
    ]
    carried = jnp.stack([time_links] + lowers)
    padded = padded_2(carried, (("gz", 5), ("gy", 6)), 1)
    anchor = (0, 0, 0)
    staples = None
    for nu_dir in range(3):
        forward = unit_steps[nu_dir]
        upper_staple = mat_product(
            mat_product(link_field[nu_dir], window_cut(padded[0], forward)),
            dagger(later_links[nu_dir]),
        )
        lower_staple = window_cut(padded[1 + nu_dir], moved(anchor, forward, -1))
        if staples is None:
            staples = upper_staple + lower_staple
        else:
            staples = staples + upper_staple + lower_staple
    mixed_link = (1.0 - smear_weight) * time_links + smear_weight / 6.0 * staples
    return project(mixed_link)


def on_device(spatial_links, time_links):
    link_field = spatial_links
    for sweep_index in range(ITERS):
        padded = padded_2(link_field, (("gz", 5), ("gy", 6)), 1)
        link_field = smear_spatial(partial(padded_neighbour, padded))
    stacked = jnp.concatenate([link_field, time_links[None]], axis=0)
    ahead_slice = shifted(stacked[:, :, :, :, 0:1], "ta", -1)
    extended = jnp.concatenate([stacked, ahead_slice], axis=4)
    depth = time_links.shape[3]
    smoothed = smooth_by_products(link_field, time_links, extended, depth)
    block_prod = smoothed[:, :, :, 0]
    block_prod = mat_product(block_prod, smoothed[:, :, :, 1])
    pieces = lax.all_gather(block_prod[None], "ta", axis=0, tiled=True)

    def advance(index, carry):
        return mat_product(carry, pieces[index])

    whole_prod = lax.fori_loop(1, pieces.shape[0], advance, pieces[0])
    polyakov = (
        jnp.stack(
            [
                whole_prod[0, 0, 0] + whole_prod[0, 1, 1] + whole_prod[0, 2, 2],
                whole_prod[1, 0, 0] + whole_prod[1, 1, 1] + whole_prod[1, 2, 2],
            ]
        )
        / 3.0
    )
    local_sums = jnp.sum(polyakov, axis=(1, 2, 3))
    totals = lax.psum(local_sums, ("gz", "gy"))
    site_count = (
        polyakov.shape[1]
        * polyakov.shape[2]
        * polyakov.shape[3]
        * lax.axis_size("gz")
        * lax.axis_size("gy")
    )
    site_mean = totals / site_count
    return (polyakov, site_mean)


HALO = ITERS + 1
MESH_ID = pl.DeviceIdType.MESH


def signed_sum(terms):
    total = None
    for sign, value in terms:
        if total is None:
            total = value if sign > 0 else -value
        elif sign > 0:
            total = total + value
        else:
            total = total - value
    return total


def times(lhs, rhs, lhs_dag=False, rhs_dag=False, rows=3):
    out = []
    for i in range(rows):
        line = []
        for j in range(3):
            real_terms, imag_terms = [], []
            for k in range(3):
                a_re, a_im = lhs[k][i] if lhs_dag else lhs[i][k]
                b_re, b_im = rhs[j][k] if rhs_dag else rhs[k][j]
                sa = -1 if lhs_dag else 1
                sb = -1 if rhs_dag else 1
                real_terms += [(1, a_re * b_re), (-sa * sb, a_im * b_im)]
                if sb > 0:
                    imag_terms += [(1, a_re * b_im), (sa, a_im * b_re)]
                else:
                    imag_terms += [(1, a_im * b_re), (-1, a_re * b_im)]
            line.append((signed_sum(real_terms), signed_sum(imag_terms)))
        out.append(line)
    return out


def unit_row(row):
    weight = signed_sum([(1, p * p) for pair in row for p in pair])
    scale = lax.rsqrt(jnp.maximum(weight, norm_floor))
    return [(re * scale, im * scale) for re, im in row]


def third_row(first, second):
    out = []
    for j in range(3):
        (a_re, a_im), (b_re, b_im) = first[(j + 1) % 3], second[(j + 2) % 3]
        (c_re, c_im), (d_re, d_im) = first[(j + 2) % 3], second[(j + 1) % 3]
        re = a_re * b_re - a_im * b_im - (c_re * d_re - c_im * d_im)
        im = c_re * d_im + c_im * d_re - (a_re * b_im + a_im * b_re)
        out.append((re, im))
    return out


def project_rows(rows):
    first = unit_row(rows[0])
    inner_re = signed_sum(
        [(1, p) for (a, b), (c, d) in zip(first, rows[1]) for p in (a * c, b * d)]
    )
    inner_im = None
    for (a, b), (c, d) in zip(first, rows[1]):
        part = a * d - b * c
        inner_im = part if inner_im is None else inner_im + part
    ortho = [
        (c - (inner_re * a - inner_im * b), d - (inner_re * b + inner_im * a))
        for (a, b), (c, d) in zip(first, rows[1])
    ]
    second = unit_row(ortho)
    return [first, second, third_row(first, second)]


def fused_kernel(
    dims, sl_hbm, tl_hbm, poly_ref, total_ref,
    raw, packed, landed, state, stash, ups, lows, outgoing, outgoing_x, ahead, ahead_x, smooth_out, smooth_in,
    trace_out, traces, row_out, rows_in,
    load_sem, a_send, a_recv, n_send, n_recv, w_send, w_recv,
    t_send, t_recv, r_send, r_recv, near_sem, far_sem, side_sem,
):
    n_ta, n_gz, n_gy, width, sites = dims
    quarter = width // n_gz
    slot = width // 3
    tiles = range(3)
    a, k, c = lax.axis_index("ta"), lax.axis_index("gz"), lax.axis_index("gy")
    lane = lax.broadcasted_iota(jnp.int32, (8, width), 1)
    n_group = n_ta * n_gz * n_gy
    middle = lax.rem((k + 1) // 2, 2)
    far_half = k // 2

    def mirrored(z):
        return z + far_half * (n_gz - 1 - 2 * z)

    barrier = pltpu.get_barrier_semaphore()

    def greet(device):
        pl.semaphore_signal(barrier, inc=1, device_id=device, device_id_type=MESH_ID)

    def tell(sem, z):
        pl.semaphore_signal(sem, inc=1, device_id={"gz": z}, device_id_type=MESH_ID)

    greet({"gy": 1 - c})
    greet({"ta": 1 - a})
    for core in range(n_gy):
        greet({"gz": mirrored(middle + 1), "gy": core})

    @pl.when(middle == 1)
    def _():
        for core in range(n_gy):
            greet({"gz": mirrored(0), "gy": core})

    loads = [pltpu.make_async_copy(sl_hbm.at[d], raw.at[d], load_sem.at[d]) for d in range(3)]
    loads.append(pltpu.make_async_copy(tl_hbm, raw.at[3], load_sem.at[3]))
    for copy in loads:
        copy.start()
    def settle(ref, sem):
        pltpu.make_async_copy(ref, ref, sem).wait()

    wide = lax.broadcasted_iota(jnp.int32, (32, width), 1)
    reach = quarter + 2 * HALO - 2
    spare = width - 3 * reach
    spread_over = list(range(8)) + [8]
    spilled = 11

    def side_by_side(d, t, dest):
        tile = None
        for j in range(3):
            shift = lax.rem(reach * j + HALO - 1 + width - quarter * dest + width, width)
            moved_block = pltpu.roll(raw[d, :, 0:2, j, t].reshape(32, width), shift, 1)
            tile = moved_block if j == 0 else jnp.where(wide >= reach * j, moved_block, tile)
        return tile.reshape(4, 8, width)

    first_dests = [mirrored(middle + 1), mirrored(2 - 2 * middle), mirrored(3), k]
    own = n_gz - 1
    later_dests = [own - i - (own - i <= k).astype(jnp.int32) for i in range(own)] + [k]

    def pack(hop, d):
        dest = (later_dests if d > 1 else first_dests)[hop]
        for t in range(2):
            block = side_by_side(d, t, dest)
            if d < 2:
                spill = side_by_side(2, t, dest)[3]
                for n in range(4):
                    at = spread_over.index(4 * d + n)
                    packed[hop, t, 4 * d + n] = jnp.where(
                        lane < 3 * reach, block[n], turn(spill, 3 * reach - spare * at)
                    )
            elif d == 2:
                at = spread_over.index(4 * d)
                packed[hop, t, 4 * d] = jnp.where(
                    lane < 3 * reach, block[0], turn(block[3], 3 * reach - spare * at)
                )
                packed[hop, t, pl.ds(4 * d + 1, 2)] = block[1:3]
            else:
                packed[hop, t, pl.ds(4 * d, 4)] = block

    def turn(value, lanes):
        lanes = lanes % width
        return pltpu.roll(value, lanes, 1) if lanes else value

    groups = ((0, 1), (2,), (3,))
    parts = [pl.ds(0, 8), pl.ds(8, 3), pl.ds(12, 4)]

    def exchange(hop, t_rel, group):
        t = lax.rem(c + t_rel, 2)
        src = packed.at[hop, t, parts[group]]
        dst = landed.at[k, parts[group], pl.ds(pl.multiple_of(8 * c, 8), 8)]
        if hop == own and t_rel == 0:
            return pltpu.make_async_copy(src, dst, a_recv.at[group])
        return pltpu.make_async_remote_copy(
            src_ref=src, dst_ref=dst,
            send_sem=a_send.at[hop // own + 2 * (group // 2)], recv_sem=a_recv.at[group],
            device_id={"gz": (later_dests if group else first_dests)[hop], "gy": t}, device_id_type=MESH_ID,
        )

    hops = list(range(n_gz))

    def hand_out(group):
        members = groups[group]
        for d in ((0, 1, 2), ())[group]:
            loads[d].wait()
        for d in members:
            pack(0, d)
        if group == 0:
            pl.semaphore_wait(barrier, 4 + 2 * middle)

            @pl.when(middle == 1)
            def _():
                tell(near_sem, mirrored(0))
                tell(far_sem, mirrored(2))
        for hop in hops:
            if hop:
                for d in members:
                    pack(hop, d)
            if group == 0 and hop == 1:

                @pl.when(middle == 0)
                def _():
                    pl.semaphore_wait(near_sem, 1)

            if group == 0 and hop == 2:
                pl.semaphore_wait(far_sem, 1)

                @pl.when(middle == 1)
                def _():
                    tell(far_sem, mirrored(0))

                pl.semaphore_signal(
                    side_sem, inc=1, device_id={"ta": 1 - a}, device_id_type=MESH_ID
                )
            for t_rel in range(2):
                exchange(hop, t_rel, group).start()

    hand_out(0)
    hand_out(1)
    loads[3].wait()
    for hop in hops:
        pack(hop, 3)

    def start_late():
        for hop in hops:
            for t_rel in range(2):
                exchange(hop, t_rel, 2).start()

    def arrived(group):
        settle(landed.at[:, parts[group]], a_recv.at[group])

    def by_slot(values):
        tile = values[-1]
        for g in reversed(range(len(values) - 1)):
            tile = jnp.where(lane < slot * (g + 1), values[g], tile)
        return tile

    places = [[(z, 0) for z in range(3)], [(z, 1) for z in range(3)], [(3, 0), (3, 1)]]

    def closed(read):
        rows = [[(read(0, r, j), read(1, r, j)) for j in range(3)] for r in range(2)]
        rows.append(third_row(rows[0], rows[1]))
        return rows

    def gather_spill():
        for z in range(n_gz):
            for half in range(2):
                rows = pl.ds(8 * half, 8)
                tile = None
                for at, n in reversed(list(enumerate(spread_over))):
                    piece = turn(landed[z, n, rows], spare * at - 3 * reach)
                    tile = (
                        piece if tile is None
                        else jnp.where(lane < spare * (at + 1), piece, tile)
                    )
                landed[z, spilled, rows] = tile

    def unpack(d):
        if d == 2:
            gather_spill()
        for tile in tiles:

            def entry(ri, r, j):
                return by_slot([
                    turn(
                        landed[z, 4 * d + 2 * ri + r, pl.ds(h, 8, stride=2)],
                        slot * g - reach * j + 1,
                    )
                    for g, (z, h) in enumerate(places[tile])
                ])

            put(d, tile, closed(entry))

    def put(d, tile, mat):
        for r in range(3):
            for j in range(3):
                for ri in range(2):
                    state[d, ri, r, j, tile] = mat[r][j][ri]

    def get(read, rows=3):
        return [[(read(0, r, j), read(1, r, j)) for j in range(3)] for r in range(rows)]

    def down(value):
        return pltpu.roll(value, 7, 0)

    def up_row(value):
        return pltpu.roll(value, 1, 0)

    def shift_plus(read, nu, tile):
        if nu == 0:
            return turn(read(tile), -1)
        if nu == 1:
            if tile == 0:
                return read(1)
            if tile == 1:
                return down(read(0))
            return by_slot([turn(read(2), -slot), down(turn(read(2), slot))])
        if tile == 2:
            return by_slot([read(0), turn(read(1), slot)])
        inner = turn(read(tile), -slot)
        return jnp.where(lane < 2 * slot, inner, turn(read(2), slot * (2 - tile)))

    def shift_minus(read, nu, tile):
        if nu == 0:
            return turn(read(tile), 1)
        if nu == 1:
            if tile == 0:
                return up_row(read(1))
            if tile == 1:
                return read(0)
            return by_slot([up_row(turn(read(2), -slot)), turn(read(2), slot)])
        if tile == 2:
            return by_slot([turn(read(0), -2 * slot), turn(read(1), -slot)])
        return by_slot([turn(read(2), -slot * tile), turn(read(tile), slot)])

    def here(d, tile):
        return get(lambda ri, r, j: state[d, ri, r, j, tile])

    def plus(d, nu, tile):
        return get(
            lambda ri, r, j: shift_plus(lambda other: state[d, ri, r, j, other], nu, tile)
        )

    def keep(ref, entry, tile, mat):
        for r in range(2):
            for j in range(3):
                for ri in range(2):
                    ref[entry, ri, r, j, tile] = mat[r][j][ri]

    pairs = [(0, 1), (0, 2), (1, 2)]
    slot_of = {}
    for mu in range(3):
        for nu in range(3):
            if mu != nu:
                slot_of[mu, nu] = len(slot_of)

    def staples(chosen):
        for tile in tiles:
            for mu, nu in chosen:
                u_mu, u_nu = here(mu, tile), here(nu, tile)
                nu_ahead, mu_ahead = plus(nu, mu, tile), plus(mu, nu, tile)
                one = times(u_mu, nu_ahead)
                keep(lows, slot_of[mu, nu], tile, times(u_nu, one, lhs_dag=True, rows=2))
                keep(ups, slot_of[nu, mu], tile, times(one, mu_ahead, rhs_dag=True, rows=2))
                two = times(u_nu, mu_ahead)
                keep(lows, slot_of[nu, mu], tile, times(u_mu, two, lhs_dag=True, rows=2))
                keep(ups, slot_of[mu, nu], tile, times(two, nu_ahead, rhs_dag=True, rows=2))

    final_x = 4

    def staples_first():
        for tile in tiles:
            for nu in (1, 2):
                u_mu, u_nu = here(0, tile), here(nu, tile)
                nu_ahead, mu_ahead = plus(nu, 0, tile), plus(0, nu, tile)
                one = times(u_mu, nu_ahead)
                two = times(u_nu, mu_ahead)
                keep(lows, slot_of[0, nu], tile, times(u_nu, one, lhs_dag=True, rows=2))
                keep(ups, slot_of[0, nu], tile, times(two, nu_ahead, rhs_dag=True, rows=2))
                for row, line in enumerate(one[0:2] + two):
                    for j in range(3):
                        for ri in range(2):
                            stash[nu - 1, row, ri, j, tile] = line[j][ri]

    def staples_rest(nu):
        for tile in tiles:
            rows = [
                [(stash[nu - 1, row, 0, j, tile], stash[nu - 1, row, 1, j, tile])
                 for j in range(3)]
                for row in range(5)
            ]
            one, two = rows[0:2], rows[2:5]
            keep(lows, slot_of[nu, 0], tile, times(here(0, tile), two, lhs_dag=True, rows=2))
            mu_ahead = plus(0, nu, tile)
            keep(ups, slot_of[nu, 0], tile, times(one, mu_ahead, rhs_dag=True, rows=2))

    def mix(d, tile, entries, factor):
        def entry(ri, r, j):
            total = None
            for at, nu in entries:
                low = shift_minus(lambda other: lows[at, ri, r, j, other], nu, tile)
                part = ups[at, ri, r, j, tile] + low
                total = part if total is None else total + part
            return (1.0 - smear_weight) * state[d, ri, r, j, tile] + factor * total

        return project_rows(get(entry, rows=2))

    def update(chosen):
        for tile in tiles:
            for mu in chosen:
                entries = [(slot_of[mu, nu], nu) for nu in range(3) if nu != mu]
                put(mu, tile, mix(mu, tile, entries, smear_weight / 4.0))
    arrived(0)
    unpack(0)
    unpack(1)

    def sweep(index, carry):
        staples(pairs[0:1])

        @pl.when(index == 0)
        def _():
            arrived(1)
            start_late()
            unpack(2)

        staples(pairs[1:3])
        update((0, 1, 2))
        return carry
    lax.fori_loop(0, ITERS - 1, sweep, 0)

    comps = [(ri, r, j) for ri in range(2) for r in range(2) for j in range(3)]
    n_dense = 2 * len(comps)
    in_slot = lax.rem(lane, slot)

    def next_copy(mu):
        return pltpu.make_async_remote_copy(
            src_ref=outgoing.at[mu - 1] if mu else outgoing_x,
            dst_ref=ahead.at[mu - 1] if mu else ahead_x,
            send_sem=n_send.at[int(mu > 0)], recv_sem=n_recv.at[mu],
            device_id={"ta": lax.rem(a + c + n_ta - 1, n_ta), "gy": 1 - c},
            device_id_type=MESH_ID,
        )

    def send_next(mu):
        out = outgoing.at[mu - 1] if mu else outgoing_x
        done = mu or final_x
        for q, (ri, r, j) in enumerate(comps):
            rest = state[done, ri, r, j, 2]
            for tile in range(2):
                full = state[done, ri, r, j, tile]
                dense = turn(rest, 3 * quarter - HALO - slot * tile)
                for g in reversed(range(3)):
                    dense = jnp.where(
                        lane < quarter * (g + 1),
                        turn(full, (quarter - slot) * g - HALO),
                        dense,
                    )
                out[2 * q + tile] = dense
        if mu == 0:
            for tile in tiles:
                edge = None
                for q, (ri, r, j) in enumerate(comps):
                    piece = turn(state[done, ri, r, j, tile], q + 1 - HALO)
                    edge = piece if edge is None else jnp.where(in_slot == q, piece, edge)
                out[n_dense + tile] = edge
        next_copy(mu).start()

    def later_links(mu, tile):
        source = ahead.at[mu - 1] if mu else ahead_x

        def entry(ri, r, j):
            q = comps.index((ri, r, j))
            if tile < 2:
                dense = source[2 * q + tile]
                value = by_slot([turn(dense, (slot - quarter) * g + HALO) for g in range(3)])
            else:
                value = by_slot([
                    turn(source[2 * q + half], slot * half + HALO - 3 * quarter)
                    for half in range(2)
                ])
            if mu == 0:
                edge = turn(source[n_dense + tile], HALO - 1 - q)
                value = jnp.where(in_slot == HALO - 1, edge, value)
            return value

        return closed(entry)
    pl.semaphore_wait(side_sem, 1)
    staples_first()
    for tile in tiles:
        entries = [(slot_of[0, nu], nu) for nu in (1, 2)]
        put(final_x, tile, mix(0, tile, entries, smear_weight / 4.0))
    send_next(0)
    staples_rest(1)
    staples(pairs[2:3])
    update((1,))
    send_next(1)
    staples_rest(2)
    update((2,))
    send_next(2)
    arrived(2)
    unpack(3)

    def time_firsts():
        for tile in tiles:
            for nu in range(3):
                u_nu = here(nu or final_x, tile)
                keep(ups, nu, tile, times(u_nu, plus(3, nu, tile), rows=2))
                keep(lows, nu, tile, times(u_nu, here(3, tile), lhs_dag=True, rows=2))

    def time_staples(nu):
        for tile in tiles:
            later = later_links(nu, tile)
            up = get(lambda ri, r, j: ups[nu, ri, r, j, tile], rows=2)
            keep(ups, nu, tile, times(up, later, rhs_dag=True, rows=2))
            low = get(lambda ri, r, j: lows[nu, ri, r, j, tile], rows=2)
            keep(lows, nu, tile, times(low, later, rows=2))

    factor = smear_weight / 6.0

    def sum_two():
        for tile in tiles:
            for ri, r, j in comps:
                total = None
                for nu in range(2):
                    low = shift_minus(lambda other: lows[nu, ri, r, j, other], nu, tile)
                    part = ups[nu, ri, r, j, tile] + low
                    total = part if total is None else total + part
                kept = (1.0 - smear_weight) * state[3, ri, r, j, tile]
                ups[3, ri, r, j, tile] = kept + factor * total

    def smooth(tile):
        def entry(ri, r, j):
            low = shift_minus(lambda other: lows[2, ri, r, j, other], 2, tile)
            return ups[3, ri, r, j, tile] + factor * (ups[2, ri, r, j, tile] + low)

        return project_rows(get(entry, rows=2))

    me = n_gy * a + c
    rank = (a * n_gz + k) * n_gy + c

    def lay_out(z, mats):
        for r in range(2):
            for j in range(3):
                dense = None
                for p in reversed(range(4)):
                    mat, g = mats[p // 2]
                    piece = turn(mat[r][j][p % 2], quarter * p - slot * g - HALO)
                    dense = (
                        piece if dense is None
                        else jnp.where(lane < quarter * (p + 1), piece, dense)
                    )
                smooth_out[z, r, j] = dense

    def deliver(z):
        pltpu.make_async_remote_copy(
            src_ref=smooth_out.at[z], dst_ref=smooth_in.at[me],
            send_sem=w_send.at[0], recv_sem=w_recv.at[0],
            device_id={"ta": z // n_gy, "gy": lax.rem(z, n_gy)}, device_id_type=MESH_ID,
        ).start()
    time_firsts()
    for nu in range(3):
        next_copy(nu).wait_recv()
        time_staples(nu)
        if nu == 1:
            sum_two()
    mats = [smooth(tile) for tile in tiles]
    for z in range(n_gz):
        lay_out(z, [(mats[0], z), (mats[1], z)] if z < 3 else [(mats[2], 0), (mats[2], 1)])
    for z in (n_gy * (1 - a), n_gy * (1 - a) + 1, n_gy * a + 1 - c):
        deliver(z)
    smooth_in[me] = smooth_out[me]
    settle(smooth_out.at[pl.ds(1, n_ta * n_gy - 1)], w_recv.at[0])

    def time_link(t):
        rows = []
        for r in range(2):
            tiles = [smooth_in[t, r, j] for j in range(3)]
            rows.append([(tile, pltpu.roll(tile, width - quarter, 1)) for tile in tiles])
        rows.append(third_row(rows[0], rows[1]))
        return rows
    early = times(time_link(0), time_link(1))
    late = times(time_link(2), time_link(3))
    re_terms, im_terms = [], []
    for i in range(3):
        for j in range(3):
            p_re, p_im = early[i][j]
            q_re, q_im = late[j][i]
            re_terms += [(1, p_re * q_re), (-1, p_im * q_im)]
            im_terms += [(1, p_re * q_im), (1, p_im * q_re)]
    trace_re = signed_sum(re_terms) / 3.0
    trace_im = signed_sum(im_terms) / 3.0
    trace = jnp.where(lax.rem(lane, 2 * quarter) < quarter, trace_re, turn(trace_im, quarter))
    trace_out[...] = trace
    sums = jnp.sum(trace, axis=0, keepdims=True)
    row_out[0] = sums
    for z in range(n_gz):
        for da in range(n_ta):
            for dc in range(n_gy):
                copy = pltpu.make_async_remote_copy(
                    src_ref=row_out, dst_ref=rows_in.at[pl.ds(rank, 1)],
                    send_sem=r_send.at[0], recv_sem=r_recv.at[0],
                    device_id={"ta": lax.rem(a + da, n_ta), "gz": z, "gy": lax.rem(c + dc, n_gy)},
                    device_id_type=MESH_ID,
                )
                if da or dc:
                    copy.start()
                else:
                    pl.when(k != z)(copy.start)
    rows_in[pl.ds(rank, 1)] = row_out[...]
    keeps_one = k == me
    for ta in range(n_ta):
        for gy in range(n_gy):
            is_self = keeps_one & (a == ta) & (c == gy)
            remote = pltpu.make_async_remote_copy(
                src_ref=trace_out, dst_ref=traces.at[k],
                send_sem=t_send.at[0], recv_sem=t_recv.at[0],
                device_id={"ta": ta, "gz": me, "gy": gy}, device_id_type=MESH_ID,
            )
            local = pltpu.make_async_copy(trace_out, traces.at[k], t_recv.at[0])
            pl.when(jnp.logical_not(is_self))(remote.start)
            pl.when(is_self)(local.start)

    settle(traces, t_recv.at[0])
    for ri in range(2):
        for h in range(2):
            out = None
            for z in reversed(range(n_gz)):
                piece = turn(traces[z], quarter * (z - 2 * h - ri))
                out = piece if out is None else jnp.where(lane < quarter * (z + 1), piece, out)
            half = pltpu.roll(out, lax.rem(8 - 4 * c, 8), 0)
            poly_ref[ri, pl.ds(h, 4, stride=2)] = half[0:4]
    settle(rows_in.at[pl.ds(1, n_group - 1)], r_recv.at[0])
    total = rows_in[0]
    for step in range(1, n_group):
        total = total + rows_in[step]
    total_ref[...] = total
    for late, sent in enumerate((pl.ds(0, 11), parts[2])):
        settle(packed.at[pl.ds(0, own), :, sent], a_send.at[2 * late])
        settle(packed.at[own, 0, sent], a_send.at[2 * late + 1])
    settle(ahead_x, n_send.at[0])
    settle(outgoing, n_send.at[1])
    settle(smooth_out.at[pl.ds(1, n_ta * n_gy - 1)], w_send.at[0])

    @pl.when(keeps_one)
    def _():
        settle(traces.at[pl.ds(1, n_gz - 1)], t_send.at[0])

    @pl.when(jnp.logical_not(keeps_one))
    def _():
        settle(traces, t_send.at[0])

    settle(rows_in.at[pl.ds(1, n_group - 1)], r_send.at[0])
def hand_over(quarter, sites, poly_in, total_in, poly_ref, mean_ref):
    poly_ref[...] = poly_in[...]
    total = total_in[...]
    place = lax.broadcasted_iota(jnp.int32, total.shape, 1)
    real = lax.rem(place, 2 * quarter) < quarter
    mean_ref[0] = jnp.sum(jnp.where(real, total, 0.0)) / sites
    mean_ref[1] = jnp.sum(jnp.where(real, 0.0, total)) / sites


def fused_on_device(mesh_shape, spatial_links, time_links):
    n_ta, n_gz, n_gy = (mesh_shape[name] for name in ("ta", "gz", "gy"))
    width = spatial_links.shape[-1]
    n_group = n_ta * n_gz * n_gy
    sites = float(n_gz * n_gy * 8 * width)
    spatial = spatial_links.reshape(3, 2, 3, 3, 2, 8, width)
    times_in = time_links.reshape(2, 3, 3, 2, 8, width)
    vm = lambda *shape: pltpu.VMEM(shape + (8, width), jnp.float32)
    dma = pltpu.SemaphoreType.DMA
    poly, total = pl.pallas_call(
        partial(fused_kernel, (n_ta, n_gz, n_gy, width, sites)),
        out_shape=(
            pltpu.VMEM((2, 8, width), jnp.float32),
            pltpu.VMEM((1, width), jnp.float32),
        ),
        in_specs=[pl.BlockSpec(memory_space=pl.ANY)] * 2,
        out_specs=(pl.BlockSpec(memory_space=pltpu.VMEM),) * 2,
        scratch_shapes=[
            vm(4, 2, 3, 3, 2),
            vm(n_gz, 2, 16),
            pltpu.VMEM((n_gz, 16, 2 * 8, width), jnp.float32),
            vm(5, 2, 3, 3, 3),
            vm(2, 5, 2, 3, 3),
            vm(6, 2, 2, 3, 3),
            vm(6, 2, 2, 3, 3),
            vm(2, 24),
            vm(27),
            vm(2, 24),
            vm(27),
            vm(4, 2, 3),
            vm(4, 2, 3),
            vm(),
            vm(n_gz),
            pltpu.VMEM((1, 1, width), jnp.float32),
            pltpu.VMEM((n_group, 1, width), jnp.float32),
            dma((4,)),
            dma((4,)), dma((3,)), dma((2,)), dma((3,)),
            *[dma((1,))] * 6,
            *[pltpu.SemaphoreType.REGULAR] * 3,
        ],
        compiler_params=pltpu.CompilerParams(collective_id=0, has_side_effects=True),
    )(spatial, times_in)
    poly, mean = pl.pallas_call(
        partial(hand_over, width // n_gz, sites),
        out_shape=(
            jax.ShapeDtypeStruct((2, 8, width), jnp.float32),
            jax.ShapeDtypeStruct((2,), jnp.float32),
        ),
        in_specs=[pl.BlockSpec(memory_space=pltpu.VMEM)] * 2,
        out_specs=(
            pl.BlockSpec(memory_space=pltpu.VMEM),
            pl.BlockSpec(memory_space=pltpu.SMEM),
        ),
    )(*[pltpu.with_memory_space_constraint(x, pltpu.VMEM) for x in (poly, total)])
    return poly.reshape(2, 1, 8, width), mean


def fits_fused(mesh_shape, shape):
    width = shape[-1]
    n_ta, n_gz, n_gy = (mesh_shape[name] for name in ("ta", "gz", "gy"))
    per = shape[4] // n_ta, shape[5] // n_gz, shape[6] // n_gy
    window = width // n_gz + 2 * HALO
    return (
        per == (2, 1, 8) and n_ta == 2 and n_gz == 4 and n_gy == 2
        and width == 128 and ITERS >= 2 and window <= width // 3
    )


def solution(mesh):
    placed = (
        P("cfg", None, None, None, "ta", "gz", "gy", None),
        P("cfg", None, None, "ta", "gz", "gy", None),
    )

    def run(spatial_links, time_links):
        fused = fits_fused(mesh.shape, spatial_links.shape)
        body = partial(fused_on_device, dict(mesh.shape)) if fused else on_device
        return jax.shard_map(
            body,
            mesh=mesh,
            in_specs=placed,
            out_specs=(P("cfg", "gz", "gy", None), P("cfg")),
            check_vma=False,
        )(spatial_links, time_links)

    return run
```

```python
from functools import partial

import jax
import jax.numpy as jnp
from jax import lax
from jax.experimental import pallas as pl
from jax.experimental.pallas import tpu as pltpu
from jax.sharding import PartitionSpec as P

ITERS = 3


smear_weight = 0.5
norm_floor = 0.25
unit_steps = ((1, 0, 0), (0, 1, 0), (0, 0, 1))


def padded_2(cells, sides, width):
    for axis, dim in sides:
        count = lax.axis_size(axis)
        head = lax.slice_in_dim(cells, 0, width, axis=dim)
        tail = lax.slice_in_dim(cells, cells.shape[dim] - width, cells.shape[dim], axis=dim)
        cells = jnp.concatenate(
            [
                lax.ppermute(tail, axis, [(i, (i + 1) % count) for i in range(count)]),
                cells,
                lax.ppermute(head, axis, [((i + 1) % count, i) for i in range(count)]),
            ],
            axis=dim,
        )
    return cells


def shifted(shard, axis, by):
    devices = lax.axis_size(axis)
    return lax.ppermute(shard, axis, [(i, (i + by) % devices) for i in range(devices)])


def mat_product(lhs_mat, rhs_mat):
    lhs_re = lhs_mat[0][:, :, None]
    lhs_im = lhs_mat[1][:, :, None]
    rhs_re = rhs_mat[0][None]
    rhs_im = rhs_mat[1][None]
    real_part = jnp.sum(lhs_re * rhs_re - lhs_im * rhs_im, axis=1)
    imag_part = jnp.sum(lhs_re * rhs_im + lhs_im * rhs_re, axis=1)
    return jnp.stack([real_part, imag_part])


def dagger(matrix):
    return jnp.stack([jnp.swapaxes(matrix[0], 0, 1), -jnp.swapaxes(matrix[1], 0, 1)])


def normalize_row(row_vec):
    weight = jnp.sum(row_vec[0] * row_vec[0] + row_vec[1] * row_vec[1], axis=0)
    return row_vec / jnp.sqrt(jnp.maximum(weight, norm_floor))


def project(matrix):
    first = normalize_row(matrix[:, 0])
    second_raw = matrix[:, 1]
    inner_re = jnp.sum(first[0] * second_raw[0] + first[1] * second_raw[1], axis=0)
    inner_im = jnp.sum(first[0] * second_raw[1] - first[1] * second_raw[0], axis=0)
    ortho = jnp.stack(
        [
            second_raw[0] - (inner_re * first[0] - inner_im * first[1]),
            second_raw[1] - (inner_re * first[1] + inner_im * first[0]),
        ]
    )
    second = normalize_row(ortho)
    first_one = jnp.roll(first, -1, axis=1)
    first_two = jnp.roll(first, -2, axis=1)
    second_one = jnp.roll(second, -1, axis=1)
    second_two = jnp.roll(second, -2, axis=1)
    cross_re = (
        first_one[0] * second_two[0]
        - first_one[1] * second_two[1]
        - (first_two[0] * second_one[0] - first_two[1] * second_one[1])
    )
    cross_im = (
        first_one[0] * second_two[1]
        + first_one[1] * second_two[0]
        - (first_two[0] * second_one[1] + first_two[1] * second_one[0])
    )
    third = jnp.stack([cross_re, -cross_im])
    return jnp.stack([first, second, third], axis=1)


def moved(offset, unit_vec, factor):
    return (
        offset[0] + factor * unit_vec[0],
        offset[1] + factor * unit_vec[1],
        offset[2] + factor * unit_vec[2],
    )


def smear_spatial(neighbour):
    anchor = (0, 0, 0)
    result = []
    for mu_dir in range(3):
        staples = None
        for nu_dir in range(3):
            if nu_dir == mu_dir:
                continue
            forward = unit_steps[nu_dir]
            sideways = unit_steps[mu_dir]
            upper_staple = mat_product(
                mat_product(neighbour(nu_dir, anchor), neighbour(mu_dir, forward)),
                dagger(neighbour(nu_dir, sideways)),
            )
            back_offset = moved(anchor, forward, -1)
            lower_staple = mat_product(
                mat_product(dagger(neighbour(nu_dir, back_offset)), neighbour(mu_dir, back_offset)),
                neighbour(nu_dir, moved(back_offset, sideways, 1)),
            )
            if staples is None:
                staples = upper_staple + lower_staple
            else:
                staples = staples + upper_staple + lower_staple
        mixed_link = (1.0 - smear_weight) * neighbour(mu_dir, anchor) + smear_weight / 4.0 * staples
        result.append(project(mixed_link))
    return jnp.stack(result)


def window_cut(field, offset):
    z_inner = field.shape[-3] - 2
    y_inner = field.shape[-2] - 2
    piece = field[
        ..., 1 + offset[2] : 1 + offset[2] + z_inner, 1 + offset[1] : 1 + offset[1] + y_inner, :
    ]
    return jnp.roll(piece, -offset[0], axis=-1)


def padded_neighbour(padded, direction, offset):
    return window_cut(padded[direction], offset)


def smooth_by_products(link_field, time_links, extended, depth):
    later_links = extended[0:3, :, :, :, 1 : depth + 1]
    lowers = [
        mat_product(mat_product(dagger(link_field[nu_dir]), time_links), later_links[nu_dir])
        for nu_dir in range(3)
    ]
    carried = jnp.stack([time_links] + lowers)
    padded = padded_2(carried, (("gz", 5), ("gy", 6)), 1)
    anchor = (0, 0, 0)
    staples = None
    for nu_dir in range(3):
        forward = unit_steps[nu_dir]
        upper_staple = mat_product(
            mat_product(link_field[nu_dir], window_cut(padded[0], forward)),
            dagger(later_links[nu_dir]),
        )
        lower_staple = window_cut(padded[1 + nu_dir], moved(anchor, forward, -1))
        if staples is None:
            staples = upper_staple + lower_staple
        else:
            staples = staples + upper_staple + lower_staple
    mixed_link = (1.0 - smear_weight) * time_links + smear_weight / 6.0 * staples
    return project(mixed_link)


def on_device(spatial_links, time_links):
    link_field = spatial_links
    for sweep_index in range(ITERS):
        padded = padded_2(link_field, (("gz", 5), ("gy", 6)), 1)
        link_field = smear_spatial(partial(padded_neighbour, padded))
    stacked = jnp.concatenate([link_field, time_links[None]], axis=0)
    ahead_slice = shifted(stacked[:, :, :, :, 0:1], "ta", -1)
    extended = jnp.concatenate([stacked, ahead_slice], axis=4)
    depth = time_links.shape[3]
    smoothed = smooth_by_products(link_field, time_links, extended, depth)
    block_prod = smoothed[:, :, :, 0]
    block_prod = mat_product(block_prod, smoothed[:, :, :, 1])
    pieces = lax.all_gather(block_prod[None], "ta", axis=0, tiled=True)

    def advance(index, carry):
        return mat_product(carry, pieces[index])

    whole_prod = lax.fori_loop(1, pieces.shape[0], advance, pieces[0])
    polyakov = (
        jnp.stack(
            [
                whole_prod[0, 0, 0] + whole_prod[0, 1, 1] + whole_prod[0, 2, 2],
                whole_prod[1, 0, 0] + whole_prod[1, 1, 1] + whole_prod[1, 2, 2],
            ]
        )
        / 3.0
    )
    local_sums = jnp.sum(polyakov, axis=(1, 2, 3))
    totals = lax.psum(local_sums, ("gz", "gy"))
    site_count = (
        polyakov.shape[1]
        * polyakov.shape[2]
        * polyakov.shape[3]
        * lax.axis_size("gz")
        * lax.axis_size("gy")
    )
    site_mean = totals / site_count
    return (polyakov, site_mean)


HALO = ITERS + 1
MESH_ID = pl.DeviceIdType.MESH


def signed_sum(terms):
    total = None
    for sign, value in terms:
        if total is None:
            total = value if sign > 0 else -value
        elif sign > 0:
            total = total + value
        else:
            total = total - value
    return total


def times(lhs, rhs, lhs_dag=False, rhs_dag=False, rows=3):
    out = []
    for i in range(rows):
        line = []
        for j in range(3):
            real_terms, imag_terms = [], []
            for k in range(3):
                a_re, a_im = lhs[k][i] if lhs_dag else lhs[i][k]
                b_re, b_im = rhs[j][k] if rhs_dag else rhs[k][j]
                sa = -1 if lhs_dag else 1
                sb = -1 if rhs_dag else 1
                real_terms += [(1, a_re * b_re), (-sa * sb, a_im * b_im)]
                if sb > 0:
                    imag_terms += [(1, a_re * b_im), (sa, a_im * b_re)]
                else:
                    imag_terms += [(1, a_im * b_re), (-1, a_re * b_im)]
            line.append((signed_sum(real_terms), signed_sum(imag_terms)))
        out.append(line)
    return out


def unit_row(row):
    weight = signed_sum([(1, p * p) for pair in row for p in pair])
    scale = lax.rsqrt(jnp.maximum(weight, norm_floor))
    return [(re * scale, im * scale) for re, im in row]


def third_row(first, second):
    out = []
    for j in range(3):
        (a_re, a_im), (b_re, b_im) = first[(j + 1) % 3], second[(j + 2) % 3]
        (c_re, c_im), (d_re, d_im) = first[(j + 2) % 3], second[(j + 1) % 3]
        re = a_re * b_re - a_im * b_im - (c_re * d_re - c_im * d_im)
        im = c_re * d_im + c_im * d_re - (a_re * b_im + a_im * b_re)
        out.append((re, im))
    return out


def project_rows(rows):
    first = unit_row(rows[0])
    inner_re = signed_sum(
        [(1, p) for (a, b), (c, d) in zip(first, rows[1]) for p in (a * c, b * d)]
    )
    inner_im = None
    for (a, b), (c, d) in zip(first, rows[1]):
        part = a * d - b * c
        inner_im = part if inner_im is None else inner_im + part
    ortho = [
        (c - (inner_re * a - inner_im * b), d - (inner_re * b + inner_im * a))
        for (a, b), (c, d) in zip(first, rows[1])
    ]
    second = unit_row(ortho)
    return [first, second, third_row(first, second)]


def fused_kernel(
    dims, sl_hbm, tl_hbm, poly_ref, total_ref,
    raw, packed, landed, state, stash, ups, lows, outgoing, outgoing_x, ahead, ahead_x, smooth_out, smooth_in,
    trace_out, traces, row_out, rows_in,
    load_sem, a_send, a_recv, n_send, n_recv, w_send, w_recv,
    t_send, t_recv, r_send, r_recv, near_sem, far_sem, side_sem,
):
    n_ta, n_gz, n_gy, width, sites = dims
    quarter = width // n_gz
    slot = width // 3
    tiles = range(3)
    a, k, c = lax.axis_index("ta"), lax.axis_index("gz"), lax.axis_index("gy")
    lane = lax.broadcasted_iota(jnp.int32, (8, width), 1)
    n_group = n_ta * n_gz * n_gy
    loads = [pltpu.make_async_copy(sl_hbm.at[d], raw.at[d], load_sem.at[d]) for d in range(3)]
    loads.append(pltpu.make_async_copy(tl_hbm, raw.at[3], load_sem.at[3]))
    for copy in loads:
        copy.start()

    middle = lax.rem((k + 1) // 2, 2)
    far_half = k // 2

    def mirrored(z):
        return z + far_half * (n_gz - 1 - 2 * z)

    barrier = pltpu.get_barrier_semaphore()

    def greet(device):
        pl.semaphore_signal(barrier, inc=1, device_id=device, device_id_type=MESH_ID)

    def tell(sem, z):
        pl.semaphore_signal(sem, inc=1, device_id={"gz": z}, device_id_type=MESH_ID)

    greet({"gy": 1 - c})
    greet({"ta": 1 - a})
    for core in range(n_gy):
        greet({"gz": mirrored(middle + 1), "gy": core})

    @pl.when(middle == 1)
    def _():
        for core in range(n_gy):
            greet({"gz": mirrored(0), "gy": core})
    def settle(ref, sem):
        pltpu.make_async_copy(ref, ref, sem).wait()

    wide = lax.broadcasted_iota(jnp.int32, (32, width), 1)
    reach = quarter + 2 * HALO - 2
    spare = width - 3 * reach
    spread_over = list(range(8)) + [8]
    spilled = 11

    def side_by_side(d, t, dest):
        tile = None
        for j in range(3):
            shift = lax.rem(reach * j + HALO - 1 + width - quarter * dest + width, width)
            moved_block = pltpu.roll(raw[d, :, 0:2, j, t].reshape(32, width), shift, 1)
            tile = moved_block if j == 0 else jnp.where(wide >= reach * j, moved_block, tile)
        return tile.reshape(4, 8, width)

    first_dests = [mirrored(middle + 1), mirrored(2 - 2 * middle), mirrored(3), k]
    own = n_gz - 1
    later_dests = [own - i - (own - i <= k).astype(jnp.int32) for i in range(own)] + [k]

    def pack(hop, d):
        dest = (later_dests if d > 1 else first_dests)[hop]
        for t in range(2):
            block = side_by_side(d, t, dest)
            if d < 2:
                spill = side_by_side(2, t, dest)[3]
                for n in range(4):
                    at = spread_over.index(4 * d + n)
                    packed[hop, t, 4 * d + n] = jnp.where(
                        lane < 3 * reach, block[n], turn(spill, 3 * reach - spare * at)
                    )
            elif d == 2:
                at = spread_over.index(4 * d)
                packed[hop, t, 4 * d] = jnp.where(
                    lane < 3 * reach, block[0], turn(block[3], 3 * reach - spare * at)
                )
                packed[hop, t, pl.ds(4 * d + 1, 2)] = block[1:3]
            else:
                packed[hop, t, pl.ds(4 * d, 4)] = block

    def turn(value, lanes):
        lanes = lanes % width
        return pltpu.roll(value, lanes, 1) if lanes else value

    groups = ((0, 1), (2,), (3,))
    parts = [pl.ds(0, 8), pl.ds(8, 3), pl.ds(12, 4)]

    def exchange(hop, t_rel, group):
        t = lax.rem(c + t_rel, 2)
        src = packed.at[hop, t, parts[group]]
        dst = landed.at[k, parts[group], pl.ds(pl.multiple_of(8 * c, 8), 8)]
        if hop == own and t_rel == 0:
            return pltpu.make_async_copy(src, dst, a_recv.at[group])
        return pltpu.make_async_remote_copy(
            src_ref=src, dst_ref=dst,
            send_sem=a_send.at[hop // own + 2 * (group // 2)], recv_sem=a_recv.at[group],
            device_id={"gz": (later_dests if group else first_dests)[hop], "gy": t}, device_id_type=MESH_ID,
        )

    hops = list(range(n_gz))

    def hand_out(group):
        members = groups[group]
        for d in ((0, 1, 2), ())[group]:
            loads[d].wait()
        for d in members:
            pack(0, d)
        if group == 0:
            pl.semaphore_wait(barrier, 4 + 2 * middle)

            @pl.when(middle == 1)
            def _():
                tell(near_sem, mirrored(0))
                tell(far_sem, mirrored(2))
        for hop in hops:
            if hop:
                for d in members:
                    pack(hop, d)
            if group == 0 and hop == 1:

                @pl.when(middle == 0)
                def _():
                    pl.semaphore_wait(near_sem, 1)

            if group == 0 and hop == 2:
                pl.semaphore_wait(far_sem, 1)

                @pl.when(middle == 1)
                def _():
                    tell(far_sem, mirrored(0))

                pl.semaphore_signal(
                    side_sem, inc=1, device_id={"ta": 1 - a}, device_id_type=MESH_ID
                )
            for t_rel in range(2):
                exchange(hop, t_rel, group).start()

    hand_out(0)
    hand_out(1)
    loads[3].wait()
    for hop in hops:
        pack(hop, 3)

    def start_late():
        for hop in hops:
            for t_rel in range(2):
                exchange(hop, t_rel, 2).start()

    def arrived(group):
        settle(landed.at[:, parts[group]], a_recv.at[group])

    def by_slot(values):
        tile = values[-1]
        for g in reversed(range(len(values) - 1)):
            tile = jnp.where(lane < slot * (g + 1), values[g], tile)
        return tile

    places = [[(z, 0) for z in range(3)], [(z, 1) for z in range(3)], [(3, 0), (3, 1)]]

    def closed(read):
        rows = [[(read(0, r, j), read(1, r, j)) for j in range(3)] for r in range(2)]
        rows.append(third_row(rows[0], rows[1]))
        return rows

    def gather_spill():
        for z in range(n_gz):
            for half in range(2):
                rows = pl.ds(8 * half, 8)
                tile = None
                for at, n in reversed(list(enumerate(spread_over))):
                    piece = turn(landed[z, n, rows], spare * at - 3 * reach)
                    tile = (
                        piece if tile is None
                        else jnp.where(lane < spare * (at + 1), piece, tile)
                    )
                landed[z, spilled, rows] = tile

    def unpack(d):
        if d == 2:
            gather_spill()
        for tile in tiles:

            def entry(ri, r, j):
                return by_slot([
                    turn(
                        landed[z, 4 * d + 2 * ri + r, pl.ds(h, 8, stride=2)],
                        slot * g - reach * j + 1,
                    )
                    for g, (z, h) in enumerate(places[tile])
                ])

            put(d, tile, closed(entry))

    def put(d, tile, mat):
        for r in range(3):
            for j in range(3):
                for ri in range(2):
                    state[d, ri, r, j, tile] = mat[r][j][ri]

    def get(read, rows=3):
        return [[(read(0, r, j), read(1, r, j)) for j in range(3)] for r in range(rows)]

    def down(value):
        return pltpu.roll(value, 7, 0)

    def up_row(value):
        return pltpu.roll(value, 1, 0)

    def shift_plus(read, nu, tile):
        if nu == 0:
            return turn(read(tile), -1)
        if nu == 1:
            if tile == 0:
                return read(1)
            if tile == 1:
                return down(read(0))
            return by_slot([turn(read(2), -slot), down(turn(read(2), slot))])
        if tile == 2:
            return by_slot([read(0), turn(read(1), slot)])
        inner = turn(read(tile), -slot)
        return jnp.where(lane < 2 * slot, inner, turn(read(2), slot * (2 - tile)))

    def shift_minus(read, nu, tile):
        if nu == 0:
            return turn(read(tile), 1)
        if nu == 1:
            if tile == 0:
                return up_row(read(1))
            if tile == 1:
                return read(0)
            return by_slot([up_row(turn(read(2), -slot)), turn(read(2), slot)])
        if tile == 2:
            return by_slot([turn(read(0), -2 * slot), turn(read(1), -slot)])
        return by_slot([turn(read(2), -slot * tile), turn(read(tile), slot)])

    def here(d, tile):
        return get(lambda ri, r, j: state[d, ri, r, j, tile])

    def plus(d, nu, tile):
        return get(
            lambda ri, r, j: shift_plus(lambda other: state[d, ri, r, j, other], nu, tile)
        )

    def keep(ref, entry, tile, mat):
        for r in range(2):
            for j in range(3):
                for ri in range(2):
                    ref[entry, ri, r, j, tile] = mat[r][j][ri]

    pairs = [(0, 1), (0, 2), (1, 2)]
    slot_of = {}
    for mu in range(3):
        for nu in range(3):
            if mu != nu:
                slot_of[mu, nu] = len(slot_of)

    def staples(chosen):
        for tile in tiles:
            for mu, nu in chosen:
                u_mu, u_nu = here(mu, tile), here(nu, tile)
                nu_ahead, mu_ahead = plus(nu, mu, tile), plus(mu, nu, tile)
                one = times(u_mu, nu_ahead)
                keep(lows, slot_of[mu, nu], tile, times(u_nu, one, lhs_dag=True, rows=2))
                keep(ups, slot_of[nu, mu], tile, times(one, mu_ahead, rhs_dag=True, rows=2))
                two = times(u_nu, mu_ahead)
                keep(lows, slot_of[nu, mu], tile, times(u_mu, two, lhs_dag=True, rows=2))
                keep(ups, slot_of[mu, nu], tile, times(two, nu_ahead, rhs_dag=True, rows=2))

    final_x = 4

    def staples_first():
        for tile in tiles:
            for nu in (1, 2):
                u_mu, u_nu = here(0, tile), here(nu, tile)
                nu_ahead, mu_ahead = plus(nu, 0, tile), plus(0, nu, tile)
                one = times(u_mu, nu_ahead)
                two = times(u_nu, mu_ahead)
                keep(lows, slot_of[0, nu], tile, times(u_nu, one, lhs_dag=True, rows=2))
                keep(ups, slot_of[0, nu], tile, times(two, nu_ahead, rhs_dag=True, rows=2))
                for row, line in enumerate(one[0:2] + two):
                    for j in range(3):
                        for ri in range(2):
                            stash[nu - 1, row, ri, j, tile] = line[j][ri]

    def staples_rest(nu):
        for tile in tiles:
            rows = [
                [(stash[nu - 1, row, 0, j, tile], stash[nu - 1, row, 1, j, tile])
                 for j in range(3)]
                for row in range(5)
            ]
            one, two = rows[0:2], rows[2:5]
            keep(lows, slot_of[nu, 0], tile, times(here(0, tile), two, lhs_dag=True, rows=2))
            mu_ahead = plus(0, nu, tile)
            keep(ups, slot_of[nu, 0], tile, times(one, mu_ahead, rhs_dag=True, rows=2))

    def mix(d, tile, entries, factor):
        def entry(ri, r, j):
            total = None
            for at, nu in entries:
                low = shift_minus(lambda other: lows[at, ri, r, j, other], nu, tile)
                part = ups[at, ri, r, j, tile] + low
                total = part if total is None else total + part
            return (1.0 - smear_weight) * state[d, ri, r, j, tile] + factor * total

        return project_rows(get(entry, rows=2))

    def update(chosen):
        for tile in tiles:
            for mu in chosen:
                entries = [(slot_of[mu, nu], nu) for nu in range(3) if nu != mu]
                put(mu, tile, mix(mu, tile, entries, smear_weight / 4.0))
    arrived(0)
    unpack(0)
    unpack(1)

    def sweep(index, carry):
        staples(pairs[0:1])

        @pl.when(index == 0)
        def _():
            arrived(1)
            start_late()
            unpack(2)

        staples(pairs[1:3])
        update((0, 1, 2))
        return carry
    lax.fori_loop(0, ITERS - 1, sweep, 0)

    comps = [(ri, r, j) for ri in range(2) for r in range(2) for j in range(3)]
    n_dense = 2 * len(comps)
    in_slot = lax.rem(lane, slot)

    def next_copy(mu):
        return pltpu.make_async_remote_copy(
            src_ref=outgoing.at[mu - 1] if mu else outgoing_x,
            dst_ref=ahead.at[mu - 1] if mu else ahead_x,
            send_sem=n_send.at[int(mu > 0)], recv_sem=n_recv.at[mu],
            device_id={"ta": lax.rem(a + c + n_ta - 1, n_ta), "gy": 1 - c},
            device_id_type=MESH_ID,
        )

    def send_next(mu):
        out = outgoing.at[mu - 1] if mu else outgoing_x
        done = mu or final_x
        for q, (ri, r, j) in enumerate(comps):
            rest = state[done, ri, r, j, 2]
            for tile in range(2):
                full = state[done, ri, r, j, tile]
                dense = turn(rest, 3 * quarter - HALO - slot * tile)
                for g in reversed(range(3)):
                    dense = jnp.where(
                        lane < quarter * (g + 1),
                        turn(full, (quarter - slot) * g - HALO),
                        dense,
                    )
                out[2 * q + tile] = dense
        if mu == 0:
            for tile in tiles:
                edge = None
                for q, (ri, r, j) in enumerate(comps):
                    piece = turn(state[done, ri, r, j, tile], q + 1 - HALO)
                    edge = piece if edge is None else jnp.where(in_slot == q, piece, edge)
                out[n_dense + tile] = edge
        next_copy(mu).start()

    def later_links(mu, tile):
        source = ahead.at[mu - 1] if mu else ahead_x

        def entry(ri, r, j):
            q = comps.index((ri, r, j))
            if tile < 2:
                dense = source[2 * q + tile]
                value = by_slot([turn(dense, (slot - quarter) * g + HALO) for g in range(3)])
            else:
                value = by_slot([
                    turn(source[2 * q + half], slot * half + HALO - 3 * quarter)
                    for half in range(2)
                ])
            if mu == 0:
                edge = turn(source[n_dense + tile], HALO - 1 - q)
                value = jnp.where(in_slot == HALO - 1, edge, value)
            return value

        return closed(entry)
    pl.semaphore_wait(side_sem, 1)
    staples_first()
    for tile in tiles:
        entries = [(slot_of[0, nu], nu) for nu in (1, 2)]
        put(final_x, tile, mix(0, tile, entries, smear_weight / 4.0))
    send_next(0)
    staples_rest(1)
    staples(pairs[2:3])
    update((1,))
    send_next(1)
    staples_rest(2)
    update((2,))
    send_next(2)
    arrived(2)
    unpack(3)

    def time_firsts():
        for tile in tiles:
            for nu in range(3):
                u_nu = here(nu or final_x, tile)
                keep(ups, nu, tile, times(u_nu, plus(3, nu, tile), rows=2))
                keep(lows, nu, tile, times(u_nu, here(3, tile), lhs_dag=True, rows=2))

    def time_staples(nu):
        for tile in tiles:
            later = later_links(nu, tile)
            up = get(lambda ri, r, j: ups[nu, ri, r, j, tile], rows=2)
            keep(ups, nu, tile, times(up, later, rhs_dag=True, rows=2))
            low = get(lambda ri, r, j: lows[nu, ri, r, j, tile], rows=2)
            keep(lows, nu, tile, times(low, later, rows=2))

    factor = smear_weight / 6.0

    def sum_two():
        for tile in tiles:
            for ri, r, j in comps:
                total = None
                for nu in range(2):
                    low = shift_minus(lambda other: lows[nu, ri, r, j, other], nu, tile)
                    part = ups[nu, ri, r, j, tile] + low
                    total = part if total is None else total + part
                kept = (1.0 - smear_weight) * state[3, ri, r, j, tile]
                ups[3, ri, r, j, tile] = kept + factor * total

    def smooth(tile):
        def entry(ri, r, j):
            low = shift_minus(lambda other: lows[2, ri, r, j, other], 2, tile)
            return ups[3, ri, r, j, tile] + factor * (ups[2, ri, r, j, tile] + low)

        return project_rows(get(entry, rows=2))

    me = n_gy * a + c
    rank = (a * n_gz + k) * n_gy + c

    def lay_out(z, mats):
        for r in range(2):
            for j in range(3):
                dense = None
                for p in reversed(range(4)):
                    mat, g = mats[p // 2]
                    piece = turn(mat[r][j][p % 2], quarter * p - slot * g - HALO)
                    dense = (
                        piece if dense is None
                        else jnp.where(lane < quarter * (p + 1), piece, dense)
                    )
                smooth_out[z, r, j] = dense

    def deliver(z):
        pltpu.make_async_remote_copy(
            src_ref=smooth_out.at[z], dst_ref=smooth_in.at[me],
            send_sem=w_send.at[0], recv_sem=w_recv.at[0],
            device_id={"ta": z // n_gy, "gy": lax.rem(z, n_gy)}, device_id_type=MESH_ID,
        ).start()
    time_firsts()
    for nu in range(3):
        next_copy(nu).wait_recv()
        time_staples(nu)
        if nu == 1:
            sum_two()
    mats = [smooth(tile) for tile in tiles]
    for z in range(n_gz):
        lay_out(z, [(mats[0], z), (mats[1], z)] if z < 3 else [(mats[2], 0), (mats[2], 1)])
    for z in (n_gy * (1 - a), n_gy * (1 - a) + 1, n_gy * a + 1 - c):
        deliver(z)
    smooth_in[me] = smooth_out[me]
    settle(smooth_out.at[pl.ds(1, n_ta * n_gy - 1)], w_recv.at[0])

    def time_link(t):
        rows = []
        for r in range(2):
            tiles = [smooth_in[t, r, j] for j in range(3)]
            rows.append([(tile, pltpu.roll(tile, width - quarter, 1)) for tile in tiles])
        rows.append(third_row(rows[0], rows[1]))
        return rows
    early = times(time_link(0), time_link(1))
    late = times(time_link(2), time_link(3))
    re_terms, im_terms = [], []
    for i in range(3):
        for j in range(3):
            p_re, p_im = early[i][j]
            q_re, q_im = late[j][i]
            re_terms += [(1, p_re * q_re), (-1, p_im * q_im)]
            im_terms += [(1, p_re * q_im), (1, p_im * q_re)]
    trace_re = signed_sum(re_terms) / 3.0
    trace_im = signed_sum(im_terms) / 3.0
    trace = jnp.where(lax.rem(lane, 2 * quarter) < quarter, trace_re, turn(trace_im, quarter))
    trace_out[...] = trace
    sums = jnp.sum(trace, axis=0, keepdims=True)
    row_out[0] = sums
    for z in range(n_gz):
        for da in range(n_ta):
            for dc in range(n_gy):
                copy = pltpu.make_async_remote_copy(
                    src_ref=row_out, dst_ref=rows_in.at[pl.ds(rank, 1)],
                    send_sem=r_send.at[0], recv_sem=r_recv.at[0],
                    device_id={"ta": lax.rem(a + da, n_ta), "gz": z, "gy": lax.rem(c + dc, n_gy)},
                    device_id_type=MESH_ID,
                )
                if da or dc:
                    copy.start()
                else:
                    pl.when(k != z)(copy.start)
    rows_in[pl.ds(rank, 1)] = row_out[...]
    keeps_one = k == me
    for ta in range(n_ta):
        for gy in range(n_gy):
            is_self = keeps_one & (a == ta) & (c == gy)
            remote = pltpu.make_async_remote_copy(
                src_ref=trace_out, dst_ref=traces.at[k],
                send_sem=t_send.at[0], recv_sem=t_recv.at[0],
                device_id={"ta": ta, "gz": me, "gy": gy}, device_id_type=MESH_ID,
            )
            local = pltpu.make_async_copy(trace_out, traces.at[k], t_recv.at[0])
            pl.when(jnp.logical_not(is_self))(remote.start)
            pl.when(is_self)(local.start)

    settle(traces, t_recv.at[0])
    for ri in range(2):
        for h in range(2):
            out = None
            for z in reversed(range(n_gz)):
                piece = turn(traces[z], quarter * (z - 2 * h - ri))
                out = piece if out is None else jnp.where(lane < quarter * (z + 1), piece, out)
            half = pltpu.roll(out, lax.rem(8 - 4 * c, 8), 0)
            poly_ref[ri, pl.ds(h, 4, stride=2)] = half[0:4]
    settle(rows_in.at[pl.ds(1, n_group - 1)], r_recv.at[0])
    total = rows_in[0]
    for step in range(1, n_group):
        total = total + rows_in[step]
    total_ref[...] = total
    for late, sent in enumerate((pl.ds(0, 11), parts[2])):
        settle(packed.at[pl.ds(0, own), :, sent], a_send.at[2 * late])
        settle(packed.at[own, 0, sent], a_send.at[2 * late + 1])
    settle(ahead_x, n_send.at[0])
    settle(outgoing, n_send.at[1])
    settle(smooth_out.at[pl.ds(1, n_ta * n_gy - 1)], w_send.at[0])

    @pl.when(keeps_one)
    def _():
        settle(traces.at[pl.ds(1, n_gz - 1)], t_send.at[0])

    @pl.when(jnp.logical_not(keeps_one))
    def _():
        settle(traces, t_send.at[0])

    settle(rows_in.at[pl.ds(1, n_group - 1)], r_send.at[0])
def hand_over(quarter, sites, poly_in, total_in, poly_ref, mean_ref):
    poly_ref[...] = poly_in[...]
    total = total_in[...]
    place = lax.broadcasted_iota(jnp.int32, total.shape, 1)
    real = lax.rem(place, 2 * quarter) < quarter
    mean_ref[0] = jnp.sum(jnp.where(real, total, 0.0)) / sites
    mean_ref[1] = jnp.sum(jnp.where(real, 0.0, total)) / sites


def fused_on_device(mesh_shape, spatial_links, time_links):
    n_ta, n_gz, n_gy = (mesh_shape[name] for name in ("ta", "gz", "gy"))
    width = spatial_links.shape[-1]
    n_group = n_ta * n_gz * n_gy
    sites = float(n_gz * n_gy * 8 * width)
    spatial = spatial_links.reshape(3, 2, 3, 3, 2, 8, width)
    times_in = time_links.reshape(2, 3, 3, 2, 8, width)
    vm = lambda *shape: pltpu.VMEM(shape + (8, width), jnp.float32)
    dma = pltpu.SemaphoreType.DMA
    poly, total = pl.pallas_call(
        partial(fused_kernel, (n_ta, n_gz, n_gy, width, sites)),
        out_shape=(
            pltpu.VMEM((2, 8, width), jnp.float32),
            pltpu.VMEM((1, width), jnp.float32),
        ),
        in_specs=[pl.BlockSpec(memory_space=pl.ANY)] * 2,
        out_specs=(pl.BlockSpec(memory_space=pltpu.VMEM),) * 2,
        scratch_shapes=[
            vm(4, 2, 3, 3, 2),
            vm(n_gz, 2, 16),
            pltpu.VMEM((n_gz, 16, 2 * 8, width), jnp.float32),
            vm(5, 2, 3, 3, 3),
            vm(2, 5, 2, 3, 3),
            vm(6, 2, 2, 3, 3),
            vm(6, 2, 2, 3, 3),
            vm(2, 24),
            vm(27),
            vm(2, 24),
            vm(27),
            vm(4, 2, 3),
            vm(4, 2, 3),
            vm(),
            vm(n_gz),
            pltpu.VMEM((1, 1, width), jnp.float32),
            pltpu.VMEM((n_group, 1, width), jnp.float32),
            dma((4,)),
            dma((4,)), dma((3,)), dma((2,)), dma((3,)),
            *[dma((1,))] * 6,
            *[pltpu.SemaphoreType.REGULAR] * 3,
        ],
        compiler_params=pltpu.CompilerParams(collective_id=0, has_side_effects=True),
    )(spatial, times_in)
    poly, mean = pl.pallas_call(
        partial(hand_over, width // n_gz, sites),
        out_shape=(
            jax.ShapeDtypeStruct((2, 8, width), jnp.float32),
            jax.ShapeDtypeStruct((2,), jnp.float32),
        ),
        in_specs=[pl.BlockSpec(memory_space=pltpu.VMEM)] * 2,
        out_specs=(
            pl.BlockSpec(memory_space=pltpu.VMEM),
            pl.BlockSpec(memory_space=pltpu.SMEM),
        ),
    )(*[pltpu.with_memory_space_constraint(x, pltpu.VMEM) for x in (poly, total)])
    return poly.reshape(2, 1, 8, width), mean


def fits_fused(mesh_shape, shape):
    width = shape[-1]
    n_ta, n_gz, n_gy = (mesh_shape[name] for name in ("ta", "gz", "gy"))
    per = shape[4] // n_ta, shape[5] // n_gz, shape[6] // n_gy
    window = width // n_gz + 2 * HALO
    return (
        per == (2, 1, 8) and n_ta == 2 and n_gz == 4 and n_gy == 2
        and width == 128 and ITERS >= 2 and window <= width // 3
    )


def solution(mesh):
    placed = (
        P("cfg", None, None, None, "ta", "gz", "gy", None),
        P("cfg", None, None, "ta", "gz", "gy", None),
    )

    def run(spatial_links, time_links):
        fused = fits_fused(mesh.shape, spatial_links.shape)
        body = partial(fused_on_device, dict(mesh.shape)) if fused else on_device
        return jax.shard_map(
            body,
            mesh=mesh,
            in_specs=placed,
            out_specs=(P("cfg", "gz", "gy", None), P("cfg")),
            check_vma=False,
        )(spatial_links, time_links)

    return run
```
